32 devices in a mesh: row: 16 (over z, y, core), col: 2 (over x).
Axes of the slice: x: 2, y: 2, z: 4, core: 2. Of those that a mesh axis runs over, the one named last changes fastest.
Arguments:
- pair_act: bfloat16 [192, 192, 128], P('row', 'col'), may hold values from -6 to 6
- tile_mask: int32 [12, 12], replicated, may hold values 0 or 1
- w_left_gate: bfloat16 [128, 128], replicated, may hold values from -0.5 to 0.5
- w_left: bfloat16 [128, 128], replicated, may hold values from -0.5 to 0.5
- w_right_gate: bfloat16 [128, 128], replicated, may hold values from -0.5 to 0.5
- w_right: bfloat16 [128, 128], replicated, may hold values from -0.5 to 0.5
- w_out_gate: bfloat16 [128, 128], replicated, may hold values from -0.5 to 0.5
- w_out: bfloat16 [128, 128], replicated, may hold values from -0.5 to 0.5
Outputs:
- update: bfloat16 [192, 192, 128], P('row', 'col')
The draws below stay inside these ranges and needn't reach their ends.
All inputs are finite; a program needn't handle non-finite values.
Results may differ from the reference program's by a relative error of at most 0.0083.
Values may be sent and summed in bfloat16 or wider, within the bound.
A program may use at most 64 MiB of HBM per device.

```python
import jax
import jax.numpy as jnp
from jax import lax

CZ = 128
CH = 128
TILES = 12
RES = 192
TILE = 16


def with_ends(result, stream_key, least, largest):
    extent = result.shape
    spot = [jax.random.randint(jax.random.fold_in(stream_key, axis), (), 0, extent[axis]) for axis in range(len(extent))]
    result = result.at[tuple(spot)].set(least)
    longest = extent.index(max(extent))
    spot[longest] = (spot[longest] + 1) % extent[longest]
    return result.at[tuple(spot)].set(largest)


def block_scale(own_key, extent, cuts, low, largest):
    gain, own = 1.0, jax.random.fold_in(own_key, 6)
    for position, shards_of in cuts:
        steps = jnp.exp(jax.random.uniform(jax.random.fold_in(own, position), (shards_of,), jnp.float32, low / len(cuts), largest / len(cuts)))
        gain = gain * jnp.repeat(steps, extent[position] // shards_of).reshape([-1 if axis == position else 1 for axis in range(len(extent))])
    return gain


def normal_values(key, shape, scale, most, cuts=(), kind=jnp.bfloat16):
    entries = scale * jax.random.normal(key, shape, jnp.float32)
    if cuts:
        entries = entries * block_scale(key, shape, cuts, -0.22, 0.18)
    return jnp.clip(entries, -most, most).astype(kind)


def setup_inputs(seed: int = 0) -> dict:
    arg_keys = jax.random.split(jax.random.key(seed), 9)
    return {
        "pair_act": normal_values(arg_keys[0], (RES, RES, CZ), 1.0, 6.0, ((0, 16), (1, 2))),
        "tile_mask": with_ends((jax.random.randint(arg_keys[1], (TILES, TILES), 0, 4) < 3).astype(jnp.int32), jax.random.fold_in(arg_keys[1], 1), 0, 1),
        "w_left_gate": normal_values(arg_keys[2], (CZ, CH), CZ ** -0.5, 0.5),
        "w_left": normal_values(arg_keys[3], (CZ, CH), CZ ** -0.5, 0.5),
        "w_right_gate": normal_values(arg_keys[4], (CZ, CH), CZ ** -0.5, 0.5),
        "w_right": normal_values(arg_keys[5], (CZ, CH), CZ ** -0.5, 0.5),
        "w_out_gate": normal_values(arg_keys[6], (CZ, CZ), CZ ** -0.5, 0.5),
        "w_out": normal_values(arg_keys[7], (CH, CZ), CH ** -0.5, 0.5),
    }


group_width = 8

def norm_last(values):
    mean = lax.optimization_barrier(jnp.mean(values, axis=-1, keepdims=True))
    centred = values - mean
    spread = lax.optimization_barrier(jnp.mean(centred * centred, axis=-1, keepdims=True))
    return centred * lax.rsqrt(spread + 1e-05)

def grouped(weight):
    return weight.reshape(CZ, CH // group_width, group_width).transpose(1, 0, 2)

def reference(pair_act, tile_mask, w_left_gate, w_left, w_right_gate, w_right, w_out_gate, w_out):
    normed = norm_last(pair_act.astype(jnp.float32)).astype(jnp.bfloat16)
    normed_f = lax.optimization_barrier(normed).astype(jnp.float32)
    tile_ids = jnp.arange(RES, dtype=jnp.int32) // TILE
    hot = (tile_ids[:, None] == jnp.arange(TILES, dtype=jnp.int32)[None, :]).astype(jnp.float32)
    pair_mask = jnp.dot(jnp.dot(hot, tile_mask.astype(jnp.float32), preferred_element_type=jnp.float32), hot.T, preferred_element_type=jnp.float32)

    def channel_group(weights):
        left_gate, left_value, right_gate, right_value = weights
        left = jax.nn.sigmoid(jnp.einsum('ikd,de->eik', normed_f, left_gate.astype(jnp.float32)))
        left = (left * jnp.einsum('ikd,de->eik', normed_f, left_value.astype(jnp.float32)) * pair_mask[None]).astype(jnp.bfloat16)
        right = jax.nn.sigmoid(jnp.einsum('jkd,de->ejk', normed_f, right_gate.astype(jnp.float32)))
        right = (right * jnp.einsum('jkd,de->ejk', normed_f, right_value.astype(jnp.float32)) * pair_mask[None]).astype(jnp.bfloat16)
        left_f = lax.optimization_barrier(left).astype(jnp.float32)
        right_f = lax.optimization_barrier(right).astype(jnp.float32)
        return jnp.einsum('cik,cjk->cij', left_f, right_f).astype(jnp.bfloat16)
    triangle = lax.map(channel_group, (grouped(w_left_gate), grouped(w_left), grouped(w_right_gate), grouped(w_right)))
    triangle = triangle.reshape(CH, RES, RES)
    triangle_f = jnp.transpose(lax.optimization_barrier(triangle), (1, 2, 0)).astype(jnp.float32)
    scaled = norm_last(triangle_f).astype(jnp.bfloat16)
    scaled_f = lax.optimization_barrier(scaled).astype(jnp.float32)
    projected = jnp.einsum('ijc,ce->ije', scaled_f, w_out.astype(jnp.float32))
    gate = jax.nn.sigmoid(jnp.einsum('ijd,de->ije', normed_f, w_out_gate.astype(jnp.float32)))
    return (gate * projected).astype(jnp.bfloat16)
```

```python
import functools

import jax
import jax.numpy as jnp
from jax import lax
from jax.experimental import pallas as pl
from jax.experimental.pallas import tpu as pltpu
from jax.sharding import PartitionSpec as P

TILES = 12
GROUP = 8
MESH = pl.DeviceIdType.MESH


def norm_axis(values, axis):
    mean = jnp.mean(values, axis=axis, keepdims=True)
    centred = values - mean
    spread = jnp.mean(centred * centred, axis=axis, keepdims=True)
    return centred * lax.rsqrt(spread + 1e-05)


def place(flat, col_size):
    return (flat // col_size, flat % col_size)


def greet(flat, first, count, col_size):
    barrier = pltpu.get_barrier_semaphore()

    def signal(step, _):
        other = first + (flat - first + step) % count
        pl.semaphore_signal(barrier, inc=1, device_id=place(other, col_size), device_id_type=MESH)
        return 0

    lax.fori_loop(1, count, signal, 0)
    pl.semaphore_wait(barrier, count - 1)


def spread_kernel(
    sizes, left, right, left_all, right_all, own_sem, left_send, left_recv, right_send, right_recv
):
    row_size, col_size, groups = sizes
    devices = row_size * col_size
    flat = lax.axis_index("row") * col_size + lax.axis_index("col")
    member = flat % groups
    first = flat - member

    def chunk(source, group):
        return source.at[group]

    own_left = pltpu.make_async_copy(chunk(left, member), left_all.at[member], own_sem.at[0])
    own_right = pltpu.make_async_copy(chunk(right, member), right_all.at[flat], own_sem.at[1])
    own_left.start()
    own_right.start()
    greet(flat, 0, devices, col_size)

    def right_copy(step):
        to = (flat + step) % devices
        return pltpu.make_async_remote_copy(
            src_ref=chunk(right, to % groups),
            dst_ref=right_all.at[flat],
            send_sem=right_send.at[step],
            recv_sem=right_recv.at[step],
            device_id=place(to, col_size),
            device_id_type=MESH,
        )

    def left_copy(step):
        to = (member + step) % groups
        return pltpu.make_async_remote_copy(
            src_ref=chunk(left, to),
            dst_ref=left_all.at[member],
            send_sem=left_send.at[step],
            recv_sem=left_recv.at[step],
            device_id=place(first + to, col_size),
            device_id_type=MESH,
        )

    def start_right(step, _):
        right_copy(step).start()
        return 0

    def start_left(step, _):
        left_copy(step).start()
        return 0

    def wait_right(step, _):
        right_copy(step).wait()
        return 0

    def wait_left(step, _):
        left_copy(step).wait()
        return 0

    lax.fori_loop(1, devices, start_right, 0)
    lax.fori_loop(1, groups, start_left, 0)
    own_left.wait()
    own_right.wait()
    lax.fori_loop(1, groups, wait_left, 0)
    lax.fori_loop(1, devices, wait_right, 0)


def return_kernel(sizes, triangle, owned, own_sem, send, recv):
    row_size, col_size, groups = sizes
    flat = lax.axis_index("row") * col_size + lax.axis_index("col")
    member = flat % groups
    first = flat - member
    own = pltpu.make_async_copy(triangle.at[member], owned.at[member], own_sem)
    own.start()
    greet(flat, first, groups, col_size)

    def copy(step):
        to = (member + step) % groups
        return pltpu.make_async_remote_copy(
            src_ref=triangle.at[to],
            dst_ref=owned.at[member],
            send_sem=send.at[step],
            recv_sem=recv.at[step],
            device_id=place(first + to, col_size),
            device_id_type=MESH,
        )

    def start(step, _):
        copy(step).start()
        return 0

    def wait(step, _):
        copy(step).wait()
        return 0

    lax.fori_loop(1, groups, start, 0)
    own.wait()
    lax.fori_loop(1, groups, wait, 0)


def local(
    sizes, pair_act, tile_mask, w_left_gate, w_left, w_right_gate, w_right, w_out_gate, w_out
):
    row_size, col_size, groups = sizes
    devices = row_size * col_size
    block_rows = groups // col_size
    rows, cols, width = pair_act.shape
    residues = rows * row_size
    tile = residues // TILES
    normed = norm_axis(pair_act.astype(jnp.float32), 2).astype(jnp.bfloat16)
    tile_range = lax.iota(jnp.int32, TILES)
    row_ids = (lax.axis_index("row") * rows + lax.iota(jnp.int32, rows)) // tile
    col_ids = (lax.axis_index("col") * cols + lax.iota(jnp.int32, cols)) // tile
    row_hot = (row_ids[:, None] == tile_range[None, :]).astype(jnp.float32)
    col_hot = (col_ids[:, None] == tile_range[None, :]).astype(jnp.float32)
    pair_mask = jnp.dot(
        jnp.dot(row_hot, tile_mask.astype(jnp.float32), preferred_element_type=jnp.float32),
        col_hot.T,
        preferred_element_type=jnp.float32,
    )
    pairs = rows * cols
    flat_normed = normed.reshape(pairs, width)
    flat_mask = pair_mask.reshape(1, pairs)

    def project(weight):
        return jnp.einsum("pd,de->ep", flat_normed, weight, preferred_element_type=jnp.float32)

    def factor(gate, value):
        out = jax.nn.sigmoid(project(gate)) * project(value) * flat_mask
        return out.astype(jnp.bfloat16).reshape(groups, GROUP, pairs)

    left = factor(w_left_gate, w_left)
    right = factor(w_right_gate, w_right)
    anywhere = pl.BlockSpec(memory_space=pl.ANY)
    left_all, right_all = pl.pallas_call(
        functools.partial(spread_kernel, sizes),
        out_shape=(
            jax.ShapeDtypeStruct((groups, GROUP, pairs), jnp.bfloat16),
            jax.ShapeDtypeStruct((devices, GROUP, pairs), jnp.bfloat16),
        ),
        in_specs=[anywhere] * 2,
        out_specs=(anywhere, anywhere),
        scratch_shapes=[
            pltpu.SemaphoreType.DMA((2,)),
            pltpu.SemaphoreType.DMA((groups,)),
            pltpu.SemaphoreType.DMA((groups,)),
            pltpu.SemaphoreType.DMA((devices,)),
            pltpu.SemaphoreType.DMA((devices,)),
        ],
        compiler_params=pltpu.CompilerParams(collective_id=0, has_side_effects=True),
    )(left, right)
    left_rows = (
        left_all.reshape(block_rows, col_size, GROUP, rows, cols)
        .transpose(2, 0, 3, 1, 4)
        .reshape(GROUP, block_rows * rows, residues)
    )
    right_rows = (
        right_all.reshape(row_size, col_size, GROUP, rows, cols)
        .transpose(2, 0, 3, 1, 4)
        .reshape(GROUP, residues, residues)
    )
    triangle = jnp.einsum(
        "cik,cjk->cij", left_rows, right_rows, preferred_element_type=jnp.float32
    ).astype(jnp.bfloat16)
    triangle = (
        triangle.reshape(GROUP, block_rows, rows, col_size, cols)
        .transpose(1, 3, 0, 2, 4)
        .reshape(groups, GROUP, pairs)
    )
    owned = pl.pallas_call(
        functools.partial(return_kernel, sizes),
        out_shape=jax.ShapeDtypeStruct((groups, GROUP, pairs), jnp.bfloat16),
        in_specs=[anywhere],
        out_specs=anywhere,
        scratch_shapes=[
            pltpu.SemaphoreType.DMA,
            pltpu.SemaphoreType.DMA((groups,)),
            pltpu.SemaphoreType.DMA((groups,)),
        ],
        compiler_params=pltpu.CompilerParams(collective_id=1, has_side_effects=True),
    )(triangle)
    owned = owned.reshape(width, pairs)
    scaled = norm_axis(owned.astype(jnp.float32), 0).astype(jnp.bfloat16)
    projected = jnp.einsum("cp,ce->pe", scaled, w_out, preferred_element_type=jnp.float32)
    gate = jax.nn.sigmoid(
        jnp.einsum("pd,de->pe", flat_normed, w_out_gate, preferred_element_type=jnp.float32)
    )
    return (gate * projected).astype(jnp.bfloat16).reshape(rows, cols, width)


LANES = 128


def fused_kernel(
    sizes, shape, pair_in, tiles_in, *rest
):
    weights_in, out = rest[:6], rest[6]
    (
        pair, tiles, w_left_gate, w_left, w_right_gate, w_right, w_out_gate, w_out, input_sem,
        normed, gate, left, right, left_all, right_all, left_mat, right_mat, left_lines, product, triangle, owned,
        left_send, left_recv, right_send, right_recv, back_send, back_recv,
    ) = rest[7:]
    kept = (pair, tiles, w_left_gate, w_left, w_right_gate, w_right, w_out_gate, w_out)
    fetches = [
        pltpu.make_async_copy(source, target, input_sem.at[index])
        for index, (source, target) in enumerate(zip((pair_in, tiles_in, *weights_in), kept))
    ]
    row_size, col_size, groups = sizes
    rows, cols, width = shape
    devices = row_size * col_size
    blocks = devices // groups
    block_rows = groups // col_size
    pairs = rows * cols
    tile = rows * row_size // TILES
    row, col = lax.axis_index("row"), lax.axis_index("col")
    flat = row * col_size + col
    member = flat % groups
    block = flat // groups
    first = block * groups

    barrier = pltpu.get_barrier_semaphore()

    def signal(step, _):
        pl.semaphore_signal(
            barrier, inc=1, device_id=place((flat + step) % devices, col_size), device_id_type=MESH
        )
        return 0

    fetches[0].start()
    lax.fori_loop(1, devices, signal, 0)
    for fetch in fetches[1:]:
        fetch.start()
    fetches[0].wait()

    values = pair[...].astype(jnp.float32)
    normed[...] = norm_axis(values, 1).astype(jnp.bfloat16)

    for fetch in fetches[1:]:
        fetch.wait()
    spot = lax.broadcasted_iota(jnp.int32, (1, pairs), 1)
    within = spot
    for line in range(1, rows):
        within = jnp.where(spot >= line * cols, spot - line * cols, within)
    tile_ids = lax.broadcasted_iota(jnp.int32, (TILES, pairs), 0)
    row_low = (tile_ids * tile - row * rows) * cols
    row_hot = ((spot >= row_low) & (spot < row_low + tile * cols)).astype(jnp.float32)
    col_low = tile_ids * tile - col * cols
    col_hot = ((within >= col_low) & (within < col_low + tile)).astype(jnp.float32)
    picked = jnp.dot(tiles[...].astype(jnp.float32).T, row_hot, preferred_element_type=jnp.float32)
    mask = jnp.sum(picked * col_hot, axis=0, keepdims=True)

    def project(weight):
        turned = weight[...].astype(jnp.float32).T.astype(jnp.bfloat16)
        return lax.dot_general(
            turned, normed[...], (((1,), (1,)), ((), ())), preferred_element_type=jnp.float32
        )

    def factor(gate_weight, weight, target):
        made = jax.nn.sigmoid(project(gate_weight)) * project(weight) * mask
        for group in range(groups):
            target[group] = made[group * GROUP : (group + 1) * GROUP].astype(jnp.bfloat16)

    def right_copy(ahead, step):
        to = (member + step) % groups
        return pltpu.make_async_remote_copy(
            src_ref=right.at[to],
            dst_ref=right_all.at[flat],
            send_sem=right_send.at[ahead * groups + step],
            recv_sem=right_recv.at[ahead * groups + step],
            device_id=place((block + ahead) % blocks * groups + to, col_size),
            device_id_type=MESH,
        )

    def member_copy(source, target, send, recv, step):
        to = (member + step) % groups
        return pltpu.make_async_remote_copy(
            src_ref=source.at[to],
            dst_ref=target.at[member],
            send_sem=send.at[step],
            recv_sem=recv.at[step],
            device_id=place(first + to, col_size),
            device_id_type=MESH,
        )

    def left_copy(step):
        return member_copy(left, left_all, left_send, left_recv, step)

    def back_copy(to, slot):
        return pltpu.make_async_remote_copy(
            src_ref=triangle.at[to],
            dst_ref=owned.at[slot],
            send_sem=back_send.at[to],
            recv_sem=back_recv.at[slot],
            device_id=place(first + to, col_size),
            device_id_type=MESH,
        )

    def each(start, stop, do):
        def body(step, _):
            do(step)
            return 0

        lax.fori_loop(start, stop, body, 0)

    factor(w_right_gate, w_right, right)
    factor(w_left_gate, w_left, left)
    pl.semaphore_wait(barrier, devices - 1)
    each(1, groups, lambda step: right_copy(0, step).start())
    each(1, groups, lambda step: left_copy(step).start())
    for ahead in range(1, blocks):
        each(0, groups, lambda step: right_copy(ahead, step).start())

    gate[...] = jax.nn.sigmoid(
        jnp.dot(normed[...], w_out_gate[...], preferred_element_type=jnp.float32)
    )
    left_mat[...] = jnp.zeros_like(left_mat)
    right_mat[...] = jnp.zeros_like(right_mat)
    lane = lax.broadcasted_iota(jnp.int32, (GROUP, LANES), 1)

    def spread(chunk, target, half, start):
        parts = [
            chunk[:, at : at + LANES].astype(jnp.float32) for at in range(0, pairs, LANES)
        ]
        for line in range(rows):
            at, off = divmod(line * cols, LANES)
            part = parts[at]
            if off:
                part = pltpu.roll(part, LANES - off, 1)
                if off + cols > LANES:
                    part = jnp.where(
                        lane < LANES - off, part, pltpu.roll(parts[at + 1], LANES - off, 1)
                    )
            part = jnp.where(lane < cols, part, 0.0)
            target[half, pl.ds(pl.multiple_of((start + line) * GROUP, GROUP), GROUP), :] = part

    def place_right(source, chunk):
        line = source // col_size * rows
        start = line // cols * LANES + line % cols
        spread(chunk, right_mat, source % col_size, start)

    def place_left(source, chunk):
        spread(chunk, left_mat, source % col_size, source // col_size * rows)

    place_right(flat, right[member])
    place_left(member, left[member])

    def take_right(ahead, step):
        right_copy(ahead, step).wait_recv()
        source = (block - ahead + blocks) % blocks * groups + (member - step + groups) % groups
        place_right(source, right_all[source])

    def take_left(step):
        left_copy(step).wait_recv()
        source = (member - step + groups) % groups
        place_left(source, left_all[source])

    each(1, groups, lambda step: take_right(0, step))
    each(1, groups, take_left)
    block_lines = block_rows * rows

    def channel(target, index, start, count):
        first_line = pl.multiple_of(start * GROUP, GROUP) + index
        return jnp.concatenate(
            [
                target[half, pl.ds(first_line, count, stride=GROUP), :].astype(jnp.bfloat16)
                for half in range(col_size)
            ],
            axis=1,
        )

    for index in range(GROUP):
        left_lines[index] = channel(left_mat, index, 0, block_lines)

    def finish(half):
        for index in range(GROUP):
            made = lax.dot_general(
                left_lines[index],
                channel(right_mat, index, half * LANES, LANES),
                (((1,), (1,)), ((), ())),
                preferred_element_type=jnp.float32,
            )
            product[pl.ds(index, block_lines, stride=GROUP), :] = made

        def pack(step):
            part_row = (member // col_size + step) % block_rows
            to = part_row * col_size + half
            lines = [
                product[pl.ds(pl.multiple_of((part_row * rows + line) * GROUP, GROUP), GROUP), :]
                for line in range(rows)
            ]
            for at in range(pairs // LANES):
                low = at * LANES
                line, off = divmod(low, cols)
                part = pltpu.roll(lines[line], LANES - off, 1) if off else lines[line]
                have = cols - off
                while have < LANES:
                    line += 1
                    part = jnp.where(lane < have, part, pltpu.roll(lines[line], have, 1))
                    have += cols
                triangle[to, :, low : low + LANES] = part.astype(jnp.bfloat16)

            @pl.when(to != member)
            def _():
                back_copy(to, member).start()

        each(0, block_rows, pack)

    finish(block)
    for ahead in range(1, blocks):
        each(0, groups, lambda step: take_right(ahead, step))
        finish((block - ahead + blocks) % blocks)
    owned[member] = triangle[member]
    each(1, groups, lambda step: left_copy(step).wait_send())
    each(1, groups, lambda step: right_copy(0, step).wait_send())
    for ahead in range(1, blocks):
        each(0, groups, lambda step: right_copy(ahead, step).wait_send())

    def wait_back(step):
        other = (member + step) % groups
        back_copy(other, other).wait()

    each(1, groups, wait_back)

    for at in range(0, pairs, LANES):
        piece = jnp.concatenate(
            [owned[group, :, at : at + LANES].astype(jnp.float32) for group in range(groups)],
            axis=0,
        )
        scaled = norm_axis(piece, 0).T.astype(jnp.bfloat16)
        projected = jnp.dot(scaled, w_out[...], preferred_element_type=jnp.float32)
        out[at : at + LANES] = (gate[at : at + LANES] * projected).astype(jnp.bfloat16)


def fused(sizes, pair_act, tile_mask, *weights):
    row_size, col_size, groups = sizes
    devices = row_size * col_size
    block_rows = groups // col_size
    rows, cols, width = pair_act.shape
    pairs = rows * cols
    kept = pl.BlockSpec(memory_space=pltpu.VMEM)
    dma = pltpu.SemaphoreType.DMA
    chunks = pltpu.VMEM((groups, GROUP, pairs), jnp.bfloat16)
    result = pl.pallas_call(
        functools.partial(fused_kernel, sizes, pair_act.shape),
        out_shape=pltpu.VMEM((pairs, width), jnp.bfloat16),
        in_specs=[pl.BlockSpec(memory_space=pltpu.HBM)] * 8,
        out_specs=pl.BlockSpec(memory_space=pltpu.VMEM),
        scratch_shapes=[
            pltpu.VMEM((pairs, width), jnp.bfloat16),
            pltpu.VMEM(tile_mask.shape, tile_mask.dtype),
            *[pltpu.VMEM(weight.shape, weight.dtype) for weight in weights],
            dma((8,)),
            pltpu.VMEM((pairs, width), jnp.bfloat16),
            pltpu.VMEM((pairs, width), jnp.float32),
            chunks,
            chunks,
            chunks,
            pltpu.VMEM((devices, GROUP, pairs), jnp.bfloat16),
            pltpu.VMEM((col_size, block_rows * rows * GROUP, LANES), jnp.float32),
            pltpu.VMEM((col_size, col_size * LANES * GROUP, LANES), jnp.float32),
            pltpu.VMEM((GROUP, block_rows * rows, col_size * LANES), jnp.bfloat16),
            pltpu.VMEM((block_rows * rows * GROUP, LANES), jnp.float32),
            chunks,
            chunks,
            dma((groups,)),
            dma((groups,)),
            dma((devices,)),
            dma((devices,)),
            dma((groups,)),
            dma((groups,)),
        ],
        compiler_params=pltpu.CompilerParams(collective_id=2, has_side_effects=True),
    )(pair_act.reshape(pairs, width), tile_mask, *weights)
    return result.reshape(rows, cols, width)


def fits(sizes, rows, cols):
    row_size, col_size, groups = sizes
    pairs = rows * cols
    if row_size * col_size != groups * col_size or groups % col_size:
        return False
    return cols <= LANES and pairs % LANES == 0 and cols % rows == 0


def solution(mesh):
    def whole(pair_act, tile_mask, *weights):
        groups = pair_act.shape[2] // GROUP
        sizes = (mesh.shape["row"], mesh.shape["col"], groups)
        rows, cols = (pair_act.shape[0] // sizes[0], pair_act.shape[1] // sizes[1])
        body = fused if fits(sizes, rows, cols) else local
        return jax.shard_map(
            functools.partial(body, sizes),
            mesh=mesh,
            in_specs=(P("row", "col", None), P(), P(), P(), P(), P(), P(), P()),
            out_specs=P("row", "col", None),
            check_vma=False,
        )(pair_act, tile_mask, *weights)

    return whole
```

```python
import functools

import jax
import jax.numpy as jnp
from jax import lax
from jax.experimental import pallas as pl
from jax.experimental.pallas import tpu as pltpu
from jax.sharding import PartitionSpec as P

TILES = 12
GROUP = 8
MESH = pl.DeviceIdType.MESH


def norm_axis(values, axis):
    mean = jnp.mean(values, axis=axis, keepdims=True)
    centred = values - mean
    spread = jnp.mean(centred * centred, axis=axis, keepdims=True)
    return centred * lax.rsqrt(spread + 1e-05)


def place(flat, col_size):
    return (flat // col_size, flat % col_size)


def greet(flat, first, count, col_size):
    barrier = pltpu.get_barrier_semaphore()

    def signal(step, _):
        other = first + (flat - first + step) % count
        pl.semaphore_signal(barrier, inc=1, device_id=place(other, col_size), device_id_type=MESH)
        return 0

    lax.fori_loop(1, count, signal, 0)
    pl.semaphore_wait(barrier, count - 1)


def spread_kernel(
    sizes, left, right, left_all, right_all, own_sem, left_send, left_recv, right_send, right_recv
):
    row_size, col_size, groups = sizes
    devices = row_size * col_size
    flat = lax.axis_index("row") * col_size + lax.axis_index("col")
    member = flat % groups
    first = flat - member

    def chunk(source, group):
        return source.at[group]

    own_left = pltpu.make_async_copy(chunk(left, member), left_all.at[member], own_sem.at[0])
    own_right = pltpu.make_async_copy(chunk(right, member), right_all.at[flat], own_sem.at[1])
    own_left.start()
    own_right.start()
    greet(flat, 0, devices, col_size)

    def right_copy(step):
        to = (flat + step) % devices
        return pltpu.make_async_remote_copy(
            src_ref=chunk(right, to % groups),
            dst_ref=right_all.at[flat],
            send_sem=right_send.at[step],
            recv_sem=right_recv.at[step],
            device_id=place(to, col_size),
            device_id_type=MESH,
        )

    def left_copy(step):
        to = (member + step) % groups
        return pltpu.make_async_remote_copy(
            src_ref=chunk(left, to),
            dst_ref=left_all.at[member],
            send_sem=left_send.at[step],
            recv_sem=left_recv.at[step],
            device_id=place(first + to, col_size),
            device_id_type=MESH,
        )

    def start_right(step, _):
        right_copy(step).start()
        return 0

    def start_left(step, _):
        left_copy(step).start()
        return 0

    def wait_right(step, _):
        right_copy(step).wait()
        return 0

    def wait_left(step, _):
        left_copy(step).wait()
        return 0

    lax.fori_loop(1, devices, start_right, 0)
    lax.fori_loop(1, groups, start_left, 0)
    own_left.wait()
    own_right.wait()
    lax.fori_loop(1, groups, wait_left, 0)
    lax.fori_loop(1, devices, wait_right, 0)


def return_kernel(sizes, triangle, owned, own_sem, send, recv):
    row_size, col_size, groups = sizes
    flat = lax.axis_index("row") * col_size + lax.axis_index("col")
    member = flat % groups
    first = flat - member
    own = pltpu.make_async_copy(triangle.at[member], owned.at[member], own_sem)
    own.start()
    greet(flat, first, groups, col_size)

    def copy(step):
        to = (member + step) % groups
        return pltpu.make_async_remote_copy(
            src_ref=triangle.at[to],
            dst_ref=owned.at[member],
            send_sem=send.at[step],
            recv_sem=recv.at[step],
            device_id=place(first + to, col_size),
            device_id_type=MESH,
        )

    def start(step, _):
        copy(step).start()
        return 0

    def wait(step, _):
        copy(step).wait()
        return 0

    lax.fori_loop(1, groups, start, 0)
    own.wait()
    lax.fori_loop(1, groups, wait, 0)


def local(
    sizes, pair_act, tile_mask, w_left_gate, w_left, w_right_gate, w_right, w_out_gate, w_out
):
    row_size, col_size, groups = sizes
    devices = row_size * col_size
    block_rows = groups // col_size
    rows, cols, width = pair_act.shape
    residues = rows * row_size
    tile = residues // TILES
    normed = norm_axis(pair_act.astype(jnp.float32), 2).astype(jnp.bfloat16)
    tile_range = lax.iota(jnp.int32, TILES)
    row_ids = (lax.axis_index("row") * rows + lax.iota(jnp.int32, rows)) // tile
    col_ids = (lax.axis_index("col") * cols + lax.iota(jnp.int32, cols)) // tile
    row_hot = (row_ids[:, None] == tile_range[None, :]).astype(jnp.float32)
    col_hot = (col_ids[:, None] == tile_range[None, :]).astype(jnp.float32)
    pair_mask = jnp.dot(
        jnp.dot(row_hot, tile_mask.astype(jnp.float32), preferred_element_type=jnp.float32),
        col_hot.T,
        preferred_element_type=jnp.float32,
    )
    pairs = rows * cols
    flat_normed = normed.reshape(pairs, width)
    flat_mask = pair_mask.reshape(1, pairs)

    def project(weight):
        return jnp.einsum("pd,de->ep", flat_normed, weight, preferred_element_type=jnp.float32)

    def factor(gate, value):
        out = jax.nn.sigmoid(project(gate)) * project(value) * flat_mask
        return out.astype(jnp.bfloat16).reshape(groups, GROUP, pairs)

    left = factor(w_left_gate, w_left)
    right = factor(w_right_gate, w_right)
    anywhere = pl.BlockSpec(memory_space=pl.ANY)
    left_all, right_all = pl.pallas_call(
        functools.partial(spread_kernel, sizes),
        out_shape=(
            jax.ShapeDtypeStruct((groups, GROUP, pairs), jnp.bfloat16),
            jax.ShapeDtypeStruct((devices, GROUP, pairs), jnp.bfloat16),
        ),
        in_specs=[anywhere] * 2,
        out_specs=(anywhere, anywhere),
        scratch_shapes=[
            pltpu.SemaphoreType.DMA((2,)),
            pltpu.SemaphoreType.DMA((groups,)),
            pltpu.SemaphoreType.DMA((groups,)),
            pltpu.SemaphoreType.DMA((devices,)),
            pltpu.SemaphoreType.DMA((devices,)),
        ],
        compiler_params=pltpu.CompilerParams(collective_id=0, has_side_effects=True),
    )(left, right)
    left_rows = (
        left_all.reshape(block_rows, col_size, GROUP, rows, cols)
        .transpose(2, 0, 3, 1, 4)
        .reshape(GROUP, block_rows * rows, residues)
    )
    right_rows = (
        right_all.reshape(row_size, col_size, GROUP, rows, cols)
        .transpose(2, 0, 3, 1, 4)
        .reshape(GROUP, residues, residues)
    )
    triangle = jnp.einsum(
        "cik,cjk->cij", left_rows, right_rows, preferred_element_type=jnp.float32
    ).astype(jnp.bfloat16)
    triangle = (
        triangle.reshape(GROUP, block_rows, rows, col_size, cols)
        .transpose(1, 3, 0, 2, 4)
        .reshape(groups, GROUP, pairs)
    )
    owned = pl.pallas_call(
        functools.partial(return_kernel, sizes),
        out_shape=jax.ShapeDtypeStruct((groups, GROUP, pairs), jnp.bfloat16),
        in_specs=[anywhere],
        out_specs=anywhere,
        scratch_shapes=[
            pltpu.SemaphoreType.DMA,
            pltpu.SemaphoreType.DMA((groups,)),
            pltpu.SemaphoreType.DMA((groups,)),
        ],
        compiler_params=pltpu.CompilerParams(collective_id=1, has_side_effects=True),
    )(triangle)
    owned = owned.reshape(width, pairs)
    scaled = norm_axis(owned.astype(jnp.float32), 0).astype(jnp.bfloat16)
    projected = jnp.einsum("cp,ce->pe", scaled, w_out, preferred_element_type=jnp.float32)
    gate = jax.nn.sigmoid(
        jnp.einsum("pd,de->pe", flat_normed, w_out_gate, preferred_element_type=jnp.float32)
    )
    return (gate * projected).astype(jnp.bfloat16).reshape(rows, cols, width)


LANES = 128
QUAD = 4


def fused_kernel(sizes, shape, pair_in, tiles_in, *rest):
    weights_in, out = rest[:6], rest[6]
    (
        pair, tiles, weights, pair_sem, input_sem,
        normed, gate, left, right, left_all, right_all, left_mat, right_mat, left_lines, product, triangle, owned,
        send, left_recv, right_recv, back_recv,
    ) = rest[7:]
    row_size, col_size, groups = sizes
    rows, cols, width = shape
    devices = row_size * col_size
    block_rows = groups // col_size
    plane_size = groups // 2
    pairs = rows * cols
    spare = LANES - cols
    count = pairs // LANES
    extra = rows - count
    third = pairs // extra
    tile = rows * row_size // TILES
    row, col = lax.axis_index("row"), lax.axis_index("col")
    flat = row * col_size + col
    member = flat % groups
    block = flat // groups
    first = block * groups
    plane = flat // plane_size
    core = flat // col_size % 2
    moves = [bit * (1 - 2 * (flat // bit % 2)) for bit in (groups, plane_size, QUAD, 1)]

    def reach(flips, to_core):
        moved = sum(move for flip, move in zip(flips, moves) if flip)
        return flat + moved + col_size * (to_core - core)

    barrier = pltpu.get_barrier_semaphore()

    fetches = [[], []]
    for part in range(extra):
        for source, target in (
            (pair_in.at[part], pair.at[part, :, pl.ds(0, extra)]),
            (pair_in.at[extra, part], pair.at[part, :, extra]),
        ):
            fetches[0].append(pltpu.make_async_copy(source, target, pair_sem.at[part]))
    for index, source in enumerate(weights_in):
        fetches[1].append(pltpu.make_async_copy(source, weights.at[index], input_sem.at[0]))
    tile_fetch = pltpu.make_async_copy(tiles_in, tiles, input_sem.at[1])

    def all_of(ref, sem):
        return pltpu.make_async_copy(ref, ref, sem)

    with jax.named_scope("a0_begin"):
        tile_fetch.start()
        for fetch in fetches[0]:
            fetch.start()

        def signal(step, _):
            pl.semaphore_signal(
                barrier, inc=1, device_id=place((flat + step) % devices, col_size), device_id_type=MESH
            )
            return 0

        lax.fori_loop(1, devices, signal, 0)
        for fetch in fetches[1]:
            fetch.start()
        tile_fetch.wait()

    with jax.named_scope("a1_mask"):
        lane = lax.broadcasted_iota(jnp.int32, (GROUP, LANES), 1)
        low = lane < cols
        spot = lax.broadcasted_iota(jnp.int32, (TILES, LANES), 1)
        tile_low = lax.broadcasted_iota(jnp.int32, (TILES, LANES), 0) * tile
        direct = spot < cols
        masks = []
        turned_tiles = tiles[...].astype(jnp.float32).T
        for at in range(count):
            line = row * rows + jnp.where(direct, at, count + at // extra)
            within = col * cols + jnp.where(direct, spot, spot - cols + at % extra * spare)
            row_hot = ((line >= tile_low) & (line < tile_low + tile)).astype(jnp.float32)
            col_hot = ((within >= tile_low) & (within < tile_low + tile)).astype(jnp.float32)
            picked = jnp.dot(turned_tiles, row_hot, preferred_element_type=jnp.float32)
            masks.append(jnp.sum(picked * col_hot, axis=0, keepdims=True))
        mask = jnp.concatenate(masks, axis=1)

    with jax.named_scope("a2_ln"):
        for part in range(extra):
            all_of(pair.at[part], pair_sem.at[part]).wait()
            values = pair[part].reshape(third, width).astype(jnp.float32)
            normed[part * third : (part + 1) * third] = norm_axis(values, 1).astype(jnp.bfloat16)
        all_of(weights, input_sem.at[0]).wait()

    def project(index):
        turned = weights[index].astype(jnp.float32).T.astype(jnp.bfloat16)
        return lax.dot_general(
            turned, normed[...], (((1,), (1,)), ((), ())), preferred_element_type=jnp.float32
        )

    def factor(gate_index, index, target):
        made = jax.nn.sigmoid(project(gate_index)) * project(index) * mask
        for group in range(groups):
            target[group] = made[group * GROUP : (group + 1) * GROUP].astype(jnp.bfloat16)

    def copy_to(source, target, sent, received, to):
        pltpu.make_async_remote_copy(
            src_ref=source.at[to % groups],
            dst_ref=target,
            send_sem=sent,
            recv_sem=received,
            device_id=place(to, col_size),
            device_id_type=MESH,
        ).start()

    def send_right(to):
        copy_to(right, right_all.at[flat], send.at[0], right_recv.at[own_quad], to)

    def send_left(to):
        copy_to(left, left_all.at[member], send.at[1], left_recv.at[member // QUAD], to)

    def keep(source, target, received):
        return pltpu.make_async_copy(source.at[member], target, received)

    own_quad = flat // QUAD
    lows = ((1, 1), (0, 1), (1, 0), (0, 0))

    def send_across(to_core):
        for low_flips in lows:
            send_right(reach((1, 0, *low_flips), to_core))
            send_right(reach((1, 1, *low_flips), to_core))

    with jax.named_scope("a3_right"):
        factor(2, 3, right)
    with jax.named_scope("a4_bar"):
        pl.semaphore_wait(barrier, devices - 1)
    with jax.named_scope("a5_send"):
        send_across(1)
    with jax.named_scope("a6_left"):
        factor(0, 1, left)
    with jax.named_scope("a7_send"):
        for low_flips in lows:
            for to_core in range(2):
                send_left(reach((0, 1, *low_flips), to_core))
        for low_flips in lows:
            send_right(reach((0, 1, *low_flips), 0))
        for low_flips in lows:
            send_right(reach((0, 0, *low_flips), 1 - core))
            send_left(reach((0, 0, *low_flips), 1 - core))
        for low_flips in lows[:-1]:
            send_right(reach((0, 0, *low_flips), core))
            send_left(reach((0, 0, *low_flips), core))
        send_across(0)
        for low_flips in lows:
            send_right(reach((0, 1, *low_flips), 1))
        keep(left, left_all.at[member], left_recv.at[member // QUAD]).start()
        keep(right, right_all.at[flat], right_recv.at[own_quad]).start()

    with jax.named_scope("b0_gate"):
        gate[...] = jax.nn.sigmoid(
            jnp.dot(normed[...], weights[4], preferred_element_type=jnp.float32)
        )
        right_mat[...] = jnp.zeros_like(right_mat)

    def spread(chunk, target, half, start, clean):
        parts = [
            chunk[:, at : at + LANES].astype(jnp.float32) for at in range(0, pairs, LANES)
        ]
        lines = list(parts)
        for line in range(extra):
            base = line * extra
            made = pltpu.roll(parts[base], spare, 1)
            for piece in range(1, extra):
                moved = pltpu.roll(parts[base + piece], (piece + 1) * spare % LANES, 1)
                made = jnp.where(lane < piece * spare, made, moved)
            lines.append(made)
        for line, made in enumerate(lines):
            if clean:
                made = jnp.where(low, made, 0.0)
            target[half, pl.ds(pl.multiple_of((start + line) * GROUP, GROUP), GROUP), :] = made

    def place_right(source):
        line = source // col_size
        start = line // block_rows * LANES + line % block_rows * rows
        spread(right_all[source], right_mat, source % col_size, start, False)

    def place_left(source):
        spread(left_all[source], left_mat, source % col_size, source // col_size * rows, True)

    def each_of(start, length, do):
        def body(step, _):
            for index in range(QUAD):
                do(start + step * QUAD + index)
            return 0

        lax.fori_loop(0, length // QUAD, body, 0)

    quads = plane_size // QUAD

    def take(source_all, received, which, put):
        for step in range(quads):
            quad = which * quads + step
            all_of(source_all.at[pl.ds(quad * QUAD, QUAD)], received.at[quad]).wait()
            each_of(quad * QUAD, QUAD, put)

    block_lines = block_rows * rows

    def channel(target, index, start, count):
        first_line = pl.multiple_of(start * GROUP, GROUP) + index
        return jnp.concatenate(
            [
                target[half, pl.ds(first_line, count, stride=GROUP), :].astype(jnp.bfloat16)
                for half in range(col_size)
            ],
            axis=1,
        )

    def finish(half):
        for index in range(GROUP):
            made = lax.dot_general(
                left_lines[index],
                channel(right_mat, index, half * LANES, LANES),
                (((1,), (1,)), ((), ())),
                preferred_element_type=jnp.float32,
            )
            product[pl.ds(index, block_lines, stride=GROUP), :] = made

        def pack(step, _):
            part_row = (member // col_size + block_rows // 2 + step) % block_rows
            to = part_row * col_size + half
            lines = [
                product[pl.ds(pl.multiple_of((part_row * rows + line) * GROUP, GROUP), GROUP), :]
                for line in range(rows)
            ]
            for at in range(count):
                moved = pltpu.roll(
                    lines[count + at // extra], (cols - at % extra * spare) % LANES, 1
                )
                made = jnp.where(low, lines[at], moved)
                triangle[to, :, at * LANES : (at + 1) * LANES] = made.astype(jnp.bfloat16)

            @pl.when(to == member)
            def _():
                keep(triangle, owned.at[member], back_recv.at[0]).start()

            @pl.when(to != member)
            def _():
                pltpu.make_async_remote_copy(
                    src_ref=triangle.at[to],
                    dst_ref=owned.at[member],
                    send_sem=send.at[2],
                    recv_sem=back_recv.at[0],
                    device_id=place(first + to, col_size),
                    device_id_type=MESH,
                ).start()

            return 0

        lax.fori_loop(0, block_rows, pack, 0)

    early = (block + core) % 2
    with jax.named_scope("b1_left"):
        take(left_all, left_recv, plane % 2, place_left)
    with jax.named_scope("b2_near"):
        take(right_all, right_recv, early * 2 + plane % 2, place_right)
    with jax.named_scope("b3_left"):
        take(left_all, left_recv, 1 - plane % 2, place_left)
    with jax.named_scope("b4_lines"):
        for index in range(GROUP):
            left_lines[index] = channel(left_mat, index, 0, block_lines)
    with jax.named_scope("b5_far"):
        take(right_all, right_recv, early * 2 + 1 - plane % 2, place_right)
    with jax.named_scope("c0_fin"):
        finish(early)
    late = 1 - early
    with jax.named_scope("c1_near"):
        take(right_all, right_recv, late * 2 + plane % 2, place_right)
    with jax.named_scope("c2_far"):
        take(right_all, right_recv, late * 2 + 1 - plane % 2, place_right)
    with jax.named_scope("c3_fin"):
        finish(late)
    with jax.named_scope("d0_back"):
        all_of(owned, back_recv.at[0]).wait()

    with jax.named_scope("d1_out"):
        for at in range(count):
            piece = jnp.concatenate(
                [
                    owned[group, :, at * LANES : (at + 1) * LANES].astype(jnp.float32)
                    for group in range(groups)
                ],
                axis=0,
            )
            scaled = norm_axis(piece, 0).T.astype(jnp.bfloat16)
            projected = jnp.dot(scaled, weights[5], preferred_element_type=jnp.float32)
            made = (gate[at * LANES : (at + 1) * LANES] * projected).astype(jnp.bfloat16)
            out[at] = made[:cols]
            start = at % extra * spare
            out[count + at // extra, start : start + spare] = made[cols:]
    with jax.named_scope("d2_sent"):
        all_of(right_all.at[pl.ds(0, devices - 1)], send.at[0]).wait()
        all_of(left_all.at[pl.ds(0, groups - 1)], send.at[1]).wait()
        all_of(triangle.at[pl.ds(0, groups - 1)], send.at[2]).wait()


def fused(sizes, pair_act, tile_mask, *weights):
    row_size, col_size, groups = sizes
    devices = row_size * col_size
    block_rows = groups // col_size
    rows, cols, width = pair_act.shape
    pairs = rows * cols
    spare = LANES - cols
    extra = rows - pairs // LANES
    dma = pltpu.SemaphoreType.DMA
    chunks = pltpu.VMEM((groups, GROUP, pairs), jnp.bfloat16)
    result = pl.pallas_call(
        functools.partial(fused_kernel, sizes, pair_act.shape),
        out_shape=pltpu.VMEM((rows, cols, width), jnp.bfloat16),
        in_specs=[pl.BlockSpec(memory_space=pltpu.HBM)] * 8,
        out_specs=pl.BlockSpec(memory_space=pltpu.VMEM),
        scratch_shapes=[
            pltpu.VMEM((extra, extra, extra + 1, spare, width), jnp.bfloat16),
            pltpu.VMEM(tile_mask.shape, tile_mask.dtype),
            pltpu.VMEM((6, width, width), jnp.bfloat16),
            dma((extra,)),
            dma((2,)),
            pltpu.VMEM((pairs, width), jnp.bfloat16),
            pltpu.VMEM((pairs, width), jnp.float32),
            chunks,
            chunks,
            chunks,
            pltpu.VMEM((devices, GROUP, pairs), jnp.bfloat16),
            pltpu.VMEM((col_size, block_rows * rows * GROUP, LANES), jnp.float32),
            pltpu.VMEM((col_size, col_size * LANES * GROUP, LANES), jnp.float32),
            pltpu.VMEM((GROUP, block_rows * rows, col_size * LANES), jnp.bfloat16),
            pltpu.VMEM((block_rows * rows * GROUP, LANES), jnp.float32),
            chunks,
            chunks,
            dma((3,)),
            dma((groups // QUAD,)),
            dma((devices // QUAD,)),
            dma((1,)),
        ],
        compiler_params=pltpu.CompilerParams(collective_id=2, has_side_effects=True),
    )(pair_act.reshape(extra + 1, extra, extra, spare, width), tile_mask, *weights)
    return result


def fits(sizes, rows, cols):
    row_size, col_size, groups = sizes
    pairs = rows * cols
    spare = LANES - cols
    extra = rows - pairs // LANES
    if (row_size, col_size, groups) != (16, 2, 16):
        return False
    if spare <= 0 or pairs % LANES or extra <= 0:
        return False
    return rows == extra * (extra + 1) and cols == extra * spare


def solution(mesh):
    def whole(pair_act, tile_mask, *weights):
        groups = pair_act.shape[2] // GROUP
        sizes = (mesh.shape["row"], mesh.shape["col"], groups)
        rows, cols = (pair_act.shape[0] // sizes[0], pair_act.shape[1] // sizes[1])
        body = fused if fits(sizes, rows, cols) else local
        return jax.shard_map(
            functools.partial(body, sizes),
            mesh=mesh,
            in_specs=(P("row", "col", None), P(), P(), P(), P(), P(), P(), P()),
            out_specs=P("row", "col", None),
            check_vma=False,
        )(pair_act, tile_mask, *weights)

    return whole
```

```python
import functools

import jax
import jax.numpy as jnp
from jax import lax
from jax.experimental import pallas as pl
from jax.experimental.pallas import tpu as pltpu
from jax.sharding import PartitionSpec as P

TILES = 12
GROUP = 8
MESH = pl.DeviceIdType.MESH


def norm_axis(values, axis):
    mean = jnp.mean(values, axis=axis, keepdims=True)
    centred = values - mean
    spread = jnp.mean(centred * centred, axis=axis, keepdims=True)
    return centred * lax.rsqrt(spread + 1e-05)


def place(flat, col_size):
    return (flat // col_size, flat % col_size)


def greet(flat, first, count, col_size):
    barrier = pltpu.get_barrier_semaphore()

    def signal(step, _):
        other = first + (flat - first + step) % count
        pl.semaphore_signal(barrier, inc=1, device_id=place(other, col_size), device_id_type=MESH)
        return 0

    lax.fori_loop(1, count, signal, 0)
    pl.semaphore_wait(barrier, count - 1)


def spread_kernel(
    sizes, left, right, left_all, right_all, own_sem, left_send, left_recv, right_send, right_recv
):
    row_size, col_size, groups = sizes
    devices = row_size * col_size
    flat = lax.axis_index("row") * col_size + lax.axis_index("col")
    member = flat % groups
    first = flat - member

    def chunk(source, group):
        return source.at[group]

    own_left = pltpu.make_async_copy(chunk(left, member), left_all.at[member], own_sem.at[0])
    own_right = pltpu.make_async_copy(chunk(right, member), right_all.at[flat], own_sem.at[1])
    own_left.start()
    own_right.start()
    greet(flat, 0, devices, col_size)

    def right_copy(step):
        to = (flat + step) % devices
        return pltpu.make_async_remote_copy(
            src_ref=chunk(right, to % groups),
            dst_ref=right_all.at[flat],
            send_sem=right_send.at[step],
            recv_sem=right_recv.at[step],
            device_id=place(to, col_size),
            device_id_type=MESH,
        )

    def left_copy(step):
        to = (member + step) % groups
        return pltpu.make_async_remote_copy(
            src_ref=chunk(left, to),
            dst_ref=left_all.at[member],
            send_sem=left_send.at[step],
            recv_sem=left_recv.at[step],
            device_id=place(first + to, col_size),
            device_id_type=MESH,
        )

    def start_right(step, _):
        right_copy(step).start()
        return 0

    def start_left(step, _):
        left_copy(step).start()
        return 0

    def wait_right(step, _):
        right_copy(step).wait()
        return 0

    def wait_left(step, _):
        left_copy(step).wait()
        return 0

    lax.fori_loop(1, devices, start_right, 0)
    lax.fori_loop(1, groups, start_left, 0)
    own_left.wait()
    own_right.wait()
    lax.fori_loop(1, groups, wait_left, 0)
    lax.fori_loop(1, devices, wait_right, 0)


def return_kernel(sizes, triangle, owned, own_sem, send, recv):
    row_size, col_size, groups = sizes
    flat = lax.axis_index("row") * col_size + lax.axis_index("col")
    member = flat % groups
    first = flat - member
    own = pltpu.make_async_copy(triangle.at[member], owned.at[member], own_sem)
    own.start()
    greet(flat, first, groups, col_size)

    def copy(step):
        to = (member + step) % groups
        return pltpu.make_async_remote_copy(
            src_ref=triangle.at[to],
            dst_ref=owned.at[member],
            send_sem=send.at[step],
            recv_sem=recv.at[step],
            device_id=place(first + to, col_size),
            device_id_type=MESH,
        )

    def start(step, _):
        copy(step).start()
        return 0

    def wait(step, _):
        copy(step).wait()
        return 0

    lax.fori_loop(1, groups, start, 0)
    own.wait()
    lax.fori_loop(1, groups, wait, 0)


def local(
    sizes, pair_act, tile_mask, w_left_gate, w_left, w_right_gate, w_right, w_out_gate, w_out
):
    row_size, col_size, groups = sizes
    devices = row_size * col_size
    block_rows = groups // col_size
    rows, cols, width = pair_act.shape
    residues = rows * row_size
    tile = residues // TILES
    normed = norm_axis(pair_act.astype(jnp.float32), 2).astype(jnp.bfloat16)
    tile_range = lax.iota(jnp.int32, TILES)
    row_ids = (lax.axis_index("row") * rows + lax.iota(jnp.int32, rows)) // tile
    col_ids = (lax.axis_index("col") * cols + lax.iota(jnp.int32, cols)) // tile
    row_hot = (row_ids[:, None] == tile_range[None, :]).astype(jnp.float32)
    col_hot = (col_ids[:, None] == tile_range[None, :]).astype(jnp.float32)
    pair_mask = jnp.dot(
        jnp.dot(row_hot, tile_mask.astype(jnp.float32), preferred_element_type=jnp.float32),
        col_hot.T,
        preferred_element_type=jnp.float32,
    )
    pairs = rows * cols
    flat_normed = normed.reshape(pairs, width)
    flat_mask = pair_mask.reshape(1, pairs)

    def project(weight):
        return jnp.einsum("pd,de->ep", flat_normed, weight, preferred_element_type=jnp.float32)

    def factor(gate, value):
        out = jax.nn.sigmoid(project(gate)) * project(value) * flat_mask
        return out.astype(jnp.bfloat16).reshape(groups, GROUP, pairs)

    left = factor(w_left_gate, w_left)
    right = factor(w_right_gate, w_right)
    anywhere = pl.BlockSpec(memory_space=pl.ANY)
    left_all, right_all = pl.pallas_call(
        functools.partial(spread_kernel, sizes),
        out_shape=(
            jax.ShapeDtypeStruct((groups, GROUP, pairs), jnp.bfloat16),
            jax.ShapeDtypeStruct((devices, GROUP, pairs), jnp.bfloat16),
        ),
        in_specs=[anywhere] * 2,
        out_specs=(anywhere, anywhere),
        scratch_shapes=[
            pltpu.SemaphoreType.DMA((2,)),
            pltpu.SemaphoreType.DMA((groups,)),
            pltpu.SemaphoreType.DMA((groups,)),
            pltpu.SemaphoreType.DMA((devices,)),
            pltpu.SemaphoreType.DMA((devices,)),
        ],
        compiler_params=pltpu.CompilerParams(collective_id=0, has_side_effects=True),
    )(left, right)
    left_rows = (
        left_all.reshape(block_rows, col_size, GROUP, rows, cols)
        .transpose(2, 0, 3, 1, 4)
        .reshape(GROUP, block_rows * rows, residues)
    )
    right_rows = (
        right_all.reshape(row_size, col_size, GROUP, rows, cols)
        .transpose(2, 0, 3, 1, 4)
        .reshape(GROUP, residues, residues)
    )
    triangle = jnp.einsum(
        "cik,cjk->cij", left_rows, right_rows, preferred_element_type=jnp.float32
    ).astype(jnp.bfloat16)
    triangle = (
        triangle.reshape(GROUP, block_rows, rows, col_size, cols)
        .transpose(1, 3, 0, 2, 4)
        .reshape(groups, GROUP, pairs)
    )
    owned = pl.pallas_call(
        functools.partial(return_kernel, sizes),
        out_shape=jax.ShapeDtypeStruct((groups, GROUP, pairs), jnp.bfloat16),
        in_specs=[anywhere],
        out_specs=anywhere,
        scratch_shapes=[
            pltpu.SemaphoreType.DMA,
            pltpu.SemaphoreType.DMA((groups,)),
            pltpu.SemaphoreType.DMA((groups,)),
        ],
        compiler_params=pltpu.CompilerParams(collective_id=1, has_side_effects=True),
    )(triangle)
    owned = owned.reshape(width, pairs)
    scaled = norm_axis(owned.astype(jnp.float32), 0).astype(jnp.bfloat16)
    projected = jnp.einsum("cp,ce->pe", scaled, w_out, preferred_element_type=jnp.float32)
    gate = jax.nn.sigmoid(
        jnp.einsum("pd,de->pe", flat_normed, w_out_gate, preferred_element_type=jnp.float32)
    )
    return (gate * projected).astype(jnp.bfloat16).reshape(rows, cols, width)


LANES = 128
QUAD = 4


def fused_kernel(sizes, shape, pair_in, tiles_in, *rest):
    weights_in, out = rest[:6], rest[6]
    (
        pair, tiles, weights, pair_sem, input_sem,
        normed, gate, left, right, left_all, right_all, left_mat, right_mat, left_lines, product, triangle, owned,
        send, left_recv, right_recv, back_recv,
    ) = rest[7:]
    row_size, col_size, groups = sizes
    rows, cols, width = shape
    devices = row_size * col_size
    block_rows = groups // col_size
    plane_size = groups // 2
    pairs = rows * cols
    spare = LANES - cols
    count = pairs // LANES
    extra = rows - count
    third = pairs // extra
    tile = rows * row_size // TILES
    row, col = lax.axis_index("row"), lax.axis_index("col")
    flat = row * col_size + col
    member = flat % groups
    block = flat // groups
    first = block * groups
    plane = flat // plane_size
    core = flat // col_size % 2
    moves = [bit * (1 - 2 * (flat // bit % 2)) for bit in (groups, plane_size, QUAD, 1)]

    def reach(flips, to_core):
        moved = sum(move for flip, move in zip(flips, moves) if flip)
        return flat + moved + col_size * (to_core - core)

    barrier = pltpu.get_barrier_semaphore()

    fetches = [[], []]
    for part in range(extra):
        for source, target in (
            (pair_in.at[part], pair.at[part, :, pl.ds(0, extra)]),
            (pair_in.at[extra, part], pair.at[part, :, extra]),
        ):
            fetches[0].append(pltpu.make_async_copy(source, target, pair_sem.at[part]))
    for index, source in enumerate(weights_in):
        fetches[1].append(pltpu.make_async_copy(source, weights.at[index], input_sem.at[0]))
    tile_fetch = pltpu.make_async_copy(tiles_in, tiles, input_sem.at[1])

    def all_of(ref, sem):
        return pltpu.make_async_copy(ref, ref, sem)

    with jax.named_scope("a0_begin"):
        tile_fetch.start()
        for fetch in fetches[0]:
            fetch.start()

        def signal(step, _):
            pl.semaphore_signal(
                barrier, inc=1, device_id=place((flat + step) % devices, col_size), device_id_type=MESH
            )
            return 0

        lax.fori_loop(1, devices, signal, 0)
        for fetch in fetches[1]:
            fetch.start()
        tile_fetch.wait()

    with jax.named_scope("a1_mask"):
        lane = lax.broadcasted_iota(jnp.int32, (GROUP, LANES), 1)
        low = lane < cols
        spot = lax.broadcasted_iota(jnp.int32, (TILES, LANES), 1)
        tile_low = lax.broadcasted_iota(jnp.int32, (TILES, LANES), 0) * tile
        direct = spot < cols
        masks = []
        turned_tiles = tiles[...].astype(jnp.float32).T
        for at in range(count):
            line = row * rows + jnp.where(direct, at, count + at // extra)
            within = col * cols + jnp.where(direct, spot, spot - cols + at % extra * spare)
            row_hot = ((line >= tile_low) & (line < tile_low + tile)).astype(jnp.float32)
            col_hot = ((within >= tile_low) & (within < tile_low + tile)).astype(jnp.float32)
            picked = jnp.dot(turned_tiles, row_hot, preferred_element_type=jnp.float32)
            masks.append(jnp.sum(picked * col_hot, axis=0, keepdims=True))
        mask = jnp.concatenate(masks, axis=1)

    with jax.named_scope("a2_ln"):
        for part in range(extra):
            all_of(pair.at[part], pair_sem.at[part]).wait()
            values = pair[part].reshape(third, width).astype(jnp.float32)
            normed[part * third : (part + 1) * third] = norm_axis(values, 1).astype(jnp.bfloat16)
        all_of(weights, input_sem.at[0]).wait()

    def project(index):
        turned = weights[index].astype(jnp.float32).T.astype(jnp.bfloat16)
        return lax.dot_general(
            turned, normed[...], (((1,), (1,)), ((), ())), preferred_element_type=jnp.float32
        )

    def factor(gate_index, index, target):
        made = jax.nn.sigmoid(project(gate_index)) * project(index) * mask
        for group in range(groups):
            target[group] = made[group * GROUP : (group + 1) * GROUP].astype(jnp.bfloat16)

    def copy_to(source, target, sent, received, to):
        pltpu.make_async_remote_copy(
            src_ref=source.at[to % groups],
            dst_ref=target,
            send_sem=sent,
            recv_sem=received,
            device_id=place(to, col_size),
            device_id_type=MESH,
        ).start()

    def send_right(to):
        copy_to(right, right_all.at[flat], send.at[0], right_recv.at[own_quad], to)

    def send_left(to):
        copy_to(left, left_all.at[member], send.at[1], left_recv.at[member // QUAD], to)

    def keep(source, target, received):
        return pltpu.make_async_copy(source.at[member], target, received)

    own_quad = flat // QUAD
    lows = ((1, 1), (0, 1), (1, 0), (0, 0))

    inner_flip = (plane % 2 + block) % 2
    to_inner = inner_flip * moves[1]
    to_outer = (1 - inner_flip) * moves[1]

    def send_across(to_core, shift):
        for low_flips in lows:
            send_right(reach((1, 0, *low_flips), to_core) + shift)

    with jax.named_scope("a3_right"):
        factor(2, 3, right)
    with jax.named_scope("a4_bar"):
        pl.semaphore_wait(barrier, devices - 1)
    with jax.named_scope("a5_send"):
        for low_flips in lows:
            send_right(reach((1, 0, *low_flips), 0))
            send_right(reach((0, 1, *low_flips), 1))
            send_right(reach((1, 1, *low_flips), 0))
    with jax.named_scope("a6_left"):
        factor(0, 1, left)
    with jax.named_scope("a7_send"):
        for low_flips in lows:
            for to_core in range(2):
                send_left(reach((0, 1, *low_flips), to_core))
        for low_flips in lows:
            send_right(reach((0, 0, *low_flips), 1 - core))
            send_left(reach((0, 0, *low_flips), 1 - core))
        for low_flips in lows[:-1]:
            send_right(reach((0, 0, *low_flips), core))
            send_left(reach((0, 0, *low_flips), core))
        for low_flips in lows:
            send_right(reach((0, 1, *low_flips), 0))
        send_across(1, to_inner)
        send_across(1, to_outer)
        keep(left, left_all.at[member], left_recv.at[member // QUAD]).start()
        keep(right, right_all.at[flat], right_recv.at[own_quad]).start()

    with jax.named_scope("b0_gate"):
        opened = jax.nn.sigmoid(
            jnp.dot(normed[...], weights[4], preferred_element_type=jnp.float32)
        )
        for at in range(count):
            middle = at * LANES + cols
            start = at % extra * spare
            gate[at] = opened[at * LANES : middle]
            gate[count + at // extra, start : start + spare] = opened[middle : middle + spare]

    def spread(chunk, target, half, start, clean):
        parts = [
            chunk[:, at : at + LANES].astype(jnp.float32) for at in range(0, pairs, LANES)
        ]
        lines = list(parts)
        for line in range(extra):
            base = line * extra
            made = pltpu.roll(parts[base], spare, 1)
            for piece in range(1, extra):
                moved = pltpu.roll(parts[base + piece], (piece + 1) * spare % LANES, 1)
                made = jnp.where(lane < piece * spare, made, moved)
            lines.append(made)
        for line, made in enumerate(lines):
            if clean:
                made = jnp.where(low, made, 0.0)
            target[half, pl.ds(pl.multiple_of((start + line) * GROUP, GROUP), GROUP), :] = made

    def place_right(source):
        spread(right_all[source], right_mat, source % col_size, source // col_size * rows, False)

    def place_left(source):
        spread(left_all[source], left_mat, source % col_size, source // col_size * rows, True)

    def each_of(start, length, do):
        def body(step, _):
            for index in range(QUAD):
                do(start + step * QUAD + index)
            return 0

        lax.fori_loop(0, length // QUAD, body, 0)

    quads = plane_size // QUAD

    def take(source_all, received, which, put):
        for step in range(quads):
            quad = which * quads + step
            all_of(source_all.at[pl.ds(quad * QUAD, QUAD)], received.at[quad]).wait()
            each_of(quad * QUAD, QUAD, put)

    block_lines = block_rows * rows

    def channel(target, index, start, count):
        first_line = pl.multiple_of(start * GROUP, GROUP) + index
        return jnp.concatenate(
            [
                target[half, pl.ds(first_line, count, stride=GROUP), :].astype(jnp.bfloat16)
                for half in range(col_size)
            ],
            axis=1,
        )

    part = cols // 2
    tiles_back = rows // 2 - 1

    def finish(which):
        half, side = which // 2, which % 2
        for index in range(GROUP):
            held = channel(right_mat, index, which * part, part)
            made = lax.dot_general(
                left_lines[index],
                jnp.concatenate([held, held, held[:spare]], axis=0),
                (((1,), (1,)), ((), ())),
                preferred_element_type=jnp.float32,
            )
            product[pl.ds(index, block_lines, stride=GROUP), :] = made

        def pack(part_row):
            to = part_row * col_size + half
            lines = [
                product[pl.ds(pl.multiple_of((part_row * rows + line) * GROUP, GROUP), GROUP), :]
                for line in range(rows)
            ]
            one, two = lines[rows - 2], lines[rows - 1]
            ends = [one, two]
            ends.append(
                jnp.where(
                    lane < LANES - spare // 2,
                    pltpu.roll(one, cols - spare, 1),
                    pltpu.roll(two, LANES - spare // 2 - part - spare, 1),
                )
            )
            for at in range(tiles_back):
                made = jnp.where(lane < part, lines[2 * at], lines[2 * at + 1])
                if at < len(ends):
                    made = jnp.where(low, made, ends[at])
                triangle[to, side, :, at * LANES : (at + 1) * LANES] = made.astype(jnp.bfloat16)

        def give(part_row):
            to = part_row * col_size + half

            @pl.when(to == member)
            def _():
                pltpu.make_async_copy(
                    triangle.at[to, side], owned.at[member, side], back_recv.at[0]
                ).start()

            @pl.when(to != member)
            def _():
                pltpu.make_async_remote_copy(
                    src_ref=triangle.at[to, side],
                    dst_ref=owned.at[member, side],
                    send_sem=send.at[2],
                    recv_sem=back_recv.at[0],
                    device_id=place(first + to, col_size),
                    device_id_type=MESH,
                ).start()

        def packs(step, _):
            for index in range(QUAD):
                pack(step * QUAD + index)
            for index in range(QUAD):
                give(step * QUAD + index)
            return 0

        lax.fori_loop(0, block_rows // QUAD, packs, 0)

    early = (block + 1 - core) % 2
    with jax.named_scope("b1_left"):
        take(left_all, left_recv, plane % 2, place_left)
    with jax.named_scope("b2_near"):
        take(right_all, right_recv, early * 2 + plane % 2, place_right)
    with jax.named_scope("b3_left"):
        take(left_all, left_recv, 1 - plane % 2, place_left)
    with jax.named_scope("b4_lines"):
        for index in range(GROUP):
            left_lines[index] = channel(left_mat, index, 0, block_lines)
    with jax.named_scope("c0_fin"):
        finish(early * 2 + plane % 2)
    with jax.named_scope("b5_far"):
        take(right_all, right_recv, early * 2 + 1 - plane % 2, place_right)
    with jax.named_scope("c1_fin"):
        finish(early * 2 + 1 - plane % 2)
    late = 1 - early
    with jax.named_scope("c2_near"):
        take(right_all, right_recv, late * 2 + plane % 2, place_right)
    with jax.named_scope("c3_fin"):
        finish(late * 2 + plane % 2)
    with jax.named_scope("c4_far"):
        take(right_all, right_recv, late * 2 + 1 - plane % 2, place_right)
    with jax.named_scope("c5_fin"):
        finish(late * 2 + 1 - plane % 2)
    with jax.named_scope("d0_back"):
        all_of(owned, back_recv.at[0]).wait()

    with jax.named_scope("d1_out"):
        for side, at in [(side, at) for side in range(2) for at in range(tiles_back)]:
            piece = jnp.concatenate(
                [
                    owned[group, side, :, at * LANES : (at + 1) * LANES].astype(jnp.float32)
                    for group in range(groups)
                ],
                axis=0,
            )
            scaled = norm_axis(piece, 0).T.astype(jnp.bfloat16)
            projected = jnp.dot(scaled, weights[5], preferred_element_type=jnp.float32)
            base = side * part
            spots = [(2 * at, base, 0, part), (2 * at + 1, base, part, part)]
            if at < 2:
                spots.append((rows - 2 + at, base, cols, spare))
            if at == 2:
                rest = part - spare
                spots.append((rows - 2, base + spare, cols, rest))
                spots.append((rows - 1, base + spare, cols + rest, rest))
            for line, start, begin, length in spots:
                stop = start + length
                made = gate[line, start:stop] * projected[begin : begin + length]
                out[line, start:stop] = made.astype(jnp.bfloat16)
    with jax.named_scope("d2_sent"):
        all_of(right_all.at[pl.ds(0, devices - 1)], send.at[0]).wait()
        all_of(left_all.at[pl.ds(0, groups - 1)], send.at[1]).wait()
        all_of(triangle.at[pl.ds(0, groups - 1)], send.at[2]).wait()


def fused(sizes, pair_act, tile_mask, *weights):
    row_size, col_size, groups = sizes
    devices = row_size * col_size
    block_rows = groups // col_size
    rows, cols, width = pair_act.shape
    pairs = rows * cols
    spare = LANES - cols
    extra = rows - pairs // LANES
    dma = pltpu.SemaphoreType.DMA
    chunks = pltpu.VMEM((groups, GROUP, pairs), jnp.bfloat16)
    parts = pltpu.VMEM((groups, 2, GROUP, (rows // 2 - 1) * LANES), jnp.bfloat16)
    result = pl.pallas_call(
        functools.partial(fused_kernel, sizes, pair_act.shape),
        out_shape=pltpu.VMEM((rows, cols, width), jnp.bfloat16),
        in_specs=[pl.BlockSpec(memory_space=pltpu.HBM)] * 8,
        out_specs=pl.BlockSpec(memory_space=pltpu.VMEM),
        scratch_shapes=[
            pltpu.VMEM((extra, extra, extra + 1, spare, width), jnp.bfloat16),
            pltpu.VMEM(tile_mask.shape, tile_mask.dtype),
            pltpu.VMEM((6, width, width), jnp.bfloat16),
            dma((extra,)),
            dma((2,)),
            pltpu.VMEM((pairs, width), jnp.bfloat16),
            pltpu.VMEM((rows, cols, width), jnp.float32),
            chunks,
            chunks,
            chunks,
            pltpu.VMEM((devices, GROUP, pairs), jnp.bfloat16),
            pltpu.VMEM((col_size, block_rows * rows * GROUP, LANES), jnp.float32),
            pltpu.VMEM((col_size, row_size * rows * GROUP, LANES), jnp.float32),
            pltpu.VMEM((GROUP, block_rows * rows, col_size * LANES), jnp.bfloat16),
            pltpu.VMEM((block_rows * rows * GROUP, LANES), jnp.float32),
            parts,
            parts,
            dma((3,)),
            dma((groups // QUAD,)),
            dma((devices // QUAD,)),
            dma((1,)),
        ],
        compiler_params=pltpu.CompilerParams(collective_id=2, has_side_effects=True),
    )(pair_act.reshape(extra + 1, extra, extra, spare, width), tile_mask, *weights)
    return result


def fits(sizes, rows, cols):
    row_size, col_size, groups = sizes
    pairs = rows * cols
    spare = LANES - cols
    extra = rows - pairs // LANES
    if (row_size, col_size, groups) != (16, 2, 16):
        return False
    if spare <= 0 or pairs % LANES or extra <= 0:
        return False
    part = cols // 2
    if 2 * part != cols or 2 * (part - spare) != spare or rows % 2:
        return False
    return rows == extra * (extra + 1) and cols == extra * spare


def solution(mesh):
    def whole(pair_act, tile_mask, *weights):
        groups = pair_act.shape[2] // GROUP
        sizes = (mesh.shape["row"], mesh.shape["col"], groups)
        rows, cols = (pair_act.shape[0] // sizes[0], pair_act.shape[1] // sizes[1])
        body = fused if fits(sizes, rows, cols) else local
        return jax.shard_map(
            functools.partial(body, sizes),
            mesh=mesh,
            in_specs=(P("row", "col", None), P(), P(), P(), P(), P(), P(), P()),
            out_specs=P("row", "col", None),
            check_vma=False,
        )(pair_act, tile_mask, *weights)

    return whole
```

```python
import functools

import jax
import jax.numpy as jnp
from jax import lax
from jax.experimental import pallas as pl
from jax.experimental.pallas import tpu as pltpu
from jax.sharding import PartitionSpec as P

TILES = 12
GROUP = 8
MESH = pl.DeviceIdType.MESH


def norm_axis(values, axis):
    mean = jnp.mean(values, axis=axis, keepdims=True)
    centred = values - mean
    spread = jnp.mean(centred * centred, axis=axis, keepdims=True)
    return centred * lax.rsqrt(spread + 1e-05)


def place(flat, col_size):
    return (flat // col_size, flat % col_size)


def greet(flat, first, count, col_size):
    barrier = pltpu.get_barrier_semaphore()

    def signal(step, _):
        other = first + (flat - first + step) % count
        pl.semaphore_signal(barrier, inc=1, device_id=place(other, col_size), device_id_type=MESH)
        return 0

    lax.fori_loop(1, count, signal, 0)
    pl.semaphore_wait(barrier, count - 1)


def spread_kernel(
    sizes, left, right, left_all, right_all, own_sem, left_send, left_recv, right_send, right_recv
):
    row_size, col_size, groups = sizes
    devices = row_size * col_size
    flat = lax.axis_index("row") * col_size + lax.axis_index("col")
    member = flat % groups
    first = flat - member

    def chunk(source, group):
        return source.at[group]

    own_left = pltpu.make_async_copy(chunk(left, member), left_all.at[member], own_sem.at[0])
    own_right = pltpu.make_async_copy(chunk(right, member), right_all.at[flat], own_sem.at[1])
    own_left.start()
    own_right.start()
    greet(flat, 0, devices, col_size)

    def right_copy(step):
        to = (flat + step) % devices
        return pltpu.make_async_remote_copy(
            src_ref=chunk(right, to % groups),
            dst_ref=right_all.at[flat],
            send_sem=right_send.at[step],
            recv_sem=right_recv.at[step],
            device_id=place(to, col_size),
            device_id_type=MESH,
        )

    def left_copy(step):
        to = (member + step) % groups
        return pltpu.make_async_remote_copy(
            src_ref=chunk(left, to),
            dst_ref=left_all.at[member],
            send_sem=left_send.at[step],
            recv_sem=left_recv.at[step],
            device_id=place(first + to, col_size),
            device_id_type=MESH,
        )

    def start_right(step, _):
        right_copy(step).start()
        return 0

    def start_left(step, _):
        left_copy(step).start()
        return 0

    def wait_right(step, _):
        right_copy(step).wait()
        return 0

    def wait_left(step, _):
        left_copy(step).wait()
        return 0

    lax.fori_loop(1, devices, start_right, 0)
    lax.fori_loop(1, groups, start_left, 0)
    own_left.wait()
    own_right.wait()
    lax.fori_loop(1, groups, wait_left, 0)
    lax.fori_loop(1, devices, wait_right, 0)


def return_kernel(sizes, triangle, owned, own_sem, send, recv):
    row_size, col_size, groups = sizes
    flat = lax.axis_index("row") * col_size + lax.axis_index("col")
    member = flat % groups
    first = flat - member
    own = pltpu.make_async_copy(triangle.at[member], owned.at[member], own_sem)
    own.start()
    greet(flat, first, groups, col_size)

    def copy(step):
        to = (member + step) % groups
        return pltpu.make_async_remote_copy(
            src_ref=triangle.at[to],
            dst_ref=owned.at[member],
            send_sem=send.at[step],
            recv_sem=recv.at[step],
            device_id=place(first + to, col_size),
            device_id_type=MESH,
        )

    def start(step, _):
        copy(step).start()
        return 0

    def wait(step, _):
        copy(step).wait()
        return 0

    lax.fori_loop(1, groups, start, 0)
    own.wait()
    lax.fori_loop(1, groups, wait, 0)


def local(
    sizes, pair_act, tile_mask, w_left_gate, w_left, w_right_gate, w_right, w_out_gate, w_out
):
    row_size, col_size, groups = sizes
    devices = row_size * col_size
    block_rows = groups // col_size
    rows, cols, width = pair_act.shape
    residues = rows * row_size
    tile = residues // TILES
    normed = norm_axis(pair_act.astype(jnp.float32), 2).astype(jnp.bfloat16)
    tile_range = lax.iota(jnp.int32, TILES)
    row_ids = (lax.axis_index("row") * rows + lax.iota(jnp.int32, rows)) // tile
    col_ids = (lax.axis_index("col") * cols + lax.iota(jnp.int32, cols)) // tile
    row_hot = (row_ids[:, None] == tile_range[None, :]).astype(jnp.float32)
    col_hot = (col_ids[:, None] == tile_range[None, :]).astype(jnp.float32)
    pair_mask = jnp.dot(
        jnp.dot(row_hot, tile_mask.astype(jnp.float32), preferred_element_type=jnp.float32),
        col_hot.T,
        preferred_element_type=jnp.float32,
    )
    pairs = rows * cols
    flat_normed = normed.reshape(pairs, width)
    flat_mask = pair_mask.reshape(1, pairs)

    def project(weight):
        return jnp.einsum("pd,de->ep", flat_normed, weight, preferred_element_type=jnp.float32)

    def factor(gate, value):
        out = jax.nn.sigmoid(project(gate)) * project(value) * flat_mask
        return out.astype(jnp.bfloat16).reshape(groups, GROUP, pairs)

    left = factor(w_left_gate, w_left)
    right = factor(w_right_gate, w_right)
    anywhere = pl.BlockSpec(memory_space=pl.ANY)
    left_all, right_all = pl.pallas_call(
        functools.partial(spread_kernel, sizes),
        out_shape=(
            jax.ShapeDtypeStruct((groups, GROUP, pairs), jnp.bfloat16),
            jax.ShapeDtypeStruct((devices, GROUP, pairs), jnp.bfloat16),
        ),
        in_specs=[anywhere] * 2,
        out_specs=(anywhere, anywhere),
        scratch_shapes=[
            pltpu.SemaphoreType.DMA((2,)),
            pltpu.SemaphoreType.DMA((groups,)),
            pltpu.SemaphoreType.DMA((groups,)),
            pltpu.SemaphoreType.DMA((devices,)),
            pltpu.SemaphoreType.DMA((devices,)),
        ],
        compiler_params=pltpu.CompilerParams(collective_id=0, has_side_effects=True),
    )(left, right)
    left_rows = (
        left_all.reshape(block_rows, col_size, GROUP, rows, cols)
        .transpose(2, 0, 3, 1, 4)
        .reshape(GROUP, block_rows * rows, residues)
    )
    right_rows = (
        right_all.reshape(row_size, col_size, GROUP, rows, cols)
        .transpose(2, 0, 3, 1, 4)
        .reshape(GROUP, residues, residues)
    )
    triangle = jnp.einsum(
        "cik,cjk->cij", left_rows, right_rows, preferred_element_type=jnp.float32
    ).astype(jnp.bfloat16)
    triangle = (
        triangle.reshape(GROUP, block_rows, rows, col_size, cols)
        .transpose(1, 3, 0, 2, 4)
        .reshape(groups, GROUP, pairs)
    )
    owned = pl.pallas_call(
        functools.partial(return_kernel, sizes),
        out_shape=jax.ShapeDtypeStruct((groups, GROUP, pairs), jnp.bfloat16),
        in_specs=[anywhere],
        out_specs=anywhere,
        scratch_shapes=[
            pltpu.SemaphoreType.DMA,
            pltpu.SemaphoreType.DMA((groups,)),
            pltpu.SemaphoreType.DMA((groups,)),
        ],
        compiler_params=pltpu.CompilerParams(collective_id=1, has_side_effects=True),
    )(triangle)
    owned = owned.reshape(width, pairs)
    scaled = norm_axis(owned.astype(jnp.float32), 0).astype(jnp.bfloat16)
    projected = jnp.einsum("cp,ce->pe", scaled, w_out, preferred_element_type=jnp.float32)
    gate = jax.nn.sigmoid(
        jnp.einsum("pd,de->pe", flat_normed, w_out_gate, preferred_element_type=jnp.float32)
    )
    return (gate * projected).astype(jnp.bfloat16).reshape(rows, cols, width)


LANES = 128
QUAD = 4


def fused_kernel(sizes, shape, pair_in, tiles_in, *rest):
    weights_in, out = rest[:6], rest[6]
    (
        pair, tiles, weights, pair_sem, input_sem,
        normed, gate, left, right, left_all, right_all, left_mat, right_mat, left_lines, product, triangle, owned,
        send, left_recv, right_recv, back_recv, heard,
    ) = rest[7:]
    row_size, col_size, groups = sizes
    rows, cols, width = shape
    devices = row_size * col_size
    block_rows = groups // col_size
    plane_size = groups // 2
    pairs = rows * cols
    spare = LANES - cols
    count = pairs // LANES
    extra = rows - count
    third = pairs // extra
    tile = rows * row_size // TILES
    row, col = lax.axis_index("row"), lax.axis_index("col")
    flat = row * col_size + col
    member = flat % groups
    block = flat // groups
    first = block * groups
    plane = flat // plane_size
    core = flat // col_size % 2
    moves = [bit * (1 - 2 * (flat // bit % 2)) for bit in (groups, plane_size, QUAD, 1)]

    def reach(flips, to_core):
        moved = sum(move for flip, move in zip(flips, moves) if flip)
        return flat + moved + col_size * (to_core - core)

    barrier = pltpu.get_barrier_semaphore()
    sides = ((1, 0), (0, 1))

    def tell(semaphore, to):
        pl.semaphore_signal(
            semaphore, inc=1, device_id=place(to, col_size), device_id_type=MESH
        )

    fetches = [[], []]
    for part in range(extra):
        for source, target in (
            (pair_in.at[part], pair.at[part, :, pl.ds(0, extra)]),
            (pair_in.at[extra, part], pair.at[part, :, extra]),
        ):
            fetches[0].append(pltpu.make_async_copy(source, target, pair_sem.at[part]))
    for index, source in enumerate(weights_in):
        fetches[1].append(pltpu.make_async_copy(source, weights.at[index], input_sem.at[0]))
    tile_fetch = pltpu.make_async_copy(tiles_in, tiles, input_sem.at[1])

    def all_of(ref, sem):
        return pltpu.make_async_copy(ref, ref, sem)

    with jax.named_scope("a0_begin"):
        tile_fetch.start()
        for fetch in fetches[0]:
            fetch.start()

        for flips in sides:
            tell(barrier, reach((0, 0, *flips), core))
        for flips in ((1, 1), (1, 0), (0, 1)):
            for to_core in range(2):
                tell(barrier, reach((*flips, 0, 0), to_core))
        tell(barrier, reach((0, 0, 0, 0), 1 - core))
        for fetch in fetches[1]:
            fetch.start()
        tile_fetch.wait()

    with jax.named_scope("a1_mask"):
        lane = lax.broadcasted_iota(jnp.int32, (GROUP, LANES), 1)
        low = lane < cols
        spot = lax.broadcasted_iota(jnp.int32, (TILES, LANES), 1)
        tile_low = lax.broadcasted_iota(jnp.int32, (TILES, LANES), 0) * tile
        direct = spot < cols
        masks = []
        turned_tiles = tiles[...].astype(jnp.float32).T
        for at in range(count):
            line = row * rows + jnp.where(direct, at, count + at // extra)
            within = col * cols + jnp.where(direct, spot, spot - cols + at % extra * spare)
            row_hot = ((line >= tile_low) & (line < tile_low + tile)).astype(jnp.float32)
            col_hot = ((within >= tile_low) & (within < tile_low + tile)).astype(jnp.float32)
            picked = jnp.dot(turned_tiles, row_hot, preferred_element_type=jnp.float32)
            masks.append(jnp.sum(picked * col_hot, axis=0, keepdims=True))
        mask = jnp.concatenate(masks, axis=1)

    with jax.named_scope("a2_ln"):
        for part in range(extra):
            all_of(pair.at[part], pair_sem.at[part]).wait()
            values = pair[part].reshape(third, width).astype(jnp.float32)
            normed[part * third : (part + 1) * third] = norm_axis(values, 1).astype(jnp.bfloat16)
        all_of(weights, input_sem.at[0]).wait()

    def project(index):
        turned = weights[index].astype(jnp.float32).T.astype(jnp.bfloat16)
        return lax.dot_general(
            turned, normed[...], (((1,), (1,)), ((), ())), preferred_element_type=jnp.float32
        )

    def factor(gate_index, index, target):
        made = jax.nn.sigmoid(project(gate_index)) * project(index) * mask
        for group in range(groups):
            target[group] = made[group * GROUP : (group + 1) * GROUP].astype(jnp.bfloat16)

    def copy_to(source, target, sent, received, to):
        pltpu.make_async_remote_copy(
            src_ref=source.at[to % groups],
            dst_ref=target,
            send_sem=sent,
            recv_sem=received,
            device_id=place(to, col_size),
            device_id_type=MESH,
        ).start()

    def send_right(to):
        copy_to(right, right_all.at[flat], send.at[0], right_recv.at[own_quad], to)

    def send_left(to):
        copy_to(left, left_all.at[member], send.at[1], left_recv.at[member // QUAD], to)

    def keep(source, target, received):
        return pltpu.make_async_copy(source.at[member], target, received)

    own_quad = flat // QUAD
    lows = ((1, 1), (0, 1), (1, 0), (0, 0))
    inner_flip = (plane % 2 + block) % 2
    to_inner = inner_flip * moves[1]
    to_outer = (1 - inner_flip) * moves[1]

    outer = (plane // 2 + plane + 1) % 2

    def send_across(low_flips, to_core, shift):
        send_right(reach((1, 0, *low_flips), to_core) + shift)

    def send_beside(low_flips, to_core):
        send_right(reach((0, 1, *low_flips), to_core))

    def send_early(low_flips):
        send_across(low_flips, 0, to_outer)
        send_beside(low_flips, 1)

        @pl.when(outer == 1)
        def _():
            send_beside(low_flips, 0)

    def send_lefts(low_flips):
        for to_core in range(2):
            send_left(reach((0, 1, *low_flips), to_core))

    with jax.named_scope("a3_right"):
        factor(2, 3, right)
    with jax.named_scope("a4_bar"):
        pl.semaphore_wait(barrier, 9)
        for index, flips in enumerate(sides):
            tell(heard.at[index], reach((0, 0, *flips), core))
    with jax.named_scope("a5_send"):
        send_early(lows[3])
    with jax.named_scope("a6_left"):
        factor(0, 1, left)
    with jax.named_scope("a7_send"):
        send_lefts(lows[3])
    with jax.named_scope("a8_hear"):
        pl.semaphore_wait(heard.at[0], 1)
        tell(heard.at[2], reach((0, 0, *sides[1]), core))
        pl.semaphore_wait(heard.at[1], 1)
    with jax.named_scope("a9_send"):
        for low_flips in lows[1:3]:
            send_early(low_flips)
            send_lefts(low_flips)
    with jax.named_scope("a91_hear"):
        pl.semaphore_wait(heard.at[2], 1)
    with jax.named_scope("a92_send"):
        send_early(lows[0])
        send_lefts(lows[0])
        for low_flips in lows:
            send_right(reach((0, 0, *low_flips), 1 - core))
            send_left(reach((0, 0, *low_flips), 1 - core))
        for low_flips in lows[:-1]:
            send_right(reach((0, 0, *low_flips), core))
            send_left(reach((0, 0, *low_flips), core))

        @pl.when(outer == 0)
        def _():
            for low_flips in lows:
                send_beside(low_flips, 0)

        for low_flips in lows:
            send_across(low_flips, 1, to_outer)
        for low_flips in lows:
            send_across(low_flips, 0, to_inner)
            send_across(low_flips, 1, to_inner)
        keep(left, left_all.at[member], left_recv.at[member // QUAD]).start()
        keep(right, right_all.at[flat], right_recv.at[own_quad]).start()

    with jax.named_scope("b0_gate"):
        opened = jax.nn.sigmoid(
            jnp.dot(normed[...], weights[4], preferred_element_type=jnp.float32)
        )
        for at in range(count):
            middle = at * LANES + cols
            start = at % extra * spare
            gate[at] = opened[at * LANES : middle]
            gate[count + at // extra, start : start + spare] = opened[middle : middle + spare]

    def spread(chunk, target, half, start, clean):
        parts = [
            chunk[:, at : at + LANES].astype(jnp.float32) for at in range(0, pairs, LANES)
        ]
        lines = list(parts)
        for line in range(extra):
            base = line * extra
            made = pltpu.roll(parts[base], spare, 1)
            for piece in range(1, extra):
                moved = pltpu.roll(parts[base + piece], (piece + 1) * spare % LANES, 1)
                made = jnp.where(lane < piece * spare, made, moved)
            lines.append(made)
        for line, made in enumerate(lines):
            if clean:
                made = jnp.where(low, made, 0.0)
            target[half, pl.ds(pl.multiple_of((start + line) * GROUP, GROUP), GROUP), :] = made

    def place_right(source):
        spread(right_all[source], right_mat, source % col_size, source // col_size * rows, False)

    def place_left(source):
        spread(left_all[source], left_mat, source % col_size, source // col_size * rows, True)

    def each_of(start, length, do):
        def body(step, _):
            for index in range(QUAD):
                do(start + step * QUAD + index)
            return 0

        lax.fori_loop(0, length // QUAD, body, 0)

    quads = plane_size // QUAD

    def take(source_all, received, which, put):
        for step in range(quads):
            quad = which * quads + step
            all_of(source_all.at[pl.ds(quad * QUAD, QUAD)], received.at[quad]).wait()
            each_of(quad * QUAD, QUAD, put)

    block_lines = block_rows * rows

    def channel(target, index, start, count):
        first_line = pl.multiple_of(start * GROUP, GROUP) + index
        return jnp.concatenate(
            [
                target[half, pl.ds(first_line, count, stride=GROUP), :].astype(jnp.bfloat16)
                for half in range(col_size)
            ],
            axis=1,
        )

    part = cols // 2
    tiles_back = rows // 2 - 1

    def finish(which):
        half, side = which // 2, which % 2
        for index in range(GROUP):
            held = channel(right_mat, index, which * part, part)
            made = lax.dot_general(
                left_lines[index],
                jnp.concatenate([held, held, held[:spare]], axis=0),
                (((1,), (1,)), ((), ())),
                preferred_element_type=jnp.float32,
            )
            product[pl.ds(index, block_lines, stride=GROUP), :] = made

        def pack(part_row):
            to = part_row * col_size + half
            lines = [
                product[pl.ds(pl.multiple_of((part_row * rows + line) * GROUP, GROUP), GROUP), :]
                for line in range(rows)
            ]
            one, two = lines[rows - 2], lines[rows - 1]
            ends = [one, two]
            ends.append(
                jnp.where(
                    lane < LANES - spare // 2,
                    pltpu.roll(one, cols - spare, 1),
                    pltpu.roll(two, LANES - spare // 2 - part - spare, 1),
                )
            )
            for at in range(tiles_back):
                made = jnp.where(lane < part, lines[2 * at], lines[2 * at + 1])
                if at < len(ends):
                    made = jnp.where(low, made, ends[at])
                triangle[to, side, :, at * LANES : (at + 1) * LANES] = made.astype(jnp.bfloat16)

        def give(part_row):
            to = part_row * col_size + half

            @pl.when(to == member)
            def _():
                pltpu.make_async_copy(
                    triangle.at[to, side], owned.at[member, side], back_recv.at[0]
                ).start()

            @pl.when(to != member)
            def _():
                pltpu.make_async_remote_copy(
                    src_ref=triangle.at[to, side],
                    dst_ref=owned.at[member, side],
                    send_sem=send.at[2],
                    recv_sem=back_recv.at[0],
                    device_id=place(first + to, col_size),
                    device_id_type=MESH,
                ).start()

        def packs(step, _):
            for index in range(QUAD):
                pack(step * QUAD + index)
            for index in range(QUAD):
                give(step * QUAD + index)
            return 0

        lax.fori_loop(0, block_rows // QUAD, packs, 0)

    early = (block + outer * (1 - core)) % 2
    with jax.named_scope("b1_left"):
        take(left_all, left_recv, plane % 2, place_left)
    with jax.named_scope("b2_near"):
        take(right_all, right_recv, early * 2 + plane % 2, place_right)
    with jax.named_scope("b3_left"):
        take(left_all, left_recv, 1 - plane % 2, place_left)
    with jax.named_scope("b4_lines"):
        for index in range(GROUP):
            left_lines[index] = channel(left_mat, index, 0, block_lines)
    with jax.named_scope("c0_fin"):
        finish(early * 2 + plane % 2)
    with jax.named_scope("b5_far"):
        take(right_all, right_recv, early * 2 + 1 - plane % 2, place_right)
    with jax.named_scope("c1_fin"):
        finish(early * 2 + 1 - plane % 2)
    late = 1 - early
    with jax.named_scope("c2_near"):
        take(right_all, right_recv, late * 2 + plane % 2, place_right)
    with jax.named_scope("c3_fin"):
        finish(late * 2 + plane % 2)
    with jax.named_scope("c4_far"):
        take(right_all, right_recv, late * 2 + 1 - plane % 2, place_right)
    with jax.named_scope("c5_fin"):
        finish(late * 2 + 1 - plane % 2)
    with jax.named_scope("d0_back"):
        all_of(owned, back_recv.at[0]).wait()

    with jax.named_scope("d1_out"):
        for side, at in [(side, at) for side in range(2) for at in range(tiles_back)]:
            piece = jnp.concatenate(
                [
                    owned[group, side, :, at * LANES : (at + 1) * LANES].astype(jnp.float32)
                    for group in range(groups)
                ],
                axis=0,
            )
            scaled = norm_axis(piece, 0).T.astype(jnp.bfloat16)
            projected = jnp.dot(scaled, weights[5], preferred_element_type=jnp.float32)
            base = side * part
            spots = [(2 * at, base, 0, part), (2 * at + 1, base, part, part)]
            if at < 2:
                spots.append((rows - 2 + at, base, cols, spare))
            if at == 2:
                rest = part - spare
                spots.append((rows - 2, base + spare, cols, rest))
                spots.append((rows - 1, base + spare, cols + rest, rest))
            for line, start, begin, length in spots:
                stop = start + length
                made = gate[line, start:stop] * projected[begin : begin + length]
                out[line, start:stop] = made.astype(jnp.bfloat16)
    with jax.named_scope("d2_sent"):
        all_of(right_all.at[pl.ds(0, devices - 1)], send.at[0]).wait()
        all_of(left_all.at[pl.ds(0, groups - 1)], send.at[1]).wait()
        all_of(triangle.at[pl.ds(0, groups - 1)], send.at[2]).wait()


def fused(sizes, pair_act, tile_mask, *weights):
    row_size, col_size, groups = sizes
    devices = row_size * col_size
    block_rows = groups // col_size
    rows, cols, width = pair_act.shape
    pairs = rows * cols
    spare = LANES - cols
    extra = rows - pairs // LANES
    dma = pltpu.SemaphoreType.DMA
    chunks = pltpu.VMEM((groups, GROUP, pairs), jnp.bfloat16)
    parts = pltpu.VMEM((groups, 2, GROUP, (rows // 2 - 1) * LANES), jnp.bfloat16)
    result = pl.pallas_call(
        functools.partial(fused_kernel, sizes, pair_act.shape),
        out_shape=pltpu.VMEM((rows, cols, width), jnp.bfloat16),
        in_specs=[pl.BlockSpec(memory_space=pltpu.HBM)] * 8,
        out_specs=pl.BlockSpec(memory_space=pltpu.VMEM),
        scratch_shapes=[
            pltpu.VMEM((extra, extra, extra + 1, spare, width), jnp.bfloat16),
            pltpu.VMEM(tile_mask.shape, tile_mask.dtype),
            pltpu.VMEM((6, width, width), jnp.bfloat16),
            dma((extra,)),
            dma((2,)),
            pltpu.VMEM((pairs, width), jnp.bfloat16),
            pltpu.VMEM((rows, cols, width), jnp.float32),
            chunks,
            chunks,
            chunks,
            pltpu.VMEM((devices, GROUP, pairs), jnp.bfloat16),
            pltpu.VMEM((col_size, block_rows * rows * GROUP, LANES), jnp.float32),
            pltpu.VMEM((col_size, row_size * rows * GROUP, LANES), jnp.float32),
            pltpu.VMEM((GROUP, block_rows * rows, col_size * LANES), jnp.bfloat16),
            pltpu.VMEM((block_rows * rows * GROUP, LANES), jnp.float32),
            parts,
            parts,
            dma((3,)),
            dma((groups // QUAD,)),
            dma((devices // QUAD,)),
            dma((1,)),
            pltpu.SemaphoreType.REGULAR((3,)),
        ],
        compiler_params=pltpu.CompilerParams(collective_id=2, has_side_effects=True),
    )(pair_act.reshape(extra + 1, extra, extra, spare, width), tile_mask, *weights)
    return result


def fits(sizes, rows, cols):
    row_size, col_size, groups = sizes
    pairs = rows * cols
    spare = LANES - cols
    extra = rows - pairs // LANES
    if (row_size, col_size, groups) != (16, 2, 16):
        return False
    if spare <= 0 or pairs % LANES or extra <= 0:
        return False
    part = cols // 2
    if 2 * part != cols or 2 * (part - spare) != spare or rows % 2:
        return False
    return rows == extra * (extra + 1) and cols == extra * spare


def solution(mesh):
    def whole(pair_act, tile_mask, *weights):
        groups = pair_act.shape[2] // GROUP
        sizes = (mesh.shape["row"], mesh.shape["col"], groups)
        rows, cols = (pair_act.shape[0] // sizes[0], pair_act.shape[1] // sizes[1])
        body = fused if fits(sizes, rows, cols) else local
        return jax.shard_map(
            functools.partial(body, sizes),
            mesh=mesh,
            in_specs=(P("row", "col", None), P(), P(), P(), P(), P(), P(), P()),
            out_specs=P("row", "col", None),
            check_vma=False,
        )(pair_act, tile_mask, *weights)

    return whole
```

```python
import functools

import jax
import jax.numpy as jnp
from jax import lax
from jax.experimental import pallas as pl
from jax.experimental.pallas import tpu as pltpu
from jax.sharding import PartitionSpec as P

TILES = 12
GROUP = 8
MESH = pl.DeviceIdType.MESH


def norm_axis(values, axis):
    mean = jnp.mean(values, axis=axis, keepdims=True)
    centred = values - mean
    spread = jnp.mean(centred * centred, axis=axis, keepdims=True)
    return centred * lax.rsqrt(spread + 1e-05)


def place(flat, col_size):
    return (flat // col_size, flat % col_size)


def greet(flat, first, count, col_size):
    barrier = pltpu.get_barrier_semaphore()

    def signal(step, _):
        other = first + (flat - first + step) % count
        pl.semaphore_signal(barrier, inc=1, device_id=place(other, col_size), device_id_type=MESH)
        return 0

    lax.fori_loop(1, count, signal, 0)
    pl.semaphore_wait(barrier, count - 1)


def spread_kernel(
    sizes, left, right, left_all, right_all, own_sem, left_send, left_recv, right_send, right_recv
):
    row_size, col_size, groups = sizes
    devices = row_size * col_size
    flat = lax.axis_index("row") * col_size + lax.axis_index("col")
    member = flat % groups
    first = flat - member

    def chunk(source, group):
        return source.at[group]

    own_left = pltpu.make_async_copy(chunk(left, member), left_all.at[member], own_sem.at[0])
    own_right = pltpu.make_async_copy(chunk(right, member), right_all.at[flat], own_sem.at[1])
    own_left.start()
    own_right.start()
    greet(flat, 0, devices, col_size)

    def right_copy(step):
        to = (flat + step) % devices
        return pltpu.make_async_remote_copy(
            src_ref=chunk(right, to % groups),
            dst_ref=right_all.at[flat],
            send_sem=right_send.at[step],
            recv_sem=right_recv.at[step],
            device_id=place(to, col_size),
            device_id_type=MESH,
        )

    def left_copy(step):
        to = (member + step) % groups
        return pltpu.make_async_remote_copy(
            src_ref=chunk(left, to),
            dst_ref=left_all.at[member],
            send_sem=left_send.at[step],
            recv_sem=left_recv.at[step],
            device_id=place(first + to, col_size),
            device_id_type=MESH,
        )

    def start_right(step, _):
        right_copy(step).start()
        return 0

    def start_left(step, _):
        left_copy(step).start()
        return 0

    def wait_right(step, _):
        right_copy(step).wait()
        return 0

    def wait_left(step, _):
        left_copy(step).wait()
        return 0

    lax.fori_loop(1, devices, start_right, 0)
    lax.fori_loop(1, groups, start_left, 0)
    own_left.wait()
    own_right.wait()
    lax.fori_loop(1, groups, wait_left, 0)
    lax.fori_loop(1, devices, wait_right, 0)


def return_kernel(sizes, triangle, owned, own_sem, send, recv):
    row_size, col_size, groups = sizes
    flat = lax.axis_index("row") * col_size + lax.axis_index("col")
    member = flat % groups
    first = flat - member
    own = pltpu.make_async_copy(triangle.at[member], owned.at[member], own_sem)
    own.start()
    greet(flat, first, groups, col_size)

    def copy(step):
        to = (member + step) % groups
        return pltpu.make_async_remote_copy(
            src_ref=triangle.at[to],
            dst_ref=owned.at[member],
            send_sem=send.at[step],
            recv_sem=recv.at[step],
            device_id=place(first + to, col_size),
            device_id_type=MESH,
        )

    def start(step, _):
        copy(step).start()
        return 0

    def wait(step, _):
        copy(step).wait()
        return 0

    lax.fori_loop(1, groups, start, 0)
    own.wait()
    lax.fori_loop(1, groups, wait, 0)


def local(
    sizes, pair_act, tile_mask, w_left_gate, w_left, w_right_gate, w_right, w_out_gate, w_out
):
    row_size, col_size, groups = sizes
    devices = row_size * col_size
    block_rows = groups // col_size
    rows, cols, width = pair_act.shape
    residues = rows * row_size
    tile = residues // TILES
    normed = norm_axis(pair_act.astype(jnp.float32), 2).astype(jnp.bfloat16)
    tile_range = lax.iota(jnp.int32, TILES)
    row_ids = (lax.axis_index("row") * rows + lax.iota(jnp.int32, rows)) // tile
    col_ids = (lax.axis_index("col") * cols + lax.iota(jnp.int32, cols)) // tile
    row_hot = (row_ids[:, None] == tile_range[None, :]).astype(jnp.float32)
    col_hot = (col_ids[:, None] == tile_range[None, :]).astype(jnp.float32)
    pair_mask = jnp.dot(
        jnp.dot(row_hot, tile_mask.astype(jnp.float32), preferred_element_type=jnp.float32),
        col_hot.T,
        preferred_element_type=jnp.float32,
    )
    pairs = rows * cols
    flat_normed = normed.reshape(pairs, width)
    flat_mask = pair_mask.reshape(1, pairs)

    def project(weight):
        return jnp.einsum("pd,de->ep", flat_normed, weight, preferred_element_type=jnp.float32)

    def factor(gate, value):
        out = jax.nn.sigmoid(project(gate)) * project(value) * flat_mask
        return out.astype(jnp.bfloat16).reshape(groups, GROUP, pairs)

    left = factor(w_left_gate, w_left)
    right = factor(w_right_gate, w_right)
    anywhere = pl.BlockSpec(memory_space=pl.ANY)
    left_all, right_all = pl.pallas_call(
        functools.partial(spread_kernel, sizes),
        out_shape=(
            jax.ShapeDtypeStruct((groups, GROUP, pairs), jnp.bfloat16),
            jax.ShapeDtypeStruct((devices, GROUP, pairs), jnp.bfloat16),
        ),
        in_specs=[anywhere] * 2,
        out_specs=(anywhere, anywhere),
        scratch_shapes=[
            pltpu.SemaphoreType.DMA((2,)),
            pltpu.SemaphoreType.DMA((groups,)),
            pltpu.SemaphoreType.DMA((groups,)),
            pltpu.SemaphoreType.DMA((devices,)),
            pltpu.SemaphoreType.DMA((devices,)),
        ],
        compiler_params=pltpu.CompilerParams(collective_id=0, has_side_effects=True),
    )(left, right)
    left_rows = (
        left_all.reshape(block_rows, col_size, GROUP, rows, cols)
        .transpose(2, 0, 3, 1, 4)
        .reshape(GROUP, block_rows * rows, residues)
    )
    right_rows = (
        right_all.reshape(row_size, col_size, GROUP, rows, cols)
        .transpose(2, 0, 3, 1, 4)
        .reshape(GROUP, residues, residues)
    )
    triangle = jnp.einsum(
        "cik,cjk->cij", left_rows, right_rows, preferred_element_type=jnp.float32
    ).astype(jnp.bfloat16)
    triangle = (
        triangle.reshape(GROUP, block_rows, rows, col_size, cols)
        .transpose(1, 3, 0, 2, 4)
        .reshape(groups, GROUP, pairs)
    )
    owned = pl.pallas_call(
        functools.partial(return_kernel, sizes),
        out_shape=jax.ShapeDtypeStruct((groups, GROUP, pairs), jnp.bfloat16),
        in_specs=[anywhere],
        out_specs=anywhere,
        scratch_shapes=[
            pltpu.SemaphoreType.DMA,
            pltpu.SemaphoreType.DMA((groups,)),
            pltpu.SemaphoreType.DMA((groups,)),
        ],
        compiler_params=pltpu.CompilerParams(collective_id=1, has_side_effects=True),
    )(triangle)
    owned = owned.reshape(width, pairs)
    scaled = norm_axis(owned.astype(jnp.float32), 0).astype(jnp.bfloat16)
    projected = jnp.einsum("cp,ce->pe", scaled, w_out, preferred_element_type=jnp.float32)
    gate = jax.nn.sigmoid(
        jnp.einsum("pd,de->pe", flat_normed, w_out_gate, preferred_element_type=jnp.float32)
    )
    return (gate * projected).astype(jnp.bfloat16).reshape(rows, cols, width)


LANES = 128
QUAD = 4


def fused_kernel(sizes, shape, pair_in, tiles_in, *rest):
    weights_in, out = rest[:6], rest[6]
    (
        pair, tiles, weights, pair_sem, input_sem,
        normed, gate, left, right, left_all, right_all, left_mat, right_mat, left_lines, product, triangle, owned,
        send, left_recv, right_recv, back_recv, heard,
    ) = rest[7:]
    row_size, col_size, groups = sizes
    rows, cols, width = shape
    devices = row_size * col_size
    block_rows = groups // col_size
    plane_size = groups // 2
    pairs = rows * cols
    spare = LANES - cols
    count = pairs // LANES
    extra = rows - count
    tile = rows * row_size // TILES
    row, col = lax.axis_index("row"), lax.axis_index("col")
    flat = row * col_size + col
    member = flat % groups
    block = flat // groups
    first = block * groups
    plane = flat // plane_size
    core = flat // col_size % 2
    moves = [bit * (1 - 2 * (flat // bit % 2)) for bit in (groups, plane_size, QUAD, 1)]

    def reach(flips, to_core):
        moved = sum(move for flip, move in zip(flips, moves) if flip)
        return flat + moved + col_size * (to_core - core)

    barrier = pltpu.get_barrier_semaphore()
    sides = ((1, 0), (0, 1))

    def tell(semaphore, to):
        pl.semaphore_signal(
            semaphore, inc=1, device_id=place(to, col_size), device_id_type=MESH
        )

    fetches = [[], []]
    for part in range(extra):
        for source, target in (
            (pair_in.at[part], pair.at[part, :, pl.ds(0, extra)]),
            (pair_in.at[extra, part], pair.at[part, :, extra]),
        ):
            fetches[0].append(pltpu.make_async_copy(source, target, pair_sem.at[0]))
    for index, source in enumerate(weights_in):
        fetches[1].append(pltpu.make_async_copy(source, weights.at[index], input_sem.at[0]))
    tile_fetch = pltpu.make_async_copy(tiles_in, tiles, input_sem.at[1])

    def all_of(ref, sem):
        return pltpu.make_async_copy(ref, ref, sem)

    with jax.named_scope("a0_begin"):
        tile_fetch.start()
        for fetch in fetches[0]:
            fetch.start()

        for flips in sides:
            tell(barrier, reach((0, 0, *flips), core))
        for flips in ((1, 1), (1, 0), (0, 1)):
            for to_core in range(2):
                tell(barrier, reach((*flips, 0, 0), to_core))
        tell(barrier, reach((0, 0, 0, 0), 1 - core))
        for fetch in fetches[1]:
            fetch.start()
        tile_fetch.wait()
        all_of(pair, pair_sem.at[0]).wait()

    with jax.named_scope("a1_mask"):
        lane = lax.broadcasted_iota(jnp.int32, (GROUP, LANES), 1)
        low = lane < cols
        spot = lax.broadcasted_iota(jnp.int32, (TILES, LANES), 1)
        tile_low = lax.broadcasted_iota(jnp.int32, (TILES, LANES), 0) * tile
        direct = spot < cols
        masks = []
        turned_tiles = tiles[...].astype(jnp.float32).T
        for at in range(count):
            line = row * rows + jnp.where(direct, at, count + at // extra)
            within = col * cols + jnp.where(direct, spot, spot - cols + at % extra * spare)
            row_hot = ((line >= tile_low) & (line < tile_low + tile)).astype(jnp.float32)
            col_hot = ((within >= tile_low) & (within < tile_low + tile)).astype(jnp.float32)
            picked = jnp.dot(turned_tiles, row_hot, preferred_element_type=jnp.float32)
            masks.append(jnp.sum(picked * col_hot, axis=0, keepdims=True))
        mask = jnp.concatenate(masks, axis=1)

    with jax.named_scope("a2_ln"):
        values = pair[...].reshape(pairs, width).astype(jnp.float32)
        normed[...] = norm_axis(values, 1).astype(jnp.bfloat16)
        all_of(weights, input_sem.at[0]).wait()

    def project(index):
        turned = weights[index].astype(jnp.float32).T.astype(jnp.bfloat16)
        return lax.dot_general(
            turned, normed[...], (((1,), (1,)), ((), ())), preferred_element_type=jnp.float32
        )

    def factor(gate_index, index, target):
        made = jax.nn.sigmoid(project(gate_index)) * project(index) * mask
        for group in range(groups):
            target[group] = made[group * GROUP : (group + 1) * GROUP].astype(jnp.bfloat16)

    def copy_to(source, target, sent, received, to):
        pltpu.make_async_remote_copy(
            src_ref=source.at[to % groups],
            dst_ref=target,
            send_sem=sent,
            recv_sem=received,
            device_id=place(to, col_size),
            device_id_type=MESH,
        ).start()

    def send_right(to):
        copy_to(right, right_all.at[flat], send.at[0], right_recv.at[own_quad], to)

    def send_left(to):
        copy_to(left, left_all.at[member], send.at[1], left_recv.at[member // QUAD], to)

    def keep(source, target, received):
        return pltpu.make_async_copy(source.at[member], target, received)

    own_quad = flat // QUAD
    lows = ((1, 1), (0, 1), (1, 0), (0, 0))
    inner_flip = (plane % 2 + block) % 2
    to_inner = inner_flip * moves[1]
    to_outer = (1 - inner_flip) * moves[1]

    outer = (plane // 2 + plane + 1) % 2

    def send_across(low_flips, to_core, shift):
        send_right(reach((1, 0, *low_flips), to_core) + shift)

    def send_beside(low_flips, to_core):
        send_right(reach((0, 1, *low_flips), to_core))

    def send_early(low_flips):
        send_across(low_flips, 1, to_inner)
        send_across(low_flips, 0, to_outer)

    def send_besides(low_flips):
        send_beside(low_flips, 0)
        send_beside(low_flips, 1)

    def send_lefts(low_flips):
        for to_core in range(2):
            send_left(reach((0, 1, *low_flips), to_core))

    with jax.named_scope("a3_right"):
        factor(2, 3, right)
    with jax.named_scope("a4_bar"):
        pl.semaphore_wait(barrier, 9)
        for index, flips in enumerate(sides):
            tell(heard.at[index], reach((0, 0, *flips), core))
    with jax.named_scope("a5_send"):

        @pl.when(outer == 1)
        def _():
            send_besides(lows[3])

        @pl.when(outer == 0)
        def _():
            send_early(lows[3])

    with jax.named_scope("a6_left"):
        factor(0, 1, left)
    with jax.named_scope("a7_send"):
        send_lefts(lows[3])

        @pl.when(outer == 1)
        def _():
            send_early(lows[3])

    def send_mixed(low_flips):
        @pl.when(outer == 1)
        def _():
            send_lefts(low_flips)
            send_besides(low_flips)
            send_early(low_flips)

        @pl.when(outer == 0)
        def _():
            send_early(low_flips)
            send_lefts(low_flips)

    def hear(index):
        pl.semaphore_wait(heard.at[index], 1)
        if index == 0:
            tell(heard.at[2], reach((0, 0, *sides[1]), core))
        send_mixed(sides[index])

    with jax.named_scope("a8_hear"):

        @pl.when(col == 0)
        def _():
            hear(0)
            hear(1)

        @pl.when(col != 0)
        def _():
            hear(1)
            hear(0)

    with jax.named_scope("a91_hear"):
        pl.semaphore_wait(heard.at[2], 1)
    with jax.named_scope("a92_send"):
        send_mixed(lows[0])
        for low_flips in lows:
            send_right(reach((0, 0, *low_flips), 1 - core))
            send_left(reach((0, 0, *low_flips), 1 - core))
        for low_flips in lows[:-1]:
            send_right(reach((0, 0, *low_flips), core))
            send_left(reach((0, 0, *low_flips), core))

        @pl.when(outer == 0)
        def _():
            for low_flips in lows:
                send_beside(low_flips, 0)
            for low_flips in lows:
                send_beside(low_flips, 1)

        for low_flips in lows:
            send_across(low_flips, 0, to_inner)
            send_across(low_flips, 1, to_outer)
        keep(left, left_all.at[member], left_recv.at[member // QUAD]).start()
        keep(right, right_all.at[flat], right_recv.at[own_quad]).start()

    with jax.named_scope("b0_gate"):
        opened = jax.nn.sigmoid(
            jnp.dot(normed[...], weights[4], preferred_element_type=jnp.float32)
        )
        for at in range(count):
            middle = at * LANES + cols
            start = at % extra * spare
            gate[at] = opened[at * LANES : middle]
            gate[count + at // extra, start : start + spare] = opened[middle : middle + spare]

    def spread(chunk, target, half, start, clean):
        parts = [
            chunk[:, at : at + LANES].astype(jnp.float32) for at in range(0, pairs, LANES)
        ]
        lines = list(parts)
        for line in range(extra):
            base = line * extra
            made = pltpu.roll(parts[base], spare, 1)
            for piece in range(1, extra):
                moved = pltpu.roll(parts[base + piece], (piece + 1) * spare % LANES, 1)
                made = jnp.where(lane < piece * spare, made, moved)
            lines.append(made)
        for line, made in enumerate(lines):
            if clean:
                made = jnp.where(low, made, 0.0)
            target[half, pl.ds(pl.multiple_of((start + line) * GROUP, GROUP), GROUP), :] = made

    def place_right(source):
        spread(right_all[source], right_mat, source % col_size, source // col_size * rows, False)

    def place_left(source):
        spread(left_all[source], left_mat, source % col_size, source // col_size * rows, True)

    def each_of(start, length, do):
        def body(step, _):
            for index in range(QUAD):
                do(start + step * QUAD + index)
            return 0

        lax.fori_loop(0, length // QUAD, body, 0)

    quads = plane_size // QUAD

    def take(source_all, received, which, put):
        for step in range(quads):
            quad = which * quads + step
            all_of(source_all.at[pl.ds(quad * QUAD, QUAD)], received.at[quad]).wait()
            each_of(quad * QUAD, QUAD, put)

    block_lines = block_rows * rows

    def channel(target, index, start, count):
        first_line = pl.multiple_of(start * GROUP, GROUP) + index
        return jnp.concatenate(
            [
                target[half, pl.ds(first_line, count, stride=GROUP), :].astype(jnp.bfloat16)
                for half in range(col_size)
            ],
            axis=1,
        )

    part = cols // 2
    tiles_back = rows // 2 - 1

    def finish(which):
        half, side = which // 2, which % 2
        for index in range(GROUP):
            held = channel(right_mat, index, which * part, part)
            made = lax.dot_general(
                left_lines[index],
                jnp.concatenate([held, held, held[:spare]], axis=0),
                (((1,), (1,)), ((), ())),
                preferred_element_type=jnp.float32,
            )
            product[pl.ds(index, block_lines, stride=GROUP), :] = made

        def pack(part_row):
            to = part_row * col_size + half
            lines = [
                product[pl.ds(pl.multiple_of((part_row * rows + line) * GROUP, GROUP), GROUP), :]
                for line in range(rows)
            ]
            one, two = lines[rows - 2], lines[rows - 1]
            ends = [one, two]
            ends.append(
                jnp.where(
                    lane < LANES - spare // 2,
                    pltpu.roll(one, cols - spare, 1),
                    pltpu.roll(two, LANES - spare // 2 - part - spare, 1),
                )
            )
            for at in range(tiles_back):
                made = jnp.where(lane < part, lines[2 * at], lines[2 * at + 1])
                if at < len(ends):
                    made = jnp.where(low, made, ends[at])
                triangle[to, side, :, at * LANES : (at + 1) * LANES] = made.astype(jnp.bfloat16)

        def give(part_row):
            to = part_row * col_size + half

            @pl.when(to == member)
            def _():
                pltpu.make_async_copy(
                    triangle.at[to, side], owned.at[member, side], back_recv.at[0]
                ).start()

            @pl.when(to != member)
            def _():
                pltpu.make_async_remote_copy(
                    src_ref=triangle.at[to, side],
                    dst_ref=owned.at[member, side],
                    send_sem=send.at[2],
                    recv_sem=back_recv.at[0],
                    device_id=place(first + to, col_size),
                    device_id_type=MESH,
                ).start()

        def packs(step, _):
            for index in range(QUAD):
                pack(step * QUAD + index)
            for index in range(QUAD):
                give(step * QUAD + index)
            return 0

        lax.fori_loop(0, block_rows // QUAD, packs, 0)

    early = block
    with jax.named_scope("b1_left"):
        take(left_all, left_recv, plane % 2, place_left)
    with jax.named_scope("b2_near"):
        take(right_all, right_recv, early * 2 + plane % 2, place_right)
    with jax.named_scope("b3_left"):
        take(left_all, left_recv, 1 - plane % 2, place_left)
    with jax.named_scope("b4_lines"):
        for index in range(GROUP):
            left_lines[index] = channel(left_mat, index, 0, block_lines)
    with jax.named_scope("c0_fin"):
        finish(early * 2 + plane % 2)
    with jax.named_scope("b5_far"):
        take(right_all, right_recv, early * 2 + 1 - plane % 2, place_right)
    with jax.named_scope("c1_fin"):
        finish(early * 2 + 1 - plane % 2)
    with jax.named_scope("c2_near"):
        take(right_all, right_recv, 2 - block, place_right)
    with jax.named_scope("c3_fin"):
        finish(2 - block)
    with jax.named_scope("c4_far"):
        take(right_all, right_recv, 3 - 3 * block, place_right)
    with jax.named_scope("c5_fin"):
        finish(3 - 3 * block)
    with jax.named_scope("d0_back"):
        all_of(owned, back_recv.at[0]).wait()

    with jax.named_scope("d1_out"):
        for side, at in [(side, at) for side in range(2) for at in range(tiles_back)]:
            piece = jnp.concatenate(
                [
                    owned[group, side, :, at * LANES : (at + 1) * LANES].astype(jnp.float32)
                    for group in range(groups)
                ],
                axis=0,
            )
            scaled = norm_axis(piece, 0).T.astype(jnp.bfloat16)
            projected = jnp.dot(scaled, weights[5], preferred_element_type=jnp.float32)
            base = side * part
            spots = [(2 * at, base, 0, part), (2 * at + 1, base, part, part)]
            if at < 2:
                spots.append((rows - 2 + at, base, cols, spare))
            if at == 2:
                rest = part - spare
                spots.append((rows - 2, base + spare, cols, rest))
                spots.append((rows - 1, base + spare, cols + rest, rest))
            for line, start, begin, length in spots:
                stop = start + length
                made = gate[line, start:stop] * projected[begin : begin + length]
                out[line, start:stop] = made.astype(jnp.bfloat16)
    with jax.named_scope("d2_sent"):
        all_of(right_all.at[pl.ds(0, devices - 1)], send.at[0]).wait()
        all_of(left_all.at[pl.ds(0, groups - 1)], send.at[1]).wait()
        all_of(triangle.at[pl.ds(0, groups - 1)], send.at[2]).wait()


def fused(sizes, pair_act, tile_mask, *weights):
    row_size, col_size, groups = sizes
    devices = row_size * col_size
    block_rows = groups // col_size
    rows, cols, width = pair_act.shape
    pairs = rows * cols
    spare = LANES - cols
    extra = rows - pairs // LANES
    dma = pltpu.SemaphoreType.DMA
    chunks = pltpu.VMEM((groups, GROUP, pairs), jnp.bfloat16)
    parts = pltpu.VMEM((groups, 2, GROUP, (rows // 2 - 1) * LANES), jnp.bfloat16)
    result = pl.pallas_call(
        functools.partial(fused_kernel, sizes, pair_act.shape),
        out_shape=pltpu.VMEM((rows, cols, width), jnp.bfloat16),
        in_specs=[pl.BlockSpec(memory_space=pltpu.HBM)] * 8,
        out_specs=pl.BlockSpec(memory_space=pltpu.VMEM),
        scratch_shapes=[
            pltpu.VMEM((extra, extra, extra + 1, spare, width), jnp.bfloat16),
            pltpu.VMEM(tile_mask.shape, tile_mask.dtype),
            pltpu.VMEM((6, width, width), jnp.bfloat16),
            dma((1,)),
            dma((2,)),
            pltpu.VMEM((pairs, width), jnp.bfloat16),
            pltpu.VMEM((rows, cols, width), jnp.float32),
            chunks,
            chunks,
            chunks,
            pltpu.VMEM((devices, GROUP, pairs), jnp.bfloat16),
            pltpu.VMEM((col_size, block_rows * rows * GROUP, LANES), jnp.float32),
            pltpu.VMEM((col_size, row_size * rows * GROUP, LANES), jnp.float32),
            pltpu.VMEM((GROUP, block_rows * rows, col_size * LANES), jnp.bfloat16),
            pltpu.VMEM((block_rows * rows * GROUP, LANES), jnp.float32),
            parts,
            parts,
            dma((3,)),
            dma((groups // QUAD,)),
            dma((devices // QUAD,)),
            dma((1,)),
            pltpu.SemaphoreType.REGULAR((3,)),
        ],
        compiler_params=pltpu.CompilerParams(collective_id=2, has_side_effects=True),
    )(pair_act.reshape(extra + 1, extra, extra, spare, width), tile_mask, *weights)
    return result


def fits(sizes, rows, cols):
    row_size, col_size, groups = sizes
    pairs = rows * cols
    spare = LANES - cols
    extra = rows - pairs // LANES
    if (row_size, col_size, groups) != (16, 2, 16):
        return False
    if spare <= 0 or pairs % LANES or extra <= 0:
        return False
    part = cols // 2
    if 2 * part != cols or 2 * (part - spare) != spare or rows % 2:
        return False
    return rows == extra * (extra + 1) and cols == extra * spare


def solution(mesh):
    def whole(pair_act, tile_mask, *weights):
        groups = pair_act.shape[2] // GROUP
        sizes = (mesh.shape["row"], mesh.shape["col"], groups)
        rows, cols = (pair_act.shape[0] // sizes[0], pair_act.shape[1] // sizes[1])
        body = fused if fits(sizes, rows, cols) else local
        return jax.shard_map(
            functools.partial(body, sizes),
            mesh=mesh,
            in_specs=(P("row", "col", None), P(), P(), P(), P(), P(), P(), P()),
            out_specs=P("row", "col", None),
            check_vma=False,
        )(pair_act, tile_mask, *weights)

    return whole
```

```python
import functools

import jax
import jax.numpy as jnp
from jax import lax
from jax.experimental import pallas as pl
from jax.experimental.pallas import tpu as pltpu
from jax.sharding import PartitionSpec as P

TILES = 12
GROUP = 8
MESH = pl.DeviceIdType.MESH


def norm_axis(values, axis):
    mean = jnp.mean(values, axis=axis, keepdims=True)
    centred = values - mean
    spread = jnp.mean(centred * centred, axis=axis, keepdims=True)
    return centred * lax.rsqrt(spread + 1e-05)


def place(flat, col_size):
    return (flat // col_size, flat % col_size)


def greet(flat, first, count, col_size):
    barrier = pltpu.get_barrier_semaphore()

    def signal(step, _):
        other = first + (flat - first + step) % count
        pl.semaphore_signal(barrier, inc=1, device_id=place(other, col_size), device_id_type=MESH)
        return 0

    lax.fori_loop(1, count, signal, 0)
    pl.semaphore_wait(barrier, count - 1)


def spread_kernel(
    sizes, left, right, left_all, right_all, own_sem, left_send, left_recv, right_send, right_recv
):
    row_size, col_size, groups = sizes
    devices = row_size * col_size
    flat = lax.axis_index("row") * col_size + lax.axis_index("col")
    member = flat % groups
    first = flat - member

    def chunk(source, group):
        return source.at[group]

    own_left = pltpu.make_async_copy(chunk(left, member), left_all.at[member], own_sem.at[0])
    own_right = pltpu.make_async_copy(chunk(right, member), right_all.at[flat], own_sem.at[1])
    own_left.start()
    own_right.start()
    greet(flat, 0, devices, col_size)

    def right_copy(step):
        to = (flat + step) % devices
        return pltpu.make_async_remote_copy(
            src_ref=chunk(right, to % groups),
            dst_ref=right_all.at[flat],
            send_sem=right_send.at[step],
            recv_sem=right_recv.at[step],
            device_id=place(to, col_size),
            device_id_type=MESH,
        )

    def left_copy(step):
        to = (member + step) % groups
        return pltpu.make_async_remote_copy(
            src_ref=chunk(left, to),
            dst_ref=left_all.at[member],
            send_sem=left_send.at[step],
            recv_sem=left_recv.at[step],
            device_id=place(first + to, col_size),
            device_id_type=MESH,
        )

    def start_right(step, _):
        right_copy(step).start()
        return 0

    def start_left(step, _):
        left_copy(step).start()
        return 0

    def wait_right(step, _):
        right_copy(step).wait()
        return 0

    def wait_left(step, _):
        left_copy(step).wait()
        return 0

    lax.fori_loop(1, devices, start_right, 0)
    lax.fori_loop(1, groups, start_left, 0)
    own_left.wait()
    own_right.wait()
    lax.fori_loop(1, groups, wait_left, 0)
    lax.fori_loop(1, devices, wait_right, 0)


def return_kernel(sizes, triangle, owned, own_sem, send, recv):
    row_size, col_size, groups = sizes
    flat = lax.axis_index("row") * col_size + lax.axis_index("col")
    member = flat % groups
    first = flat - member
    own = pltpu.make_async_copy(triangle.at[member], owned.at[member], own_sem)
    own.start()
    greet(flat, first, groups, col_size)

    def copy(step):
        to = (member + step) % groups
        return pltpu.make_async_remote_copy(
            src_ref=triangle.at[to],
            dst_ref=owned.at[member],
            send_sem=send.at[step],
            recv_sem=recv.at[step],
            device_id=place(first + to, col_size),
            device_id_type=MESH,
        )

    def start(step, _):
        copy(step).start()
        return 0

    def wait(step, _):
        copy(step).wait()
        return 0

    lax.fori_loop(1, groups, start, 0)
    own.wait()
    lax.fori_loop(1, groups, wait, 0)


def local(
    sizes, pair_act, tile_mask, w_left_gate, w_left, w_right_gate, w_right, w_out_gate, w_out
):
    row_size, col_size, groups = sizes
    devices = row_size * col_size
    block_rows = groups // col_size
    rows, cols, width = pair_act.shape
    residues = rows * row_size
    tile = residues // TILES
    normed = norm_axis(pair_act.astype(jnp.float32), 2).astype(jnp.bfloat16)
    tile_range = lax.iota(jnp.int32, TILES)
    row_ids = (lax.axis_index("row") * rows + lax.iota(jnp.int32, rows)) // tile
    col_ids = (lax.axis_index("col") * cols + lax.iota(jnp.int32, cols)) // tile
    row_hot = (row_ids[:, None] == tile_range[None, :]).astype(jnp.float32)
    col_hot = (col_ids[:, None] == tile_range[None, :]).astype(jnp.float32)
    pair_mask = jnp.dot(
        jnp.dot(row_hot, tile_mask.astype(jnp.float32), preferred_element_type=jnp.float32),
        col_hot.T,
        preferred_element_type=jnp.float32,
    )
    pairs = rows * cols
    flat_normed = normed.reshape(pairs, width)
    flat_mask = pair_mask.reshape(1, pairs)

    def project(weight):
        return jnp.einsum("pd,de->ep", flat_normed, weight, preferred_element_type=jnp.float32)

    def factor(gate, value):
        out = jax.nn.sigmoid(project(gate)) * project(value) * flat_mask
        return out.astype(jnp.bfloat16).reshape(groups, GROUP, pairs)

    left = factor(w_left_gate, w_left)
    right = factor(w_right_gate, w_right)
    anywhere = pl.BlockSpec(memory_space=pl.ANY)
    left_all, right_all = pl.pallas_call(
        functools.partial(spread_kernel, sizes),
        out_shape=(
            jax.ShapeDtypeStruct((groups, GROUP, pairs), jnp.bfloat16),
            jax.ShapeDtypeStruct((devices, GROUP, pairs), jnp.bfloat16),
        ),
        in_specs=[anywhere] * 2,
        out_specs=(anywhere, anywhere),
        scratch_shapes=[
            pltpu.SemaphoreType.DMA((2,)),
            pltpu.SemaphoreType.DMA((groups,)),
            pltpu.SemaphoreType.DMA((groups,)),
            pltpu.SemaphoreType.DMA((devices,)),
            pltpu.SemaphoreType.DMA((devices,)),
        ],
        compiler_params=pltpu.CompilerParams(collective_id=0, has_side_effects=True),
    )(left, right)
    left_rows = (
        left_all.reshape(block_rows, col_size, GROUP, rows, cols)
        .transpose(2, 0, 3, 1, 4)
        .reshape(GROUP, block_rows * rows, residues)
    )
    right_rows = (
        right_all.reshape(row_size, col_size, GROUP, rows, cols)
        .transpose(2, 0, 3, 1, 4)
        .reshape(GROUP, residues, residues)
    )
    triangle = jnp.einsum(
        "cik,cjk->cij", left_rows, right_rows, preferred_element_type=jnp.float32
    ).astype(jnp.bfloat16)
    triangle = (
        triangle.reshape(GROUP, block_rows, rows, col_size, cols)
        .transpose(1, 3, 0, 2, 4)
        .reshape(groups, GROUP, pairs)
    )
    owned = pl.pallas_call(
        functools.partial(return_kernel, sizes),
        out_shape=jax.ShapeDtypeStruct((groups, GROUP, pairs), jnp.bfloat16),
        in_specs=[anywhere],
        out_specs=anywhere,
        scratch_shapes=[
            pltpu.SemaphoreType.DMA,
            pltpu.SemaphoreType.DMA((groups,)),
            pltpu.SemaphoreType.DMA((groups,)),
        ],
        compiler_params=pltpu.CompilerParams(collective_id=1, has_side_effects=True),
    )(triangle)
    owned = owned.reshape(width, pairs)
    scaled = norm_axis(owned.astype(jnp.float32), 0).astype(jnp.bfloat16)
    projected = jnp.einsum("cp,ce->pe", scaled, w_out, preferred_element_type=jnp.float32)
    gate = jax.nn.sigmoid(
        jnp.einsum("pd,de->pe", flat_normed, w_out_gate, preferred_element_type=jnp.float32)
    )
    return (gate * projected).astype(jnp.bfloat16).reshape(rows, cols, width)


LANES = 128
QUAD = 4


def fused_kernel(sizes, shape, pair_in, tiles_in, *rest):
    weights_in, out = rest[:6], rest[6]
    (
        pair, tiles, weights, pair_sem, input_sem,
        normed, gate, left, right, left_all, right_all, left_mat, right_mat, left_lines, product, triangle, owned,
        send, left_recv, right_recv, back_recv, heard,
    ) = rest[7:]
    row_size, col_size, groups = sizes
    rows, cols, width = shape
    devices = row_size * col_size
    block_rows = groups // col_size
    plane_size = groups // 2
    pairs = rows * cols
    spare = LANES - cols
    count = pairs // LANES
    extra = rows - count
    tile = rows * row_size // TILES
    row, col = lax.axis_index("row"), lax.axis_index("col")
    flat = row * col_size + col
    member = flat % groups
    block = flat // groups
    first = block * groups
    plane = flat // plane_size
    core = flat // col_size % 2
    moves = [bit * (1 - 2 * (flat // bit % 2)) for bit in (groups, plane_size, QUAD, 1)]

    def reach(flips, to_core):
        moved = sum(move for flip, move in zip(flips, moves) if flip)
        return flat + moved + col_size * (to_core - core)

    barrier = pltpu.get_barrier_semaphore()
    sides = ((1, 0), (0, 1))

    def tell(semaphore, to):
        pl.semaphore_signal(
            semaphore, inc=1, device_id=place(to, col_size), device_id_type=MESH
        )

    fetches = [[], []]
    for part in range(extra):
        for source, target in (
            (pair_in.at[part], pair.at[part, :, pl.ds(0, extra)]),
            (pair_in.at[extra, part], pair.at[part, :, extra]),
        ):
            fetches[0].append(pltpu.make_async_copy(source, target, pair_sem.at[0]))
    for index, source in enumerate(weights_in):
        fetches[1].append(pltpu.make_async_copy(source, weights.at[index], input_sem.at[0]))
    tile_fetch = pltpu.make_async_copy(tiles_in, tiles, input_sem.at[1])

    def all_of(ref, sem):
        return pltpu.make_async_copy(ref, ref, sem)

    with jax.named_scope("a0_begin"):
        tile_fetch.start()
        for fetch in fetches[0]:
            fetch.start()

        for flips in sides:
            tell(barrier, reach((0, 0, *flips), core))
        for flips in ((1, 1), (1, 0), (0, 1)):
            for to_core in range(2):
                tell(barrier, reach((*flips, 0, 0), to_core))
        tell(barrier, reach((0, 0, 0, 0), 1 - core))
        for fetch in fetches[1]:
            fetch.start()
        tile_fetch.wait()
        all_of(pair, pair_sem.at[0]).wait()

    with jax.named_scope("a1_mask"):
        lane = lax.broadcasted_iota(jnp.int32, (GROUP, LANES), 1)
        low = lane < cols
        spot = lax.broadcasted_iota(jnp.int32, (TILES, LANES), 1)
        tile_low = lax.broadcasted_iota(jnp.int32, (TILES, LANES), 0) * tile
        direct = spot < cols
        masks = []
        turned_tiles = tiles[...].astype(jnp.float32).T
        for at in range(count):
            line = row * rows + jnp.where(direct, at, count + at // extra)
            within = col * cols + jnp.where(direct, spot, spot - cols + at % extra * spare)
            row_hot = ((line >= tile_low) & (line < tile_low + tile)).astype(jnp.float32)
            col_hot = ((within >= tile_low) & (within < tile_low + tile)).astype(jnp.float32)
            picked = jnp.dot(turned_tiles, row_hot, preferred_element_type=jnp.float32)
            masks.append(jnp.sum(picked * col_hot, axis=0, keepdims=True))
        mask = jnp.concatenate(masks, axis=1)

    with jax.named_scope("a2_ln"):
        values = pair[...].reshape(pairs, width).astype(jnp.float32)
        normed[...] = norm_axis(values, 1).astype(jnp.bfloat16)
        all_of(weights, input_sem.at[0]).wait()

    def project(index):
        turned = weights[index].astype(jnp.float32).T.astype(jnp.bfloat16)
        return lax.dot_general(
            turned, normed[...], (((1,), (1,)), ((), ())), preferred_element_type=jnp.float32
        )

    def factor(gate_index, index, target):
        made = jax.nn.sigmoid(project(gate_index)) * project(index) * mask
        for group in range(groups):
            target[group] = made[group * GROUP : (group + 1) * GROUP].astype(jnp.bfloat16)

    def copy_to(source, target, sent, received, to):
        pltpu.make_async_remote_copy(
            src_ref=source.at[to % groups],
            dst_ref=target,
            send_sem=sent,
            recv_sem=received,
            device_id=place(to, col_size),
            device_id_type=MESH,
        ).start()

    def send_right(to):
        copy_to(right, right_all.at[flat], send.at[0], right_recv.at[own_quad], to)

    def send_left(to):
        copy_to(left, left_all.at[member], send.at[1], left_recv.at[member // QUAD], to)

    def keep(source, target, received):
        return pltpu.make_async_copy(source.at[member], target, received)

    own_quad = flat // QUAD
    lows = ((1, 1), (0, 1), (1, 0), (0, 0))
    inner_flip = (plane % 2 + block) % 2
    to_inner = inner_flip * moves[1]
    to_outer = (1 - inner_flip) * moves[1]

    outer = (plane // 2 + plane + 1) % 2

    def send_across(low_flips, to_core, shift):
        send_right(reach((1, 0, *low_flips), to_core) + shift)

    def send_beside(low_flips, to_core):
        send_right(reach((0, 1, *low_flips), to_core))

    def send_early(low_flips):
        send_across(low_flips, 1, to_inner)
        send_across(low_flips, 0, to_outer)

    def send_besides(low_flips):
        send_beside(low_flips, 0)
        send_beside(low_flips, 1)

    def send_lefts(low_flips):
        for to_core in range(2):
            send_left(reach((0, 1, *low_flips), to_core))

    with jax.named_scope("a3_right"):
        factor(2, 3, right)
    with jax.named_scope("a4_bar"):
        pl.semaphore_wait(barrier, 9)
        for index, flips in enumerate(sides):
            tell(heard.at[index], reach((0, 0, *flips), core))
    with jax.named_scope("a5_send"):

        @pl.when(outer == 1)
        def _():
            send_besides(lows[3])

        @pl.when(outer == 0)
        def _():
            send_early(lows[3])

    with jax.named_scope("a6_left"):
        factor(0, 1, left)
    with jax.named_scope("a7_send"):
        send_lefts(lows[3])

        @pl.when(outer == 1)
        def _():
            send_early(lows[3])

    def send_level(low_flips, to_core):
        send_right(reach((0, 0, *low_flips), to_core))
        send_left(reach((0, 0, *low_flips), to_core))

    def send_mixed(low_flips):
        @pl.when(outer == 1)
        def _():
            send_lefts(low_flips)
            send_besides(low_flips)
            send_early(low_flips)

        @pl.when(outer == 0)
        def _():
            send_early(low_flips)
            send_lefts(low_flips)

        send_level(low_flips, 0)
        send_level(low_flips, 1)

    def hear(index):
        pl.semaphore_wait(heard.at[index], 1)
        if index == 0:
            tell(heard.at[2], reach((0, 0, *sides[1]), core))
        send_mixed(sides[index])

    with jax.named_scope("a8_hear"):
        send_level(lows[3], 1 - core)

        @pl.when(col == 0)
        def _():
            hear(0)
            hear(1)

        @pl.when(col != 0)
        def _():
            hear(1)
            hear(0)

    with jax.named_scope("a91_hear"):
        pl.semaphore_wait(heard.at[2], 1)
    with jax.named_scope("a92_send"):
        send_mixed(lows[0])

        @pl.when(outer == 0)
        def _():
            for low_flips in lows:
                send_beside(low_flips, 0)
            for low_flips in lows:
                send_beside(low_flips, 1)

        for low_flips in lows:
            send_across(low_flips, 0, to_inner)
            send_across(low_flips, 1, to_outer)
        keep(left, left_all.at[member], left_recv.at[member // QUAD]).start()
        keep(right, right_all.at[flat], right_recv.at[own_quad]).start()

    with jax.named_scope("b0_gate"):
        opened = jax.nn.sigmoid(
            jnp.dot(normed[...], weights[4], preferred_element_type=jnp.float32)
        )
        for at in range(count):
            middle = at * LANES + cols
            start = at % extra * spare
            gate[at] = opened[at * LANES : middle]
            gate[count + at // extra, start : start + spare] = opened[middle : middle + spare]

    def spread(chunk, target, half, start, clean):
        parts = [
            chunk[:, at : at + LANES].astype(jnp.float32) for at in range(0, pairs, LANES)
        ]
        lines = list(parts)
        for line in range(extra):
            base = line * extra
            made = pltpu.roll(parts[base], spare, 1)
            for piece in range(1, extra):
                moved = pltpu.roll(parts[base + piece], (piece + 1) * spare % LANES, 1)
                made = jnp.where(lane < piece * spare, made, moved)
            lines.append(made)
        for line, made in enumerate(lines):
            if clean:
                made = jnp.where(low, made, 0.0)
            target[half, pl.ds(pl.multiple_of((start + line) * GROUP, GROUP), GROUP), :] = made

    def place_right(source):
        spread(right_all[source], right_mat, source % col_size, source // col_size * rows, False)

    def place_left(source):
        spread(left_all[source], left_mat, source % col_size, source // col_size * rows, True)

    def each_of(start, length, do):
        def body(step, _):
            for index in range(QUAD):
                do(start + step * QUAD + index)
            return 0

        lax.fori_loop(0, length // QUAD, body, 0)

    quads = plane_size // QUAD

    def take(source_all, received, which, put):
        for step in range(quads):
            quad = which * quads + step
            all_of(source_all.at[pl.ds(quad * QUAD, QUAD)], received.at[quad]).wait()
            each_of(quad * QUAD, QUAD, put)

    block_lines = block_rows * rows

    def channel(target, index, start, count):
        first_line = pl.multiple_of(start * GROUP, GROUP) + index
        return jnp.concatenate(
            [
                target[half, pl.ds(first_line, count, stride=GROUP), :].astype(jnp.bfloat16)
                for half in range(col_size)
            ],
            axis=1,
        )

    part = cols // 2
    tiles_back = rows // 2 - 1

    def finish(which):
        half, side = which // 2, which % 2
        for index in range(GROUP):
            held = channel(right_mat, index, which * part, part)
            made = lax.dot_general(
                left_lines[index],
                jnp.concatenate([held, held, held[:spare]], axis=0),
                (((1,), (1,)), ((), ())),
                preferred_element_type=jnp.float32,
            )
            product[pl.ds(index, block_lines, stride=GROUP), :] = made

        def pack(part_row):
            to = part_row * col_size + half
            lines = [
                product[pl.ds(pl.multiple_of((part_row * rows + line) * GROUP, GROUP), GROUP), :]
                for line in range(rows)
            ]
            one, two = lines[rows - 2], lines[rows - 1]
            ends = [one, two]
            ends.append(
                jnp.where(
                    lane < LANES - spare // 2,
                    pltpu.roll(one, cols - spare, 1),
                    pltpu.roll(two, LANES - spare // 2 - part - spare, 1),
                )
            )
            for at in range(tiles_back):
                made = jnp.where(lane < part, lines[2 * at], lines[2 * at + 1])
                if at < len(ends):
                    made = jnp.where(low, made, ends[at])
                triangle[to, side, :, at * LANES : (at + 1) * LANES] = made.astype(jnp.bfloat16)

        def give(part_row):
            to = part_row * col_size + half

            @pl.when(to == member)
            def _():
                pltpu.make_async_copy(
                    triangle.at[to, side], owned.at[member, side], back_recv.at[0]
                ).start()

            @pl.when(to != member)
            def _():
                pltpu.make_async_remote_copy(
                    src_ref=triangle.at[to, side],
                    dst_ref=owned.at[member, side],
                    send_sem=send.at[2],
                    recv_sem=back_recv.at[0],
                    device_id=place(first + to, col_size),
                    device_id_type=MESH,
                ).start()

        def packs(step, _):
            for index in range(QUAD):
                pack(step * QUAD + index)
            for index in range(QUAD):
                give(step * QUAD + index)
            return 0

        lax.fori_loop(0, block_rows // QUAD, packs, 0)

    across_inner, across_outer = 2 - block, 3 - 3 * block
    beside = plane + 1 - 2 * (plane % 2)
    with jax.named_scope("b1_left"):
        take(left_all, left_recv, plane % 2, place_left)
    with jax.named_scope("b2_near"):
        take(right_all, right_recv, plane, place_right)
    with jax.named_scope("b3_left"):
        take(left_all, left_recv, 1 - plane % 2, place_left)
    with jax.named_scope("b4_lines"):
        for index in range(GROUP):
            left_lines[index] = channel(left_mat, index, 0, block_lines)
    with jax.named_scope("b5_fin"):
        finish(plane)
    swap = outer * core
    second = beside + swap * (across_inner - beside)
    third = across_inner + swap * (beside - across_inner)
    for index, which in enumerate((second, third, across_outer)):
        with jax.named_scope(f"c{2 * index}_take"):
            take(right_all, right_recv, which, place_right)
        with jax.named_scope(f"c{2 * index + 1}_fin"):
            finish(which)
    with jax.named_scope("d0_back"):
        all_of(owned, back_recv.at[0]).wait()

    with jax.named_scope("d1_out"):
        for side, at in [(side, at) for side in range(2) for at in range(tiles_back)]:
            piece = jnp.concatenate(
                [
                    owned[group, side, :, at * LANES : (at + 1) * LANES].astype(jnp.float32)
                    for group in range(groups)
                ],
                axis=0,
            )
            scaled = norm_axis(piece, 0).T.astype(jnp.bfloat16)
            projected = jnp.dot(scaled, weights[5], preferred_element_type=jnp.float32)
            base = side * part
            spots = [(2 * at, base, 0, part), (2 * at + 1, base, part, part)]
            if at < 2:
                spots.append((rows - 2 + at, base, cols, spare))
            if at == 2:
                rest = part - spare
                spots.append((rows - 2, base + spare, cols, rest))
                spots.append((rows - 1, base + spare, cols + rest, rest))
            for line, start, begin, length in spots:
                stop = start + length
                made = gate[line, start:stop] * projected[begin : begin + length]
                out[line, start:stop] = made.astype(jnp.bfloat16)
    with jax.named_scope("d2_sent"):
        all_of(right_all.at[pl.ds(0, devices - 1)], send.at[0]).wait()
        all_of(left_all.at[pl.ds(0, groups - 1)], send.at[1]).wait()
        all_of(triangle.at[pl.ds(0, groups - 1)], send.at[2]).wait()


def fused(sizes, pair_act, tile_mask, *weights):
    row_size, col_size, groups = sizes
    devices = row_size * col_size
    block_rows = groups // col_size
    rows, cols, width = pair_act.shape
    pairs = rows * cols
    spare = LANES - cols
    extra = rows - pairs // LANES
    dma = pltpu.SemaphoreType.DMA
    chunks = pltpu.VMEM((groups, GROUP, pairs), jnp.bfloat16)
    parts = pltpu.VMEM((groups, 2, GROUP, (rows // 2 - 1) * LANES), jnp.bfloat16)
    result = pl.pallas_call(
        functools.partial(fused_kernel, sizes, pair_act.shape),
        out_shape=pltpu.VMEM((rows, cols, width), jnp.bfloat16),
        in_specs=[pl.BlockSpec(memory_space=pltpu.HBM)] * 8,
        out_specs=pl.BlockSpec(memory_space=pltpu.VMEM),
        scratch_shapes=[
            pltpu.VMEM((extra, extra, extra + 1, spare, width), jnp.bfloat16),
            pltpu.VMEM(tile_mask.shape, tile_mask.dtype),
            pltpu.VMEM((6, width, width), jnp.bfloat16),
            dma((1,)),
            dma((2,)),
            pltpu.VMEM((pairs, width), jnp.bfloat16),
            pltpu.VMEM((rows, cols, width), jnp.float32),
            chunks,
            chunks,
            chunks,
            pltpu.VMEM((devices, GROUP, pairs), jnp.bfloat16),
            pltpu.VMEM((col_size, block_rows * rows * GROUP, LANES), jnp.float32),
            pltpu.VMEM((col_size, row_size * rows * GROUP, LANES), jnp.float32),
            pltpu.VMEM((GROUP, block_rows * rows, col_size * LANES), jnp.bfloat16),
            pltpu.VMEM((block_rows * rows * GROUP, LANES), jnp.float32),
            parts,
            parts,
            dma((3,)),
            dma((groups // QUAD,)),
            dma((devices // QUAD,)),
            dma((1,)),
            pltpu.SemaphoreType.REGULAR((3,)),
        ],
        compiler_params=pltpu.CompilerParams(collective_id=2, has_side_effects=True),
    )(pair_act.reshape(extra + 1, extra, extra, spare, width), tile_mask, *weights)
    return result


def fits(sizes, rows, cols):
    row_size, col_size, groups = sizes
    pairs = rows * cols
    spare = LANES - cols
    extra = rows - pairs // LANES
    if (row_size, col_size, groups) != (16, 2, 16):
        return False
    if spare <= 0 or pairs % LANES or extra <= 0:
        return False
    part = cols // 2
    if 2 * part != cols or 2 * (part - spare) != spare or rows % 2:
        return False
    return rows == extra * (extra + 1) and cols == extra * spare


def solution(mesh):
    def whole(pair_act, tile_mask, *weights):
        groups = pair_act.shape[2] // GROUP
        sizes = (mesh.shape["row"], mesh.shape["col"], groups)
        rows, cols = (pair_act.shape[0] // sizes[0], pair_act.shape[1] // sizes[1])
        body = fused if fits(sizes, rows, cols) else local
        return jax.shard_map(
            functools.partial(body, sizes),
            mesh=mesh,
            in_specs=(P("row", "col", None), P(), P(), P(), P(), P(), P(), P()),
            out_specs=P("row", "col", None),
            check_vma=False,
        )(pair_act, tile_mask, *weights)

    return whole
```

```python
import functools

import jax
import jax.numpy as jnp
from jax import lax
from jax.experimental import pallas as pl
from jax.experimental.pallas import tpu as pltpu
from jax.sharding import PartitionSpec as P

TILES = 12
GROUP = 8
MESH = pl.DeviceIdType.MESH


def norm_axis(values, axis):
    mean = jnp.mean(values, axis=axis, keepdims=True)
    centred = values - mean
    spread = jnp.mean(centred * centred, axis=axis, keepdims=True)
    return centred * lax.rsqrt(spread + 1e-05)


def place(flat, col_size):
    return (flat // col_size, flat % col_size)


def greet(flat, first, count, col_size):
    barrier = pltpu.get_barrier_semaphore()

    def signal(step, _):
        other = first + (flat - first + step) % count
        pl.semaphore_signal(barrier, inc=1, device_id=place(other, col_size), device_id_type=MESH)
        return 0

    lax.fori_loop(1, count, signal, 0)
    pl.semaphore_wait(barrier, count - 1)


def spread_kernel(
    sizes, left, right, left_all, right_all, own_sem, left_send, left_recv, right_send, right_recv
):
    row_size, col_size, groups = sizes
    devices = row_size * col_size
    flat = lax.axis_index("row") * col_size + lax.axis_index("col")
    member = flat % groups
    first = flat - member

    def chunk(source, group):
        return source.at[group]

    own_left = pltpu.make_async_copy(chunk(left, member), left_all.at[member], own_sem.at[0])
    own_right = pltpu.make_async_copy(chunk(right, member), right_all.at[flat], own_sem.at[1])
    own_left.start()
    own_right.start()
    greet(flat, 0, devices, col_size)

    def right_copy(step):
        to = (flat + step) % devices
        return pltpu.make_async_remote_copy(
            src_ref=chunk(right, to % groups),
            dst_ref=right_all.at[flat],
            send_sem=right_send.at[step],
            recv_sem=right_recv.at[step],
            device_id=place(to, col_size),
            device_id_type=MESH,
        )

    def left_copy(step):
        to = (member + step) % groups
        return pltpu.make_async_remote_copy(
            src_ref=chunk(left, to),
            dst_ref=left_all.at[member],
            send_sem=left_send.at[step],
            recv_sem=left_recv.at[step],
            device_id=place(first + to, col_size),
            device_id_type=MESH,
        )

    def start_right(step, _):
        right_copy(step).start()
        return 0

    def start_left(step, _):
        left_copy(step).start()
        return 0

    def wait_right(step, _):
        right_copy(step).wait()
        return 0

    def wait_left(step, _):
        left_copy(step).wait()
        return 0

    lax.fori_loop(1, devices, start_right, 0)
    lax.fori_loop(1, groups, start_left, 0)
    own_left.wait()
    own_right.wait()
    lax.fori_loop(1, groups, wait_left, 0)
    lax.fori_loop(1, devices, wait_right, 0)


def return_kernel(sizes, triangle, owned, own_sem, send, recv):
    row_size, col_size, groups = sizes
    flat = lax.axis_index("row") * col_size + lax.axis_index("col")
    member = flat % groups
    first = flat - member
    own = pltpu.make_async_copy(triangle.at[member], owned.at[member], own_sem)
    own.start()
    greet(flat, first, groups, col_size)

    def copy(step):
        to = (member + step) % groups
        return pltpu.make_async_remote_copy(
            src_ref=triangle.at[to],
            dst_ref=owned.at[member],
            send_sem=send.at[step],
            recv_sem=recv.at[step],
            device_id=place(first + to, col_size),
            device_id_type=MESH,
        )

    def start(step, _):
        copy(step).start()
        return 0

    def wait(step, _):
        copy(step).wait()
        return 0

    lax.fori_loop(1, groups, start, 0)
    own.wait()
    lax.fori_loop(1, groups, wait, 0)


def local(
    sizes, pair_act, tile_mask, w_left_gate, w_left, w_right_gate, w_right, w_out_gate, w_out
):
    row_size, col_size, groups = sizes
    devices = row_size * col_size
    block_rows = groups // col_size
    rows, cols, width = pair_act.shape
    residues = rows * row_size
    tile = residues // TILES
    normed = norm_axis(pair_act.astype(jnp.float32), 2).astype(jnp.bfloat16)
    tile_range = lax.iota(jnp.int32, TILES)
    row_ids = (lax.axis_index("row") * rows + lax.iota(jnp.int32, rows)) // tile
    col_ids = (lax.axis_index("col") * cols + lax.iota(jnp.int32, cols)) // tile
    row_hot = (row_ids[:, None] == tile_range[None, :]).astype(jnp.float32)
    col_hot = (col_ids[:, None] == tile_range[None, :]).astype(jnp.float32)
    pair_mask = jnp.dot(
        jnp.dot(row_hot, tile_mask.astype(jnp.float32), preferred_element_type=jnp.float32),
        col_hot.T,
        preferred_element_type=jnp.float32,
    )
    pairs = rows * cols
    flat_normed = normed.reshape(pairs, width)
    flat_mask = pair_mask.reshape(1, pairs)

    def project(weight):
        return jnp.einsum("pd,de->ep", flat_normed, weight, preferred_element_type=jnp.float32)

    def factor(gate, value):
        out = jax.nn.sigmoid(project(gate)) * project(value) * flat_mask
        return out.astype(jnp.bfloat16).reshape(groups, GROUP, pairs)

    left = factor(w_left_gate, w_left)
    right = factor(w_right_gate, w_right)
    anywhere = pl.BlockSpec(memory_space=pl.ANY)
    left_all, right_all = pl.pallas_call(
        functools.partial(spread_kernel, sizes),
        out_shape=(
            jax.ShapeDtypeStruct((groups, GROUP, pairs), jnp.bfloat16),
            jax.ShapeDtypeStruct((devices, GROUP, pairs), jnp.bfloat16),
        ),
        in_specs=[anywhere] * 2,
        out_specs=(anywhere, anywhere),
        scratch_shapes=[
            pltpu.SemaphoreType.DMA((2,)),
            pltpu.SemaphoreType.DMA((groups,)),
            pltpu.SemaphoreType.DMA((groups,)),
            pltpu.SemaphoreType.DMA((devices,)),
            pltpu.SemaphoreType.DMA((devices,)),
        ],
        compiler_params=pltpu.CompilerParams(collective_id=0, has_side_effects=True),
    )(left, right)
    left_rows = (
        left_all.reshape(block_rows, col_size, GROUP, rows, cols)
        .transpose(2, 0, 3, 1, 4)
        .reshape(GROUP, block_rows * rows, residues)
    )
    right_rows = (
        right_all.reshape(row_size, col_size, GROUP, rows, cols)
        .transpose(2, 0, 3, 1, 4)
        .reshape(GROUP, residues, residues)
    )
    triangle = jnp.einsum(
        "cik,cjk->cij", left_rows, right_rows, preferred_element_type=jnp.float32
    ).astype(jnp.bfloat16)
    triangle = (
        triangle.reshape(GROUP, block_rows, rows, col_size, cols)
        .transpose(1, 3, 0, 2, 4)
        .reshape(groups, GROUP, pairs)
    )
    owned = pl.pallas_call(
        functools.partial(return_kernel, sizes),
        out_shape=jax.ShapeDtypeStruct((groups, GROUP, pairs), jnp.bfloat16),
        in_specs=[anywhere],
        out_specs=anywhere,
        scratch_shapes=[
            pltpu.SemaphoreType.DMA,
            pltpu.SemaphoreType.DMA((groups,)),
            pltpu.SemaphoreType.DMA((groups,)),
        ],
        compiler_params=pltpu.CompilerParams(collective_id=1, has_side_effects=True),
    )(triangle)
    owned = owned.reshape(width, pairs)
    scaled = norm_axis(owned.astype(jnp.float32), 0).astype(jnp.bfloat16)
    projected = jnp.einsum("cp,ce->pe", scaled, w_out, preferred_element_type=jnp.float32)
    gate = jax.nn.sigmoid(
        jnp.einsum("pd,de->pe", flat_normed, w_out_gate, preferred_element_type=jnp.float32)
    )
    return (gate * projected).astype(jnp.bfloat16).reshape(rows, cols, width)


LANES = 128
QUAD = 4


def fused_kernel(sizes, shape, pair_in, tiles_in, *rest):
    weights_in, out = rest[:6], rest[6]
    (
        pair, tiles, weights, pair_sem, input_sem,
        normed, gate, left, right, left_all, right_all, left_mat, right_mat, left_lines, product, triangle, owned,
        send, left_recv, right_recv, back_recv, heard,
    ) = rest[7:]
    row_size, col_size, groups = sizes
    rows, cols, width = shape
    devices = row_size * col_size
    block_rows = groups // col_size
    plane_size = groups // 2
    pairs = rows * cols
    spare = LANES - cols
    count = pairs // LANES
    extra = rows - count
    tile = rows * row_size // TILES
    row, col = lax.axis_index("row"), lax.axis_index("col")
    flat = row * col_size + col
    member = flat % groups
    block = flat // groups
    first = block * groups
    plane = flat // plane_size
    core = flat // col_size % 2
    moves = [bit * (1 - 2 * (flat // bit % 2)) for bit in (groups, plane_size, QUAD, 1)]

    def reach(flips, to_core):
        moved = sum(move for flip, move in zip(flips, moves) if flip)
        return flat + moved + col_size * (to_core - core)

    barrier = pltpu.get_barrier_semaphore()
    sides = ((1, 0), (0, 1))

    def tell(semaphore, to):
        pl.semaphore_signal(
            semaphore, inc=1, device_id=place(to, col_size), device_id_type=MESH
        )

    fetches = [[], []]
    for part in range(extra):
        for source, target in (
            (pair_in.at[part], pair.at[part, :, pl.ds(0, extra)]),
            (pair_in.at[extra, part], pair.at[part, :, extra]),
        ):
            fetches[0].append(pltpu.make_async_copy(source, target, pair_sem.at[0]))
    for index, source in enumerate(weights_in):
        fetches[1].append(pltpu.make_async_copy(source, weights.at[index], input_sem.at[0]))
    tile_fetch = pltpu.make_async_copy(tiles_in, tiles, input_sem.at[1])

    def all_of(ref, sem):
        return pltpu.make_async_copy(ref, ref, sem)

    with jax.named_scope("a0_begin"):
        tile_fetch.start()
        for fetch in fetches[0]:
            fetch.start()

        for flips in sides:
            tell(barrier, reach((0, 0, *flips), core))
        for flips in ((1, 1), (1, 0), (0, 1)):
            for to_core in range(2):
                tell(barrier, reach((*flips, 0, 0), to_core))
        tell(barrier, reach((0, 0, 0, 0), 1 - core))
        for fetch in fetches[1]:
            fetch.start()
        tile_fetch.wait()
        all_of(pair, pair_sem.at[0]).wait()

    with jax.named_scope("a1_mask"):
        lane = lax.broadcasted_iota(jnp.int32, (GROUP, LANES), 1)
        low = lane < cols
        spot = lax.broadcasted_iota(jnp.int32, (TILES, LANES), 1)
        tile_low = lax.broadcasted_iota(jnp.int32, (TILES, LANES), 0) * tile
        direct = spot < cols
        masks = []
        turned_tiles = tiles[...].astype(jnp.float32).T
        for at in range(count):
            line = row * rows + jnp.where(direct, at, count + at // extra)
            within = col * cols + jnp.where(direct, spot, spot - cols + at % extra * spare)
            row_hot = ((line >= tile_low) & (line < tile_low + tile)).astype(jnp.float32)
            col_hot = ((within >= tile_low) & (within < tile_low + tile)).astype(jnp.float32)
            picked = jnp.dot(turned_tiles, row_hot, preferred_element_type=jnp.float32)
            masks.append(jnp.sum(picked * col_hot, axis=0, keepdims=True))
        mask = jnp.concatenate(masks, axis=1)

    with jax.named_scope("a2_ln"):
        values = pair[...].reshape(pairs, width).astype(jnp.float32)
        normed[...] = norm_axis(values, 1).astype(jnp.bfloat16)
        all_of(weights, input_sem.at[0]).wait()

    def project(index):
        turned = weights[index].astype(jnp.float32).T.astype(jnp.bfloat16)
        return lax.dot_general(
            turned, normed[...], (((1,), (1,)), ((), ())), preferred_element_type=jnp.float32
        )

    def factor(gate_index, index, target):
        made = jax.nn.sigmoid(project(gate_index)) * project(index) * mask
        for group in range(groups):
            target[group] = made[group * GROUP : (group + 1) * GROUP].astype(jnp.bfloat16)

    def copy_to(source, target, sent, received, to):
        pltpu.make_async_remote_copy(
            src_ref=source.at[to % groups],
            dst_ref=target,
            send_sem=sent,
            recv_sem=received,
            device_id=place(to, col_size),
            device_id_type=MESH,
        ).start()

    def send_right(to):
        copy_to(right, right_all.at[flat], send.at[0], right_recv.at[own_quad], to)

    def send_left(to):
        copy_to(left, left_all.at[member], send.at[1], left_recv.at[member // QUAD], to)

    def keep(source, target, received):
        return pltpu.make_async_copy(source.at[member], target, received)

    own_quad = flat // QUAD
    lows = ((1, 1), (0, 1), (1, 0), (0, 0))
    inner_flip = (plane % 2 + block) % 2
    to_inner = inner_flip * moves[1]
    to_outer = (1 - inner_flip) * moves[1]

    outer = (plane // 2 + plane + 1) % 2

    def send_across(low_flips, to_core, shift):
        send_right(reach((1, 0, *low_flips), to_core) + shift)

    def send_beside(low_flips, to_core):
        send_right(reach((0, 1, *low_flips), to_core))

    def send_early(low_flips):
        send_across(low_flips, 1, to_inner)
        send_across(low_flips, 0, to_outer)

    def send_besides(low_flips):
        send_beside(low_flips, 0)
        send_beside(low_flips, 1)

    def send_lefts(low_flips):
        for to_core in range(2):
            send_left(reach((0, 1, *low_flips), to_core))

    with jax.named_scope("a3_right"):
        factor(2, 3, right)
    with jax.named_scope("a4_bar"):
        pl.semaphore_wait(barrier, 9)
        for index, flips in enumerate(sides):
            tell(heard.at[index], reach((0, 0, *flips), core))
    with jax.named_scope("a5_send"):

        @pl.when(outer == 1)
        def _():
            send_besides(lows[3])

        @pl.when(outer == 0)
        def _():
            send_early(lows[3])

    with jax.named_scope("a6_left"):
        factor(0, 1, left)
    with jax.named_scope("a7_send"):
        send_lefts(lows[3])

        @pl.when(outer == 1)
        def _():
            send_early(lows[3])

        @pl.when(outer == 0)
        def _():
            send_across(lows[3], 0, to_inner)
            send_across(lows[3], 1, to_outer)

    def send_level(low_flips, to_core):
        send_right(reach((0, 0, *low_flips), to_core))
        send_left(reach((0, 0, *low_flips), to_core))

    def send_mixed(low_flips):
        @pl.when(plane == 0)
        def _():
            send_lefts(low_flips)
            send_besides(low_flips)
            send_early(low_flips)

        @pl.when(plane == 3)
        def _():
            send_lefts(low_flips)
            send_early(low_flips)
            send_besides(low_flips)

        @pl.when(outer == 0)
        def _():
            send_early(low_flips)
            send_lefts(low_flips)

        send_level(low_flips, 0)
        send_level(low_flips, 1)

    def hear(index):
        pl.semaphore_wait(heard.at[index], 1)
        if index == 0:
            tell(heard.at[2], reach((0, 0, *sides[1]), core))
        send_mixed(sides[index])

    with jax.named_scope("a8_hear"):
        send_level(lows[3], 1 - core)

        @pl.when(col == 0)
        def _():
            hear(0)
            hear(1)

        @pl.when(col != 0)
        def _():
            hear(1)
            hear(0)

    with jax.named_scope("a91_hear"):
        pl.semaphore_wait(heard.at[2], 1)
    with jax.named_scope("a92_send"):
        send_mixed(lows[0])

        @pl.when(outer == 0)
        def _():
            for low_flips in lows:
                send_beside(low_flips, 0)
            for low_flips in lows:
                send_beside(low_flips, 1)

        for low_flips in lows[:3]:
            send_across(low_flips, 0, to_inner)
            send_across(low_flips, 1, to_outer)

        @pl.when(outer == 1)
        def _():
            send_across(lows[3], 0, to_inner)
            send_across(lows[3], 1, to_outer)

        keep(left, left_all.at[member], left_recv.at[member // QUAD]).start()
        keep(right, right_all.at[flat], right_recv.at[own_quad]).start()

    with jax.named_scope("b0_gate"):
        opened = jax.nn.sigmoid(
            jnp.dot(normed[...], weights[4], preferred_element_type=jnp.float32)
        )
        for at in range(count):
            middle = at * LANES + cols
            start = at % extra * spare
            gate[at] = opened[at * LANES : middle]
            gate[count + at // extra, start : start + spare] = opened[middle : middle + spare]

    def spread(chunk, target, half, start, clean):
        parts = [
            chunk[:, at : at + LANES].astype(jnp.float32) for at in range(0, pairs, LANES)
        ]
        lines = list(parts)
        for line in range(extra):
            base = line * extra
            made = pltpu.roll(parts[base], spare, 1)
            for piece in range(1, extra):
                moved = pltpu.roll(parts[base + piece], (piece + 1) * spare % LANES, 1)
                made = jnp.where(lane < piece * spare, made, moved)
            lines.append(made)
        for line, made in enumerate(lines):
            if clean:
                made = jnp.where(low, made, 0.0)
            target[half, pl.ds(pl.multiple_of((start + line) * GROUP, GROUP), GROUP), :] = made

    def place_right(source):
        spread(right_all[source], right_mat, source % col_size, source // col_size * rows, False)

    def place_left(source):
        spread(left_all[source], left_mat, source % col_size, source // col_size * rows, True)

    def each_of(start, length, do):
        def body(step, _):
            for index in range(QUAD):
                do(start + step * QUAD + index)
            return 0

        lax.fori_loop(0, length // QUAD, body, 0)

    quads = plane_size // QUAD

    def take(source_all, received, which, put):
        for step in range(quads):
            quad = which * quads + step
            all_of(source_all.at[pl.ds(quad * QUAD, QUAD)], received.at[quad]).wait()
            each_of(quad * QUAD, QUAD, put)

    block_lines = block_rows * rows

    def channel(target, index, start, count):
        first_line = pl.multiple_of(start * GROUP, GROUP) + index
        return jnp.concatenate(
            [
                target[half, pl.ds(first_line, count, stride=GROUP), :].astype(jnp.bfloat16)
                for half in range(col_size)
            ],
            axis=1,
        )

    part = cols // 2
    tiles_back = rows // 2 - 1

    def finish(which):
        half, side = which // 2, which % 2
        for index in range(GROUP):
            held = channel(right_mat, index, which * part, part)
            made = lax.dot_general(
                left_lines[index],
                jnp.concatenate([held, held, held[:spare]], axis=0),
                (((1,), (1,)), ((), ())),
                preferred_element_type=jnp.float32,
            )
            product[pl.ds(index, block_lines, stride=GROUP), :] = made

        def pack(part_row):
            to = part_row * col_size + half
            lines = [
                product[pl.ds(pl.multiple_of((part_row * rows + line) * GROUP, GROUP), GROUP), :]
                for line in range(rows)
            ]
            one, two = lines[rows - 2], lines[rows - 1]
            ends = [one, two]
            ends.append(
                jnp.where(
                    lane < LANES - spare // 2,
                    pltpu.roll(one, cols - spare, 1),
                    pltpu.roll(two, LANES - spare // 2 - part - spare, 1),
                )
            )
            for at in range(tiles_back):
                made = jnp.where(lane < part, lines[2 * at], lines[2 * at + 1])
                if at < len(ends):
                    made = jnp.where(low, made, ends[at])
                triangle[to, side, :, at * LANES : (at + 1) * LANES] = made.astype(jnp.bfloat16)

        def give(part_row):
            to = part_row * col_size + half

            @pl.when(to == member)
            def _():
                pltpu.make_async_copy(
                    triangle.at[to, side], owned.at[member, side], back_recv.at[0]
                ).start()

            @pl.when(to != member)
            def _():
                pltpu.make_async_remote_copy(
                    src_ref=triangle.at[to, side],
                    dst_ref=owned.at[member, side],
                    send_sem=send.at[2],
                    recv_sem=back_recv.at[0],
                    device_id=place(first + to, col_size),
                    device_id_type=MESH,
                ).start()

        def packs(step, _):
            for index in range(QUAD):
                pack(step * QUAD + index)
            for index in range(QUAD):
                give(step * QUAD + index)
            return 0

        lax.fori_loop(0, block_rows // QUAD, packs, 0)

    across_inner, across_outer = 2 - block, 3 - 3 * block
    beside = plane + 1 - 2 * (plane % 2)
    with jax.named_scope("b1_left"):
        take(left_all, left_recv, plane % 2, place_left)
    with jax.named_scope("b2_near"):
        take(right_all, right_recv, plane, place_right)
    with jax.named_scope("b3_left"):
        take(left_all, left_recv, 1 - plane % 2, place_left)
    with jax.named_scope("b4_lines"):
        for index in range(GROUP):
            left_lines[index] = channel(left_mat, index, 0, block_lines)
    with jax.named_scope("b5_fin"):
        finish(plane)
    swap = outer * core
    second = beside + swap * (across_inner - beside)
    third = across_inner + swap * (beside - across_inner)
    for index, which in enumerate((second, third, across_outer)):
        with jax.named_scope(f"c{2 * index}_take"):
            take(right_all, right_recv, which, place_right)
        with jax.named_scope(f"c{2 * index + 1}_fin"):
            finish(which)
    with jax.named_scope("d0_back"):
        all_of(owned, back_recv.at[0]).wait()

    with jax.named_scope("d1_out"):
        for side, at in [(side, at) for side in range(2) for at in range(tiles_back)]:
            piece = jnp.concatenate(
                [
                    owned[group, side, :, at * LANES : (at + 1) * LANES].astype(jnp.float32)
                    for group in range(groups)
                ],
                axis=0,
            )
            scaled = norm_axis(piece, 0).T.astype(jnp.bfloat16)
            projected = jnp.dot(scaled, weights[5], preferred_element_type=jnp.float32)
            base = side * part
            spots = [(2 * at, base, 0, part), (2 * at + 1, base, part, part)]
            if at < 2:
                spots.append((rows - 2 + at, base, cols, spare))
            if at == 2:
                rest = part - spare
                spots.append((rows - 2, base + spare, cols, rest))
                spots.append((rows - 1, base + spare, cols + rest, rest))
            for line, start, begin, length in spots:
                stop = start + length
                made = gate[line, start:stop] * projected[begin : begin + length]
                out[line, start:stop] = made.astype(jnp.bfloat16)
    with jax.named_scope("d2_sent"):
        all_of(right_all.at[pl.ds(0, devices - 1)], send.at[0]).wait()
        all_of(left_all.at[pl.ds(0, groups - 1)], send.at[1]).wait()
        all_of(triangle.at[pl.ds(0, groups - 1)], send.at[2]).wait()


def fused(sizes, pair_act, tile_mask, *weights):
    row_size, col_size, groups = sizes
    devices = row_size * col_size
    block_rows = groups // col_size
    rows, cols, width = pair_act.shape
    pairs = rows * cols
    spare = LANES - cols
    extra = rows - pairs // LANES
    dma = pltpu.SemaphoreType.DMA
    chunks = pltpu.VMEM((groups, GROUP, pairs), jnp.bfloat16)
    parts = pltpu.VMEM((groups, 2, GROUP, (rows // 2 - 1) * LANES), jnp.bfloat16)
    result = pl.pallas_call(
        functools.partial(fused_kernel, sizes, pair_act.shape),
        out_shape=pltpu.VMEM((rows, cols, width), jnp.bfloat16),
        in_specs=[pl.BlockSpec(memory_space=pltpu.HBM)] * 8,
        out_specs=pl.BlockSpec(memory_space=pltpu.VMEM),
        scratch_shapes=[
            pltpu.VMEM((extra, extra, extra + 1, spare, width), jnp.bfloat16),
            pltpu.VMEM(tile_mask.shape, tile_mask.dtype),
            pltpu.VMEM((6, width, width), jnp.bfloat16),
            dma((1,)),
            dma((2,)),
            pltpu.VMEM((pairs, width), jnp.bfloat16),
            pltpu.VMEM((rows, cols, width), jnp.float32),
            chunks,
            chunks,
            chunks,
            pltpu.VMEM((devices, GROUP, pairs), jnp.bfloat16),
            pltpu.VMEM((col_size, block_rows * rows * GROUP, LANES), jnp.float32),
            pltpu.VMEM((col_size, row_size * rows * GROUP, LANES), jnp.float32),
            pltpu.VMEM((GROUP, block_rows * rows, col_size * LANES), jnp.bfloat16),
            pltpu.VMEM((block_rows * rows * GROUP, LANES), jnp.float32),
            parts,
            parts,
            dma((3,)),
            dma((groups // QUAD,)),
            dma((devices // QUAD,)),
            dma((1,)),
            pltpu.SemaphoreType.REGULAR((3,)),
        ],
        compiler_params=pltpu.CompilerParams(collective_id=2, has_side_effects=True),
    )(pair_act.reshape(extra + 1, extra, extra, spare, width), tile_mask, *weights)
    return result


def fits(sizes, rows, cols):
    row_size, col_size, groups = sizes
    pairs = rows * cols
    spare = LANES - cols
    extra = rows - pairs // LANES
    if (row_size, col_size, groups) != (16, 2, 16):
        return False
    if spare <= 0 or pairs % LANES or extra <= 0:
        return False
    part = cols // 2
    if 2 * part != cols or 2 * (part - spare) != spare or rows % 2:
        return False
    return rows == extra * (extra + 1) and cols == extra * spare


def solution(mesh):
    def whole(pair_act, tile_mask, *weights):
        groups = pair_act.shape[2] // GROUP
        sizes = (mesh.shape["row"], mesh.shape["col"], groups)
        rows, cols = (pair_act.shape[0] // sizes[0], pair_act.shape[1] // sizes[1])
        body = fused if fits(sizes, rows, cols) else local
        return jax.shard_map(
            functools.partial(body, sizes),
            mesh=mesh,
            in_specs=(P("row", "col", None), P(), P(), P(), P(), P(), P(), P()),
            out_specs=P("row", "col", None),
            check_vma=False,
        )(pair_act, tile_mask, *weights)

    return whole
```

```python
import functools

import jax
import jax.numpy as jnp
from jax import lax
from jax.experimental import pallas as pl
from jax.experimental.pallas import tpu as pltpu
from jax.sharding import PartitionSpec as P

TILES = 12
GROUP = 8
MESH = pl.DeviceIdType.MESH


def norm_axis(values, axis):
    mean = jnp.mean(values, axis=axis, keepdims=True)
    centred = values - mean
    spread = jnp.mean(centred * centred, axis=axis, keepdims=True)
    return centred * lax.rsqrt(spread + 1e-05)


def place(flat, col_size):
    return (flat // col_size, flat % col_size)


def greet(flat, first, count, col_size):
    barrier = pltpu.get_barrier_semaphore()

    def signal(step, _):
        other = first + (flat - first + step) % count
        pl.semaphore_signal(barrier, inc=1, device_id=place(other, col_size), device_id_type=MESH)
        return 0

    lax.fori_loop(1, count, signal, 0)
    pl.semaphore_wait(barrier, count - 1)


def spread_kernel(
    sizes, left, right, left_all, right_all, own_sem, left_send, left_recv, right_send, right_recv
):
    row_size, col_size, groups = sizes
    devices = row_size * col_size
    flat = lax.axis_index("row") * col_size + lax.axis_index("col")
    member = flat % groups
    first = flat - member

    def chunk(source, group):
        return source.at[group]

    own_left = pltpu.make_async_copy(chunk(left, member), left_all.at[member], own_sem.at[0])
    own_right = pltpu.make_async_copy(chunk(right, member), right_all.at[flat], own_sem.at[1])
    own_left.start()
    own_right.start()
    greet(flat, 0, devices, col_size)

    def right_copy(step):
        to = (flat + step) % devices
        return pltpu.make_async_remote_copy(
            src_ref=chunk(right, to % groups),
            dst_ref=right_all.at[flat],
            send_sem=right_send.at[step],
            recv_sem=right_recv.at[step],
            device_id=place(to, col_size),
            device_id_type=MESH,
        )

    def left_copy(step):
        to = (member + step) % groups
        return pltpu.make_async_remote_copy(
            src_ref=chunk(left, to),
            dst_ref=left_all.at[member],
            send_sem=left_send.at[step],
            recv_sem=left_recv.at[step],
            device_id=place(first + to, col_size),
            device_id_type=MESH,
        )

    def start_right(step, _):
        right_copy(step).start()
        return 0

    def start_left(step, _):
        left_copy(step).start()
        return 0

    def wait_right(step, _):
        right_copy(step).wait()
        return 0

    def wait_left(step, _):
        left_copy(step).wait()
        return 0

    lax.fori_loop(1, devices, start_right, 0)
    lax.fori_loop(1, groups, start_left, 0)
    own_left.wait()
    own_right.wait()
    lax.fori_loop(1, groups, wait_left, 0)
    lax.fori_loop(1, devices, wait_right, 0)


def return_kernel(sizes, triangle, owned, own_sem, send, recv):
    row_size, col_size, groups = sizes
    flat = lax.axis_index("row") * col_size + lax.axis_index("col")
    member = flat % groups
    first = flat - member
    own = pltpu.make_async_copy(triangle.at[member], owned.at[member], own_sem)
    own.start()
    greet(flat, first, groups, col_size)

    def copy(step):
        to = (member + step) % groups
        return pltpu.make_async_remote_copy(
            src_ref=triangle.at[to],
            dst_ref=owned.at[member],
            send_sem=send.at[step],
            recv_sem=recv.at[step],
            device_id=place(first + to, col_size),
            device_id_type=MESH,
        )

    def start(step, _):
        copy(step).start()
        return 0

    def wait(step, _):
        copy(step).wait()
        return 0

    lax.fori_loop(1, groups, start, 0)
    own.wait()
    lax.fori_loop(1, groups, wait, 0)


def local(
    sizes, pair_act, tile_mask, w_left_gate, w_left, w_right_gate, w_right, w_out_gate, w_out
):
    row_size, col_size, groups = sizes
    devices = row_size * col_size
    block_rows = groups // col_size
    rows, cols, width = pair_act.shape
    residues = rows * row_size
    tile = residues // TILES
    normed = norm_axis(pair_act.astype(jnp.float32), 2).astype(jnp.bfloat16)
    tile_range = lax.iota(jnp.int32, TILES)
    row_ids = (lax.axis_index("row") * rows + lax.iota(jnp.int32, rows)) // tile
    col_ids = (lax.axis_index("col") * cols + lax.iota(jnp.int32, cols)) // tile
    row_hot = (row_ids[:, None] == tile_range[None, :]).astype(jnp.float32)
    col_hot = (col_ids[:, None] == tile_range[None, :]).astype(jnp.float32)
    pair_mask = jnp.dot(
        jnp.dot(row_hot, tile_mask.astype(jnp.float32), preferred_element_type=jnp.float32),
        col_hot.T,
        preferred_element_type=jnp.float32,
    )
    pairs = rows * cols
    flat_normed = normed.reshape(pairs, width)
    flat_mask = pair_mask.reshape(1, pairs)

    def project(weight):
        return jnp.einsum("pd,de->ep", flat_normed, weight, preferred_element_type=jnp.float32)

    def factor(gate, value):
        out = jax.nn.sigmoid(project(gate)) * project(value) * flat_mask
        return out.astype(jnp.bfloat16).reshape(groups, GROUP, pairs)

    left = factor(w_left_gate, w_left)
    right = factor(w_right_gate, w_right)
    anywhere = pl.BlockSpec(memory_space=pl.ANY)
    left_all, right_all = pl.pallas_call(
        functools.partial(spread_kernel, sizes),
        out_shape=(
            jax.ShapeDtypeStruct((groups, GROUP, pairs), jnp.bfloat16),
            jax.ShapeDtypeStruct((devices, GROUP, pairs), jnp.bfloat16),
        ),
        in_specs=[anywhere] * 2,
        out_specs=(anywhere, anywhere),
        scratch_shapes=[
            pltpu.SemaphoreType.DMA((2,)),
            pltpu.SemaphoreType.DMA((groups,)),
            pltpu.SemaphoreType.DMA((groups,)),
            pltpu.SemaphoreType.DMA((devices,)),
            pltpu.SemaphoreType.DMA((devices,)),
        ],
        compiler_params=pltpu.CompilerParams(collective_id=0, has_side_effects=True),
    )(left, right)
    left_rows = (
        left_all.reshape(block_rows, col_size, GROUP, rows, cols)
        .transpose(2, 0, 3, 1, 4)
        .reshape(GROUP, block_rows * rows, residues)
    )
    right_rows = (
        right_all.reshape(row_size, col_size, GROUP, rows, cols)
        .transpose(2, 0, 3, 1, 4)
        .reshape(GROUP, residues, residues)
    )
    triangle = jnp.einsum(
        "cik,cjk->cij", left_rows, right_rows, preferred_element_type=jnp.float32
    ).astype(jnp.bfloat16)
    triangle = (
        triangle.reshape(GROUP, block_rows, rows, col_size, cols)
        .transpose(1, 3, 0, 2, 4)
        .reshape(groups, GROUP, pairs)
    )
    owned = pl.pallas_call(
        functools.partial(return_kernel, sizes),
        out_shape=jax.ShapeDtypeStruct((groups, GROUP, pairs), jnp.bfloat16),
        in_specs=[anywhere],
        out_specs=anywhere,
        scratch_shapes=[
            pltpu.SemaphoreType.DMA,
            pltpu.SemaphoreType.DMA((groups,)),
            pltpu.SemaphoreType.DMA((groups,)),
        ],
        compiler_params=pltpu.CompilerParams(collective_id=1, has_side_effects=True),
    )(triangle)
    owned = owned.reshape(width, pairs)
    scaled = norm_axis(owned.astype(jnp.float32), 0).astype(jnp.bfloat16)
    projected = jnp.einsum("cp,ce->pe", scaled, w_out, preferred_element_type=jnp.float32)
    gate = jax.nn.sigmoid(
        jnp.einsum("pd,de->pe", flat_normed, w_out_gate, preferred_element_type=jnp.float32)
    )
    return (gate * projected).astype(jnp.bfloat16).reshape(rows, cols, width)


LANES = 128
QUAD = 4


def fused_kernel(sizes, shape, pair_in, tiles_in, *rest):
    weights_in, (owned, gate, weights) = rest[:6], rest[6:9]
    (
        pair, tiles, pair_sem, input_sem,
        normed, left, right, left_all, right_all, left_mat, right_mat, left_lines, product, triangle,
        send, left_recv, right_recv, back_recv, heard,
    ) = rest[9:]
    row_size, col_size, groups = sizes
    rows, cols, width = shape
    devices = row_size * col_size
    block_rows = groups // col_size
    plane_size = groups // 2
    pairs = rows * cols
    spare = LANES - cols
    count = pairs // LANES
    extra = rows - count
    tile = rows * row_size // TILES
    row, col = lax.axis_index("row"), lax.axis_index("col")
    flat = row * col_size + col
    member = flat % groups
    block = flat // groups
    first = block * groups
    plane = flat // plane_size
    core = flat // col_size % 2
    moves = [bit * (1 - 2 * (flat // bit % 2)) for bit in (groups, plane_size, QUAD, 1)]

    def reach(flips, to_core):
        moved = sum(move for flip, move in zip(flips, moves) if flip)
        return flat + moved + col_size * (to_core - core)

    barrier = pltpu.get_barrier_semaphore()
    sides = ((1, 0), (0, 1))

    def tell(semaphore, to):
        pl.semaphore_signal(
            semaphore, inc=1, device_id=place(to, col_size), device_id_type=MESH
        )

    fetches = [[], []]
    for part in range(extra):
        for source, target in (
            (pair_in.at[part], pair.at[part, :, pl.ds(0, extra)]),
            (pair_in.at[extra, part], pair.at[part, :, extra]),
        ):
            fetches[0].append(pltpu.make_async_copy(source, target, pair_sem.at[0]))
    for index, source in enumerate(weights_in):
        fetches[1].append(pltpu.make_async_copy(source, weights.at[index], input_sem.at[0]))
    tile_fetch = pltpu.make_async_copy(tiles_in, tiles, input_sem.at[1])

    def all_of(ref, sem):
        return pltpu.make_async_copy(ref, ref, sem)

    with jax.named_scope("a0_begin"):
        tile_fetch.start()
        for fetch in fetches[0]:
            fetch.start()

        for flips in sides:
            tell(barrier, reach((0, 0, *flips), core))
        for flips in ((1, 1), (1, 0), (0, 1)):
            for to_core in range(2):
                tell(barrier, reach((*flips, 0, 0), to_core))
        tell(barrier, reach((0, 0, 0, 0), 1 - core))
        for fetch in fetches[1]:
            fetch.start()
        tile_fetch.wait()
        all_of(pair, pair_sem.at[0]).wait()

    with jax.named_scope("a1_mask"):
        lane = lax.broadcasted_iota(jnp.int32, (GROUP, LANES), 1)
        low = lane < cols
        spot = lax.broadcasted_iota(jnp.int32, (TILES, LANES), 1)
        tile_low = lax.broadcasted_iota(jnp.int32, (TILES, LANES), 0) * tile
        direct = spot < cols
        masks = []
        turned_tiles = tiles[...].astype(jnp.float32).T
        for at in range(count):
            line = row * rows + jnp.where(direct, at, count + at // extra)
            within = col * cols + jnp.where(direct, spot, spot - cols + at % extra * spare)
            row_hot = ((line >= tile_low) & (line < tile_low + tile)).astype(jnp.float32)
            col_hot = ((within >= tile_low) & (within < tile_low + tile)).astype(jnp.float32)
            picked = jnp.dot(turned_tiles, row_hot, preferred_element_type=jnp.float32)
            masks.append(jnp.sum(picked * col_hot, axis=0, keepdims=True))
        mask = jnp.concatenate(masks, axis=1)

    with jax.named_scope("a2_ln"):
        values = pair[...].reshape(pairs, width).astype(jnp.float32)
        normed[...] = norm_axis(values, 1).astype(jnp.bfloat16)
        all_of(weights, input_sem.at[0]).wait()

    def project(index):
        turned = weights[index].astype(jnp.float32).T.astype(jnp.bfloat16)
        return lax.dot_general(
            turned, normed[...], (((1,), (1,)), ((), ())), preferred_element_type=jnp.float32
        )

    def factor(gate_index, index, target):
        made = jax.nn.sigmoid(project(gate_index)) * project(index) * mask
        for group in range(groups):
            target[group] = made[group * GROUP : (group + 1) * GROUP].astype(jnp.bfloat16)

    def copy_to(source, target, sent, received, to):
        pltpu.make_async_remote_copy(
            src_ref=source.at[to % groups],
            dst_ref=target,
            send_sem=sent,
            recv_sem=received,
            device_id=place(to, col_size),
            device_id_type=MESH,
        ).start()

    def send_right(to):
        copy_to(right, right_all.at[flat], send.at[0], right_recv.at[own_quad], to)

    def send_left(to):
        copy_to(left, left_all.at[member], send.at[1], left_recv.at[member // QUAD], to)

    def keep(source, target, received):
        return pltpu.make_async_copy(source.at[member], target, received)

    own_quad = flat // QUAD
    lows = ((1, 1), (0, 1), (1, 0), (0, 0))
    inner_flip = (plane % 2 + block) % 2
    to_inner = inner_flip * moves[1]
    to_outer = (1 - inner_flip) * moves[1]

    outer = (plane // 2 + plane + 1) % 2

    def send_across(low_flips, to_core, shift):
        send_right(reach((1, 0, *low_flips), to_core) + shift)

    def send_beside(low_flips, to_core):
        send_right(reach((0, 1, *low_flips), to_core))

    def send_early(low_flips):
        send_across(low_flips, 1, to_inner)
        send_across(low_flips, 0, to_outer)

    def send_besides(low_flips):
        send_beside(low_flips, 0)
        send_beside(low_flips, 1)

    def send_lefts(low_flips):
        for to_core in range(2):
            send_left(reach((0, 1, *low_flips), to_core))

    with jax.named_scope("a3_right"):
        factor(2, 3, right)
    with jax.named_scope("a4_bar"):
        pl.semaphore_wait(barrier, 9)
        for index, flips in enumerate(sides):
            tell(heard.at[index], reach((0, 0, *flips), core))
    with jax.named_scope("a5_send"):

        @pl.when(outer == 1)
        def _():
            send_besides(lows[3])

        @pl.when(outer == 0)
        def _():
            send_early(lows[3])

    with jax.named_scope("a6_left"):
        factor(0, 1, left)
    with jax.named_scope("a7_send"):
        send_lefts(lows[3])

        @pl.when(outer == 1)
        def _():
            send_early(lows[3])

        @pl.when(outer == 0)
        def _():
            send_across(lows[3], 0, to_inner)
            send_across(lows[3], 1, to_outer)

    def send_level(low_flips, to_core):
        send_right(reach((0, 0, *low_flips), to_core))
        send_left(reach((0, 0, *low_flips), to_core))

    def send_mixed(low_flips):
        @pl.when(plane == 0)
        def _():
            send_lefts(low_flips)
            send_besides(low_flips)
            send_early(low_flips)

        @pl.when(plane == 3)
        def _():
            send_lefts(low_flips)
            send_early(low_flips)
            send_besides(low_flips)

        @pl.when(outer == 0)
        def _():
            send_early(low_flips)
            send_lefts(low_flips)

        send_level(low_flips, 0)
        send_level(low_flips, 1)

    def hear(index):
        pl.semaphore_wait(heard.at[index], 1)
        if index == 0:
            tell(heard.at[2], reach((0, 0, *sides[1]), core))
        send_mixed(sides[index])

    with jax.named_scope("a8_hear"):
        send_level(lows[3], 1 - core)

        @pl.when(col == 0)
        def _():
            hear(0)
            hear(1)

        @pl.when(col != 0)
        def _():
            hear(1)
            hear(0)

    with jax.named_scope("a91_hear"):
        pl.semaphore_wait(heard.at[2], 1)
    with jax.named_scope("a92_send"):
        send_mixed(lows[0])

        @pl.when(outer == 0)
        def _():
            for low_flips in lows:
                send_beside(low_flips, 0)
            for low_flips in lows:
                send_beside(low_flips, 1)

        for low_flips in lows[:3]:
            send_across(low_flips, 0, to_inner)
            send_across(low_flips, 1, to_outer)

        @pl.when(outer == 1)
        def _():
            send_across(lows[3], 0, to_inner)
            send_across(lows[3], 1, to_outer)

        keep(left, left_all.at[member], left_recv.at[member // QUAD]).start()
        keep(right, right_all.at[flat], right_recv.at[own_quad]).start()

    with jax.named_scope("b0_gate"):
        opened = jax.nn.sigmoid(
            jnp.dot(normed[...], weights[4], preferred_element_type=jnp.float32)
        )
        for at in range(count):
            middle = at * LANES + cols
            start = at % extra * spare
            gate[at] = opened[at * LANES : middle]
            gate[count + at // extra, start : start + spare] = opened[middle : middle + spare]

    def spread(chunk, target, half, start, clean):
        parts = [
            chunk[:, at : at + LANES].astype(jnp.float32) for at in range(0, pairs, LANES)
        ]
        lines = list(parts)
        for line in range(extra):
            base = line * extra
            made = pltpu.roll(parts[base], spare, 1)
            for piece in range(1, extra):
                moved = pltpu.roll(parts[base + piece], (piece + 1) * spare % LANES, 1)
                made = jnp.where(lane < piece * spare, made, moved)
            lines.append(made)
        for line, made in enumerate(lines):
            if clean:
                made = jnp.where(low, made, 0.0)
            target[half, pl.ds(pl.multiple_of((start + line) * GROUP, GROUP), GROUP), :] = made

    def place_right(source):
        spread(right_all[source], right_mat, source % col_size, source // col_size * rows, False)

    def place_left(source):
        spread(left_all[source], left_mat, source % col_size, source // col_size * rows, True)

    def each_of(start, length, do):
        def body(step, _):
            for index in range(QUAD):
                do(start + step * QUAD + index)
            return 0

        lax.fori_loop(0, length // QUAD, body, 0)

    quads = plane_size // QUAD

    def take(source_all, received, which, put):
        for step in range(quads):
            quad = which * quads + step
            all_of(source_all.at[pl.ds(quad * QUAD, QUAD)], received.at[quad]).wait()
            each_of(quad * QUAD, QUAD, put)

    block_lines = block_rows * rows

    def channel(target, index, start, count):
        first_line = pl.multiple_of(start * GROUP, GROUP) + index
        return jnp.concatenate(
            [
                target[half, pl.ds(first_line, count, stride=GROUP), :].astype(jnp.bfloat16)
                for half in range(col_size)
            ],
            axis=1,
        )

    part = cols // 2
    tiles_back = rows // 2 - 1

    def finish(which):
        half, side = which // 2, which % 2
        for index in range(GROUP):
            held = channel(right_mat, index, which * part, part)
            made = lax.dot_general(
                left_lines[index],
                jnp.concatenate([held, held, held[:spare]], axis=0),
                (((1,), (1,)), ((), ())),
                preferred_element_type=jnp.float32,
            )
            product[pl.ds(index, block_lines, stride=GROUP), :] = made

        def pack(part_row):
            to = part_row * col_size + half
            lines = [
                product[pl.ds(pl.multiple_of((part_row * rows + line) * GROUP, GROUP), GROUP), :]
                for line in range(rows)
            ]
            one, two = lines[rows - 2], lines[rows - 1]
            ends = [one, two]
            ends.append(
                jnp.where(
                    lane < LANES - spare // 2,
                    pltpu.roll(one, cols - spare, 1),
                    pltpu.roll(two, LANES - spare // 2 - part - spare, 1),
                )
            )
            for at in range(tiles_back):
                made = jnp.where(lane < part, lines[2 * at], lines[2 * at + 1])
                if at < len(ends):
                    made = jnp.where(low, made, ends[at])
                triangle[to, side, :, at * LANES : (at + 1) * LANES] = made.astype(jnp.bfloat16)

        def give(part_row):
            to = part_row * col_size + half

            @pl.when(to == member)
            def _():
                pltpu.make_async_copy(
                    triangle.at[to, side], owned.at[member, side], back_recv.at[0]
                ).start()

            @pl.when(to != member)
            def _():
                pltpu.make_async_remote_copy(
                    src_ref=triangle.at[to, side],
                    dst_ref=owned.at[member, side],
                    send_sem=send.at[2],
                    recv_sem=back_recv.at[0],
                    device_id=place(first + to, col_size),
                    device_id_type=MESH,
                ).start()

        def packs(step, _):
            for index in range(QUAD):
                pack(step * QUAD + index)
            for index in range(QUAD):
                give(step * QUAD + index)
            return 0

        lax.fori_loop(0, block_rows // QUAD, packs, 0)

    across_inner, across_outer = 2 - block, 3 - 3 * block
    beside = plane + 1 - 2 * (plane % 2)
    with jax.named_scope("b1_left"):
        take(left_all, left_recv, plane % 2, place_left)
    with jax.named_scope("b2_near"):
        take(right_all, right_recv, plane, place_right)
    with jax.named_scope("b3_left"):
        take(left_all, left_recv, 1 - plane % 2, place_left)
    with jax.named_scope("b4_lines"):
        for index in range(GROUP):
            left_lines[index] = channel(left_mat, index, 0, block_lines)
    with jax.named_scope("b5_fin"):
        finish(plane)
    swap = outer * core
    second = beside + swap * (across_inner - beside)
    third = across_inner + swap * (beside - across_inner)
    for index, which in enumerate((second, third, across_outer)):
        with jax.named_scope(f"c{2 * index}_take"):
            take(right_all, right_recv, which, place_right)
        with jax.named_scope(f"c{2 * index + 1}_fin"):
            finish(which)
    with jax.named_scope("d0_back"):
        all_of(owned, back_recv.at[0]).wait()

    with jax.named_scope("d2_sent"):
        all_of(right_all.at[pl.ds(0, devices - 1)], send.at[0]).wait()
        all_of(left_all.at[pl.ds(0, groups - 1)], send.at[1]).wait()
        all_of(triangle.at[pl.ds(0, groups - 1)], send.at[2]).wait()


def close_kernel(owned, gate, weights, out, made_out, sem):
    groups = owned.shape[0]
    rows, cols, width = gate.shape
    spare = LANES - cols
    part = cols // 2
    tiles_back = rows // 2 - 1
    for side, at in [(side, at) for side in range(2) for at in range(tiles_back)]:
        piece = jnp.concatenate(
            [
                owned[group, side, :, at * LANES : (at + 1) * LANES].astype(jnp.float32)
                for group in range(groups)
            ],
            axis=0,
        )
        scaled = norm_axis(piece, 0).T.astype(jnp.bfloat16)
        projected = jnp.dot(scaled, weights[5], preferred_element_type=jnp.float32)
        base = side * part
        spots = [(2 * at, base, 0, part), (2 * at + 1, base, part, part)]
        if at < 2:
            spots.append((rows - 2 + at, base, cols, spare))
        if at == 2:
            rest = part - spare
            spots.append((rows - 2, base + spare, cols, rest))
            spots.append((rows - 1, base + spare, cols + rest, rest))
        for line, start, begin, length in spots:
            stop = start + length
            made = gate[line, start:stop] * projected[begin : begin + length]
            made_out[line, start:stop] = made.astype(jnp.bfloat16)
        lines = [(2 * at, 2)]
        if at == 2:
            lines.append((rows - 2, 2))
        for line, length in lines:
            piece = (pl.ds(line, length), pl.ds(base, part))
            pltpu.make_async_copy(made_out.at[piece], out.at[piece], sem).start()
    pltpu.make_async_copy(made_out, made_out, sem).wait()


def fused(sizes, pair_act, tile_mask, *weights):
    row_size, col_size, groups = sizes
    devices = row_size * col_size
    block_rows = groups // col_size
    rows, cols, width = pair_act.shape
    pairs = rows * cols
    spare = LANES - cols
    extra = rows - pairs // LANES
    dma = pltpu.SemaphoreType.DMA
    chunks = pltpu.VMEM((groups, GROUP, pairs), jnp.bfloat16)
    parts = pltpu.VMEM((groups, 2, GROUP, (rows // 2 - 1) * LANES), jnp.bfloat16)
    kept = pl.BlockSpec(memory_space=pltpu.VMEM)
    results = pl.pallas_call(
        functools.partial(fused_kernel, sizes, pair_act.shape),
        out_shape=(
            parts,
            pltpu.VMEM((rows, cols, width), jnp.float32),
            pltpu.VMEM((6, width, width), jnp.bfloat16),
        ),
        in_specs=[pl.BlockSpec(memory_space=pltpu.HBM)] * 8,
        out_specs=(kept, kept, kept),
        scratch_shapes=[
            pltpu.VMEM((extra, extra, extra + 1, spare, width), jnp.bfloat16),
            pltpu.VMEM(tile_mask.shape, tile_mask.dtype),
            dma((1,)),
            dma((2,)),
            pltpu.VMEM((pairs, width), jnp.bfloat16),
            chunks,
            chunks,
            chunks,
            pltpu.VMEM((devices, GROUP, pairs), jnp.bfloat16),
            pltpu.VMEM((col_size, block_rows * rows * GROUP, LANES), jnp.float32),
            pltpu.VMEM((col_size, row_size * rows * GROUP, LANES), jnp.float32),
            pltpu.VMEM((GROUP, block_rows * rows, col_size * LANES), jnp.bfloat16),
            pltpu.VMEM((block_rows * rows * GROUP, LANES), jnp.float32),
            parts,
            dma((3,)),
            dma((groups // QUAD,)),
            dma((devices // QUAD,)),
            dma((1,)),
            pltpu.SemaphoreType.REGULAR((3,)),
        ],
        compiler_params=pltpu.CompilerParams(collective_id=2, has_side_effects=True),
    )(pair_act.reshape(extra + 1, extra, extra, spare, width), tile_mask, *weights)
    return pl.pallas_call(
        close_kernel,
        out_shape=jax.ShapeDtypeStruct((rows, cols, width), jnp.bfloat16),
        in_specs=[kept] * 3,
        out_specs=pl.BlockSpec(memory_space=pltpu.HBM),
        scratch_shapes=[pltpu.VMEM((rows, cols, width), jnp.bfloat16), pltpu.SemaphoreType.DMA],
    )(*[pltpu.with_memory_space_constraint(array, pltpu.VMEM) for array in results])


def fits(sizes, rows, cols):
    row_size, col_size, groups = sizes
    pairs = rows * cols
    spare = LANES - cols
    extra = rows - pairs // LANES
    if (row_size, col_size, groups) != (16, 2, 16):
        return False
    if spare <= 0 or pairs % LANES or extra <= 0:
        return False
    part = cols // 2
    if 2 * part != cols or 2 * (part - spare) != spare or rows % 2:
        return False
    return rows == extra * (extra + 1) and cols == extra * spare


def solution(mesh):
    def whole(pair_act, tile_mask, *weights):
        groups = pair_act.shape[2] // GROUP
        sizes = (mesh.shape["row"], mesh.shape["col"], groups)
        rows, cols = (pair_act.shape[0] // sizes[0], pair_act.shape[1] // sizes[1])
        body = fused if fits(sizes, rows, cols) else local
        return jax.shard_map(
            functools.partial(body, sizes),
            mesh=mesh,
            in_specs=(P("row", "col", None), P(), P(), P(), P(), P(), P(), P()),
            out_specs=P("row", "col", None),
            check_vma=False,
        )(pair_act, tile_mask, *weights)

    return whole
```
